32 devices in a mesh: tp: 32 (over z, y, x, core).
Axes of the slice: x: 2, y: 2, z: 4, core: 2. Of those that a mesh axis runs over, the one named last changes fastest.
Arguments:
- tokens: int32 [2, 1024], replicated
- lengths: int32 [1024], replicated
- embedding: bfloat16 [50304, 2560], P('tp')
- ln_scale: float32 [2, 2560], replicated
- w_q: bfloat16 [2, 2560, 32, 80], P(None, None, 'tp')
- w_kv: bfloat16 [2, 2560, 160], replicated
- w_o: bfloat16 [2, 32, 80, 2560], P(None, 'tp')
- w_gate: bfloat16 [2, 2560, 10240], P(None, None, 'tp')
- w_up: bfloat16 [2, 2560, 10240], P(None, None, 'tp')
- w_down: bfloat16 [2, 10240, 2560], P(None, 'tp')
- final_scale: float32 [2560], replicated
- k_cache: bfloat16 [2, 1024, 256, 80], P(None, 'tp')
- v_cache: bfloat16 [2, 1024, 256, 80], P(None, 'tp')
Outputs:
- output 1: float32 [2, 1024, 50304], P(None, None, 'tp')
- output 2: bfloat16 [2, 1024, 256, 80], P(None, 'tp')
- output 3: bfloat16 [2, 1024, 256, 80], P(None, 'tp')
All inputs are finite; a program needn't handle non-finite values.
Results may differ from the reference program's by a relative error of at most 0.00699987.
Values are sent between devices in bfloat16 or wider.
A program may use at most 1 GiB of HBM per device.

```python
import jax
import jax.numpy as jnp
from jax import lax

VOCAB = 50304
D = 2560
HEADS = 32
HEAD = 80
FF = 10240
BATCH = 1024
SEQ = 256
STEPS = 2
LAYERS = 2
LN_EPS = 1e-6


def draw_tokens(rng_key):
    key_off, key_perm = jax.random.split(rng_key)
    stride = VOCAB // BATCH
    starts = (jnp.arange(BATCH, dtype=jnp.int32) * VOCAB) // BATCH
    offsets = jax.random.randint(key_off, (STEPS, BATCH), 0, stride, dtype=jnp.int32)
    orders = jax.vmap(lambda one_key: jax.random.permutation(one_key, BATCH))(jax.random.split(key_perm, STEPS))
    return jnp.take_along_axis(starts[None, :] + offsets, orders, axis=1)


def draw_lengths(rng_key):
    key_base, key_shift, key_pick = jax.random.split(rng_key, 3)
    longest = SEQ - STEPS
    base_len = jax.random.randint(key_base, (BATCH,), 1, longest + 1, dtype=jnp.int32)
    shifts = jax.random.randint(key_shift, (BATCH,), 0, 8, dtype=jnp.int32)
    short_len = jnp.maximum(jnp.right_shift(base_len, shifts), 1)
    chosen = jax.random.randint(key_pick, (), 0, BATCH, dtype=jnp.int32)
    return jnp.where(jnp.arange(BATCH, dtype=jnp.int32) == chosen, longest, short_len).astype(jnp.int32)


def normal_draw(rng_key, arr_shape, spread):
    return jax.random.normal(rng_key, arr_shape, jnp.float32) * spread


def setup_inputs(seed: int = 0) -> dict:
    key_list = jax.random.split(jax.random.key(seed), 14)
    cache_shape = (LAYERS, BATCH, SEQ, HEAD)
    return {
        'tokens': draw_tokens(key_list[0]),
        'lengths': draw_lengths(key_list[1]),
        'embedding': normal_draw(key_list[2], (VOCAB, D), 1.0).astype(jnp.bfloat16),
        'ln_scale': 1.0 + normal_draw(key_list[3], (LAYERS, D), 0.2),
        'w_q': normal_draw(key_list[4], (LAYERS, D, HEADS, HEAD), D ** -0.5).astype(jnp.bfloat16),
        'w_kv': normal_draw(key_list[5], (LAYERS, D, 2 * HEAD), D ** -0.5).astype(jnp.bfloat16),
        'w_o': normal_draw(key_list[6], (LAYERS, HEADS, HEAD, D), (HEADS * HEAD) ** -0.5).astype(jnp.bfloat16),
        'w_gate': normal_draw(key_list[7], (LAYERS, D, FF), D ** -0.5).astype(jnp.bfloat16),
        'w_up': normal_draw(key_list[8], (LAYERS, D, FF), D ** -0.5).astype(jnp.bfloat16),
        'w_down': normal_draw(key_list[9], (LAYERS, FF, D), FF ** -0.5).astype(jnp.bfloat16),
        'final_scale': 1.0 + normal_draw(key_list[10], (D,), 0.2),
        'k_cache': normal_draw(key_list[11], cache_shape, 1.5).astype(jnp.bfloat16),
        'v_cache': (normal_draw(key_list[12], cache_shape, 1.0) + normal_draw(key_list[13], (LAYERS, BATCH, 1, HEAD), 0.7)).astype(jnp.bfloat16),
    }


def layer_norm(residual, ln_gain):
    x_f32 = residual.astype(jnp.float32)
    row_mean = jnp.mean(x_f32, axis=-1, keepdims=True)
    centred = x_f32 - row_mean
    row_var = jnp.mean(centred * centred, axis=-1, keepdims=True)
    return (centred * lax.rsqrt(row_var + LN_EPS) * ln_gain).astype(jnp.bfloat16)


def rotary(features, positions):
    half_dim = features.shape[-1] // 2
    inv_freq = 10000.0 ** (-jnp.arange(half_dim, dtype=jnp.float32) / half_dim)
    angles = positions[..., None].astype(jnp.float32) * inv_freq
    cos_t = jnp.cos(angles)
    sin_t = jnp.sin(angles)
    lo_half = features[..., :half_dim]
    hi_half = features[..., half_dim:]
    return jnp.concatenate([lo_half * cos_t - hi_half * sin_t, lo_half * sin_t + hi_half * cos_t], axis=-1)


def attend_one(operands):
    query_rows, keys_seq, values_seq, position = operands
    scores = jnp.dot(query_rows, keys_seq.T, preferred_element_type=jnp.float32) * HEAD ** -0.5
    visible = jnp.arange(SEQ) <= position
    scores = jnp.where(visible[None, :], scores, -jnp.inf)
    attn_probs = jax.nn.softmax(scores, axis=-1).astype(jnp.bfloat16)
    return jnp.dot(attn_probs, values_seq, preferred_element_type=jnp.float32).astype(jnp.bfloat16)


def decode_layer(residual, positions, layer_params):
    ln_gain, w_q, w_kv, w_o, w_gate, w_up, w_down, k_layer, v_layer = layer_params
    normed = layer_norm(residual, ln_gain)
    q_flat = jnp.dot(normed, w_q.reshape(D, HEADS * HEAD), preferred_element_type=jnp.float32)
    queries = rotary(q_flat.reshape(BATCH, HEADS, HEAD), positions[:, None]).astype(jnp.bfloat16)
    kv_new = jnp.dot(normed, w_kv, preferred_element_type=jnp.float32)
    k_new = rotary(kv_new[:, :HEAD], positions).astype(jnp.bfloat16)
    v_new = kv_new[:, HEAD:].astype(jnp.bfloat16)
    batch_idx = jnp.arange(BATCH)
    k_layer = k_layer.at[batch_idx, positions].set(k_new)
    v_layer = v_layer.at[batch_idx, positions].set(v_new)
    attn_out = lax.map(attend_one, (queries, k_layer, v_layer, positions))
    attn_sum = jnp.dot(attn_out.reshape(BATCH, HEADS * HEAD), w_o.reshape(HEADS * HEAD, D), preferred_element_type=jnp.float32)
    gate_proj = jnp.dot(normed, w_gate, preferred_element_type=jnp.float32)
    up_proj = jnp.dot(normed, w_up, preferred_element_type=jnp.float32)
    hidden = (jax.nn.silu(gate_proj) * up_proj).astype(jnp.bfloat16)
    mlp_sum = jnp.dot(hidden, w_down, preferred_element_type=jnp.float32)
    residual = (residual.astype(jnp.float32) + (attn_sum + mlp_sum)).astype(jnp.bfloat16)
    return residual, k_layer, v_layer


def reference(tokens, lengths, embedding, ln_scale, w_q, w_kv, w_o, w_gate, w_up, w_down, final_scale, k_cache, v_cache):
    def one_step(caches, step_in):
        k_all, v_all = caches
        tok_row, step_idx = step_in
        positions = lengths + step_idx
        residual = embedding[tok_row]

        def one_layer(resid_in, layer_params):
            resid_out, k_layer, v_layer = decode_layer(resid_in, positions, layer_params)
            return resid_out, (k_layer, v_layer)

        residual, (k_all, v_all) = lax.scan(one_layer, residual, (ln_scale, w_q, w_kv, w_o, w_gate, w_up, w_down, k_all, v_all))
        normed = layer_norm(residual, final_scale)
        logits = jnp.dot(normed, embedding.T, preferred_element_type=jnp.float32) * D ** -0.5
        return (k_all, v_all), logits

    (k_out, v_out), logits = lax.scan(one_step, (k_cache, v_cache), (tokens, jnp.arange(STEPS, dtype=jnp.int32)))
    return logits, k_out, v_out
```

```python
import jax
import jax.numpy as jnp
from jax import lax
from jax.sharding import PartitionSpec as P

LN_EPS = 1e-6


def layer_norm(residual, ln_gain):
    x_f32 = residual.astype(jnp.float32)
    row_mean = jnp.mean(x_f32, axis=-1, keepdims=True)
    centred = x_f32 - row_mean
    row_var = jnp.mean(centred * centred, axis=-1, keepdims=True)
    return (centred * lax.rsqrt(row_var + LN_EPS) * ln_gain).astype(jnp.bfloat16)


def rotary(features, positions):
    half_dim = features.shape[-1] // 2
    inv_freq = 10000.0 ** (-jnp.arange(half_dim, dtype=jnp.float32) / half_dim)
    angles = positions[..., None].astype(jnp.float32) * inv_freq
    cos_t = jnp.cos(angles)
    sin_t = jnp.sin(angles)
    lo_half = features[..., :half_dim]
    hi_half = features[..., half_dim:]
    return jnp.concatenate([lo_half * cos_t - hi_half * sin_t, lo_half * sin_t + hi_half * cos_t], axis=-1)


def solution(mesh):
    def device_fn(tokens, lengths, embedding, ln_scale, w_q, w_kv, w_o, w_gate, w_up, w_down, final_scale, k_cache, v_cache):
        me = lax.axis_index('tp')
        steps, batch = tokens.shape
        vocab_local, dim = embedding.shape
        layers, seqs, seq_len, head_dim = k_cache.shape
        step_ids = jnp.arange(steps, dtype=jnp.int32)[:, None]
        positions = lengths[None, :] + step_ids
        local_pos = lax.dynamic_slice_in_dim(positions, me * seqs, seqs, axis=1)
        row_ids = lax.broadcasted_iota(jnp.int32, (1, seq_len, 1), 1)

        def write(cache, new):
            for t in range(steps):
                cache = jnp.where(row_ids == local_pos[t][:, None, None], new[t][:, None, :], cache)
            return cache

        tok = tokens - me * vocab_local
        mine = (tok >= 0) & (tok < vocab_local)
        rows = jnp.take(embedding, jnp.clip(tok, 0, vocab_local - 1), axis=0)
        rows = jnp.where(mine[..., None], rows, jnp.zeros_like(rows))
        x = lax.psum_scatter(rows, 'tp', scatter_dimension=1, tiled=True)
        k_out, v_out = [], []
        for l in range(layers):
            h = layer_norm(x, ln_scale[l])
            full = lax.all_gather(h, 'tp', axis=1, tiled=True)
            q = jnp.einsum('tbd,dhc->tbhc', full, w_q[l], preferred_element_type=jnp.float32)
            q = rotary(q, positions[..., None]).astype(jnp.bfloat16)
            kv = jnp.einsum('tbd,dc->tbc', h, w_kv[l], preferred_element_type=jnp.float32)
            k_out.append(write(k_cache[l], rotary(kv[..., :head_dim], local_pos).astype(jnp.bfloat16)))
            v_out.append(write(v_cache[l], kv[..., head_dim:].astype(jnp.bfloat16)))
            q = lax.all_to_all(q, 'tp', 1, 2, tiled=True)
            s = jnp.einsum('tbhc,bsc->bths', q, k_out[l], preferred_element_type=jnp.float32) * head_dim ** -0.5
            seen = row_ids.reshape(1, 1, 1, seq_len) <= local_pos.T[:, :, None, None]
            w = jax.nn.softmax(jnp.where(seen, s, -jnp.inf), axis=-1).astype(jnp.bfloat16)
            o = jnp.einsum('bths,bsc->tbhc', w, v_out[l], preferred_element_type=jnp.float32).astype(jnp.bfloat16)
            o = lax.all_to_all(o, 'tp', 2, 1, tiled=True)
            gate = jnp.einsum('tbd,df->tbf', full, w_gate[l], preferred_element_type=jnp.float32)
            up = jnp.einsum('tbd,df->tbf', full, w_up[l], preferred_element_type=jnp.float32)
            m = (jax.nn.silu(gate) * up).astype(jnp.bfloat16)
            y = jnp.einsum('tbf,fd->tbd', m, w_down[l], preferred_element_type=jnp.float32)
            y = y + jnp.einsum('tbhc,hcd->tbd', o, w_o[l], preferred_element_type=jnp.float32)
            y = lax.psum_scatter(y, 'tp', scatter_dimension=1, tiled=True)
            x = (x.astype(jnp.float32) + y).astype(jnp.bfloat16)
        h = layer_norm(x, final_scale)
        full = lax.all_gather(h, 'tp', axis=1, tiled=True)
        logits = jnp.einsum('tbd,vd->tbv', full, embedding, preferred_element_type=jnp.float32) * dim ** -0.5
        return logits, jnp.stack(k_out), jnp.stack(v_out)

    cache_spec = P(None, 'tp', None, None)
    in_specs = (P(), P(), P('tp', None), P(), P(None, None, 'tp', None), P(), P(None, 'tp', None, None), P(None, None, 'tp'), P(None, None, 'tp'), P(None, 'tp', None), P(), cache_spec, cache_spec)
    out_specs = (P(None, None, 'tp'), cache_spec, cache_spec)
    return jax.shard_map(device_fn, mesh=mesh, in_specs=in_specs, out_specs=out_specs, check_vma=False)
```

```python
import functools

import jax
import jax.numpy as jnp
from jax import lax
from jax.experimental import pallas as pl
from jax.experimental.pallas import tpu as pltpu
from jax.sharding import PartitionSpec as P

LN_EPS = 1e-6
MESH = pl.DeviceIdType.MESH
BF16, F32 = jnp.bfloat16, jnp.float32
ANY = pl.BlockSpec(memory_space=pl.ANY)
VMEM = pl.BlockSpec(memory_space=pltpu.VMEM)
SMEM = pl.BlockSpec(memory_space=pltpu.SMEM)
DMA = pltpu.SemaphoreType.DMA
FLIPS = [(a, b, e) for a in range(2) for b in range(2) for e in range(2)]
ROUND = (3, 2, 1, 0)
HALF, BLOCK, ROWS, LANES = 32, 64, 256, 128


class Here:
    def __init__(self):
        me = lax.axis_index("tp")
        self.c = lax.rem(me, 2)
        self.x = lax.rem(lax.div(me, 2), 2)
        self.y = lax.rem(lax.div(me, 4), 2)
        z = lax.div(me, 8)
        self.zs = [z, z + 1 - 2 * lax.rem(z, 2), lax.rem(z + 2, 4), 3 - z]
        self.z = z
        self.slot = ((z * 2 + self.c) * 2 + self.y) * 2 + self.x

    def flip(self, v, on):
        return 1 - v if on else v

    def dev(self, j=0, a=0, b=0, e=0):
        y, x, c = self.flip(self.y, b), self.flip(self.x, e), self.flip(self.c, a)
        return ((self.zs[j] * 2 + y) * 2 + x) * 2 + c

    def lines(self):
        return [self.dev(j) for j in (1, 2, 3)] + [self.dev(a=1), self.dev(b=1), self.dev(e=1)]

    def all(self):
        return [self.dev(j, a, b, e) for j in range(4) for a, b, e in FLIPS if j or a or b or e]


def meet(devices):
    sem = pltpu.get_barrier_semaphore()
    for d in devices:
        pl.semaphore_signal(sem, inc=1, device_id={"tp": d}, device_id_type=MESH)
    pl.semaphore_wait(sem, len(devices))


def remote(src, dst, send, recv, k, device):
    return pltpu.make_async_remote_copy(
        src_ref=src, dst_ref=dst, send_sem=send.at[k], recv_sem=recv.at[k], device_id={"tp": device}, device_id_type=MESH
    )


def nt(a, b):
    return lax.dot_general(a, b, (((1,), (1,)), ((), ())), preferred_element_type=F32)


def nn(a, b):
    return lax.dot_general(a, b, (((1,), (0,)), ((), ())), preferred_element_type=F32)


class Gather:
    COPIES = 3 + 4 * 8

    def __init__(self, here, own, block, send, recv):
        self.here, self.own, self.block = here, own, block
        self.sems = send, recv
        self.started = []

    def copy(self, k, src, dst, device):
        return remote(src, dst, *self.sems, k, device)

    def start(self, copy):
        copy.start()
        self.started.append(copy)

    def at(self, j, a=0, b=0, e=0):
        h = self.here
        return self.block(h.zs[j], h.flip(h.c, a), h.flip(h.y, b), h.flip(h.x, e))

    def along_z(self, j):
        return self.copy(j - 1, self.own, self.at(0), self.here.dev(j))

    def source(self, j):
        return self.own if j == 0 else self.at(j)

    def step(self, j, what):
        h, k = self.here, 3 + 8 * j
        if what == "x":
            return self.copy(k, self.source(j), self.at(j), h.dev(e=1))
        if what == "y":
            return self.copy(k + 1, self.source(j), self.at(j), h.dev(b=1))
        if what == "xy":
            return self.copy(k + 2, self.at(j, e=1).at[0], self.at(j, e=1).at[0], h.dev(b=1))
        if what == "yx":
            return self.copy(k + 3, self.at(j, b=1).at[1], self.at(j, b=1).at[1], h.dev(e=1))
        if what == "c":
            return self.copy(k + 4, self.source(j), self.at(j), h.dev(a=1))
        b, e = {"cx": (0, 1), "cy": (1, 0), "cd": (1, 1)}[what]
        k += {"cx": 5, "cy": 6, "cd": 7}[what]
        return self.copy(k, self.at(j, b=b, e=e), self.at(j, b=b, e=e), h.dev(a=1))

    def open(self):
        for j in (1, 3, 2):
            self.start(self.along_z(j))
        self.share(0)

    def share(self, j):
        if j:
            self.along_z(j).wait_recv()
        for what in ("x", "y", "c"):
            self.start(self.step(j, what))

    def turn(self, j):
        self.step(j, "x").wait_recv()
        self.start(self.step(j, "xy"))
        self.start(self.step(j, "cx"))
        self.step(j, "y").wait_recv()
        self.start(self.step(j, "yx"))
        self.start(self.step(j, "cy"))

    def close(self, j):
        self.step(j, "xy").wait_recv()
        self.step(j, "yx").wait_recv()
        self.start(self.step(j, "cd"))

    def whole(self, j):
        for what in ("c", "cx", "cy", "cd"):
            self.step(j, what).wait_recv()

    def drain(self):
        for copy in self.started:
            copy.wait_send()

    def run(self, meanwhile, use):
        order = (0, 1, 3, 2)
        self.open()
        meanwhile()
        self.share(1)
        self.turn(0)
        self.share(3)
        self.close(0)
        self.turn(1)
        self.share(2)
        self.close(1)
        self.whole(0)
        use(0)
        self.turn(3)
        self.close(3)
        self.turn(2)
        self.whole(1)
        use(1)
        self.close(2)
        self.whole(3)
        use(3)
        self.whole(2)
        use(2)
        self.drain()


class Reduce:
    COPIES = 4 * 7 + 3

    @staticmethod
    def scratch(dim, dtype):
        return [
            pltpu.VMEM((4, 2, 4, 2, HALF, dim), dtype),
            pltpu.VMEM((4, 4, 2, HALF, dim), dtype),
            pltpu.VMEM((4, 2, HALF, dim), dtype),
            pltpu.VMEM((4, 2, HALF, dim), dtype),
            pltpu.VMEM((4, 2, HALF, dim), dtype),
            pltpu.VMEM((3, 2, HALF, dim), dtype),
            DMA((Reduce.COPIES,)),
            DMA((Reduce.COPIES,)),
        ]

    def __init__(self, here, part, core_in, diag_in, x_in, y_in, z_in, send, recv):
        self.here = here
        self.part, self.core_in, self.diag_in, self.x_in, self.y_in, self.z_in = part, core_in, diag_in, x_in, y_in, z_in
        self.sems = send, recv
        self.started = []

    def quad(self, b, e):
        h = self.here
        return h.flip(h.y, b) * 2 + h.flip(h.x, e)

    def step(self, j, what):
        h, k, part = self.here, 7 * j, self.part
        if what == "c":
            args = k, part.at[j, 1 - h.c], self.core_in.at[j], h.dev(a=1)
        elif what == "dy":
            args = k + 1, part.at[j, h.c, self.quad(1, 1), 0], self.diag_in.at[j, 0], h.dev(b=1)
        elif what == "dx":
            args = k + 2, part.at[j, h.c, self.quad(1, 1), 1], self.diag_in.at[j, 1], h.dev(e=1)
        elif what in ("x0", "x1"):
            t = int(what[1])
            args = k + 3 + t, part.at[j, h.c, self.quad(0, 1), t], self.x_in.at[j, t], h.dev(e=1)
        elif what in ("y0", "y1"):
            t = int(what[1])
            args = k + 5 + t, part.at[j, h.c, self.quad(1, 0), t], self.y_in.at[j, t], h.dev(b=1)
        else:
            args = 28 + j - 1, part.at[j, h.c, self.quad(0, 0)], self.z_in.at[j - 1], h.dev(j)
        k, src, dst, device = args
        return remote(src, dst, *self.sems, k, device)

    def start(self, copy):
        copy.start()
        self.started.append(copy)

    def first(self, j, fill):
        c = self.here.c
        fill(j, 1 - c)
        self.start(self.step(j, "c"))
        fill(j, c)

    def second(self, j):
        part, core_in, c = self.part, self.core_in, self.here.c
        self.step(j, "c").wait_recv()

        def add(q):
            for t in range(2):
                part[j, c, q, t] = part[j, c, q, t] + core_in[j, q, t]

        add(self.quad(1, 1))
        self.start(self.step(j, "dy"))
        self.start(self.step(j, "dx"))
        add(self.quad(0, 1))
        self.start(self.step(j, "x1"))
        add(self.quad(1, 0))
        self.start(self.step(j, "y0"))
        add(self.quad(0, 0))

    def third(self, j):
        part, c = self.part, self.here.c
        self.step(j, "dy").wait_recv()
        q = self.quad(0, 1)
        part[j, c, q, 0] = part[j, c, q, 0] + self.diag_in[j, 0]
        self.start(self.step(j, "x0"))
        self.step(j, "dx").wait_recv()
        q = self.quad(1, 0)
        part[j, c, q, 1] = part[j, c, q, 1] + self.diag_in[j, 1]
        self.start(self.step(j, "y1"))

    def fourth(self, j):
        part, c, q = self.part, self.here.c, self.quad(0, 0)
        for what in ("x1", "y0", "x0", "y1"):
            self.step(j, what).wait_recv()
        if j:
            for t in range(2):
                part[j, c, q, t] = part[j, c, q, t] + (self.x_in[j, t] + self.y_in[j, t])
            self.start(self.step(j, "z"))

    def run(self, fill, finish):
        a, b, d, e = ROUND
        self.first(a, fill)
        self.second(a)
        self.first(b, fill)
        self.second(b)
        self.third(a)
        self.first(d, fill)
        self.second(d)
        self.third(b)
        self.fourth(a)
        self.first(e, fill)
        self.second(e)
        self.third(d)
        self.fourth(b)
        self.third(e)
        self.fourth(d)
        self.fourth(e)
        for j in (1, 2, 3):
            self.step(j, "z").wait_recv()
        part, c, q = self.part, self.here.c, self.quad(0, 0)
        for t in range(2):
            for lo in range(0, HALF, 16):
                s = pl.ds(lo, 16)
                rows = part[0, c, q, t, s] + (self.x_in[0, t, s] + self.y_in[0, t, s])
                rows = rows + (self.z_in[0, t, s] + self.z_in[1, t, s] + self.z_in[2, t, s])
                finish(t, lo, rows)
        for copy in self.started:
            copy.wait_send()


def normed(x, gain):
    rows = x.astype(F32)
    centred = rows - jnp.mean(rows, axis=-1, keepdims=True)
    var = jnp.mean(centred * centred, axis=-1, keepdims=True)
    return (centred * lax.rsqrt(var + LN_EPS) * gain).astype(BF16)


def load(pairs, sems):
    copies = [pltpu.make_async_copy(src, dst, sems.at[i]) for i, (src, dst) in enumerate(pairs)]
    for copy in copies:
        copy.start()
    return copies


def embed_kernel(tok_ref, emb_hbm, gain_ref, x_ref, h_ref, emb, tail, sem, *rs):
    here = Here()
    vocab, dim = emb_hbm.shape
    whole = vocab // ROWS * ROWS
    rest = vocab - whole
    (fetch,) = load([(emb_hbm, emb)], sem)
    meet(here.lines())
    fetch.wait()
    tail[...] = jnp.zeros_like(tail)
    tail[0:rest] = emb[whole:vocab]
    red = Reduce(here, *rs)
    base = lax.axis_index("tp") * vocab

    def fill(j, core):
        tok = tok_ref[here.zs[j] * 2 + core] - base
        hot = (tok == lax.broadcasted_iota(jnp.int32, (ROWS, whole), 1)).astype(F32).astype(BF16)
        hot_tail = (tok == lax.broadcasted_iota(jnp.int32, (ROWS, LANES), 1) + whole).astype(F32).astype(BF16)

        def columns(n, carry):
            cols = pl.ds(pl.multiple_of(n * ROWS, ROWS), ROWS)
            rows = nn(hot, emb[0:whole, cols]) + nn(hot_tail, tail[:, cols])
            red.part[j, core, :, :, :, cols] = rows.astype(BF16).reshape(4, 2, HALF, ROWS)
            return carry

        lax.fori_loop(0, dim // ROWS, columns, 0)

    def finish(t, lo, rows):
        x_ref[t, lo : lo + 16] = rows
        h_ref[t, lo : lo + 16] = normed(rows, gain_ref[...])

    red.run(fill, finish)


def in_kernel(layer, h_ref, cos_ref, sin_ref, cos_own, sin_own, wg_hbm, wu_hbm, wq_hbm, wkv_hbm, m_ref, q_ref, kv_ref,
              every, wg, wu, wq, wkv, q_out, sem, send, recv, q_send, q_recv):
    here = Here()
    dim = h_ref.shape[-1]
    half = cos_ref.shape[1]
    width = 2 * half
    fetch = load([(wkv_hbm.at[layer], wkv), (wg_hbm.at[layer], wg), (wu_hbm.at[layer], wu), (wq_hbm.at[layer], wq.at[0:width])], sem)
    meet(here.all())
    gather = Gather(here, h_ref, lambda z, c, y, x: every.at[z, c, y, x], send, recv)

    def turned(rows, cos, sin):
        lo, hi = rows[0:half], rows[half:width]
        return lo * cos - hi * sin, lo * sin + hi * cos

    def meanwhile():
        every[here.z, here.c, here.y, here.x] = h_ref[...]
        wq[width:LANES] = jnp.zeros((LANES - width, dim), BF16)
        fetch[0].wait()
        kv = nt(wkv[...], h_ref[...].reshape(BLOCK, dim))
        blank = jnp.zeros((LANES - width, BLOCK), BF16)
        lo, hi = turned(kv, cos_own[...], sin_own[...])
        kv_ref[...] = jnp.concatenate([jnp.concatenate([lo, hi], 0).astype(BF16), blank, kv[width:].astype(BF16), blank], 0)
        for copy in fetch[1:]:
            copy.wait()

    sent = []

    def use(j):
        z = here.zs[j]

        def half_chunk(core, carry):
            rows = every[z, core].reshape(ROWS, dim)
            q = nt(wq[...], rows)
            lo, hi = turned(q, cos_ref[z * 2 + core], sin_ref[z * 2 + core])
            q = jnp.concatenate([lo, hi, jnp.zeros((LANES - width, ROWS), F32)], 0)
            q_out[z, core] = q.T.astype(BF16).reshape(4, BLOCK, LANES)
            gate = nt(rows, wg[...])
            up = nt(rows, wu[...])
            m_ref[z * 2 + core] = (gate * jax.nn.sigmoid(gate) * up).astype(BF16)
            return carry

        lax.fori_loop(0, 2, half_chunk, 0)
        for a, b, e in FLIPS:
            core, quad = here.flip(here.c, a), here.flip(here.y, b) * 2 + here.flip(here.x, e)
            r = j * 8 + a * 4 + b * 2 + e
            if r == 0:
                q_ref[here.slot] = q_out[z, core, quad]
                continue
            copy = remote(q_out.at[z, core, quad], q_ref.at[here.slot], q_send, q_recv, r, here.dev(j, a, b, e))
            copy.start()
            sent.append(copy)

    gather.run(meanwhile, use)
    for copy in sent:
        copy.wait_recv()
    for copy in sent:
        copy.wait_send()


def attend_kernel(layer, pos_ref, q_ref, kv_ref, k_hbm, v_hbm, o_ref, keys, values, q_rows, o_rows, o_out, sem, send, recv):
    here = Here()
    seqs, width, length = keys.shape
    fetch = load([(k_hbm.at[layer], keys), (v_hbm.at[layer], values)], sem)
    q_rows[...] = q_ref[...].reshape(2048, LANES).astype(F32)
    meet(here.all())
    for copy in fetch:
        copy.wait()
    row = lax.broadcasted_iota(jnp.int32, (BLOCK, length), 0)
    col = lax.broadcasted_iota(jnp.int32, (BLOCK, length), 1)
    cols = lax.broadcasted_iota(jnp.int32, (LANES, length), 1)
    blank = jnp.zeros((LANES - width, length), BF16)

    def one(s):
        pos = pos_ref[s]
        place = ((row == s) & (col == pos)) | ((row == s + HALF) & (col == pos + 1))
        new = nn(kv_ref[...], place.astype(F32).astype(BF16)).astype(BF16)
        fresh = (cols == pos) | (cols == pos + 1)
        k = jnp.where(fresh, new[0:LANES], jnp.concatenate([keys[s], blank], 0))
        v = jnp.where(fresh, new[LANES:ROWS], jnp.concatenate([values[s], blank], 0))
        q = q_rows[pl.ds(s, BLOCK, stride=HALF), :].astype(BF16)
        score = nn(q, k) * width**-0.5
        score = jnp.where(col <= pos + lax.rem(row, 2), score, -jnp.inf)
        weight = jnp.exp(score - jnp.max(score, axis=-1, keepdims=True))
        weight = (weight / jnp.sum(weight, axis=-1, keepdims=True)).astype(BF16)
        o_rows[pl.ds(s, BLOCK, stride=HALF), :] = nt(weight, v)

    def several(i, carry):
        for u in range(4):
            one(i * 4 + u)
        return carry

    lax.fori_loop(0, seqs // 4, several, 0)
    o_out[...] = o_rows[...].astype(BF16).reshape(HALF, BLOCK, LANES)
    sent = []
    for j in range(4):
        for a, b, e in FLIPS:
            r = j * 8 + a * 4 + b * 2 + e
            slot = ((here.zs[j] * 2 + here.flip(here.c, a)) * 2 + here.flip(here.y, b)) * 2 + here.flip(here.x, e)
            if r == 0:
                o_ref[slot] = o_out[slot]
                continue
            copy = remote(o_out.at[slot], o_ref.at[here.slot], send, recv, r, here.dev(j, a, b, e))
            copy.start()
            sent.append(copy)
    for copy in sent:
        copy.wait_recv()
    for copy in sent:
        copy.wait_send()


def out_kernel(layer, m_ref, o_ref, x_ref, gain_ref, wd_hbm, wo_hbm, x_out, h_out, wd, wo, sem, *rs):
    here = Here()
    dim = wd.shape[-1]
    width = wo_hbm.shape[1]
    fetch = load([(wd_hbm.at[layer], wd), (wo_hbm.at[layer], wo.at[0:width])], sem)
    wo[width:LANES] = jnp.zeros((LANES - width, dim), BF16)
    meet(here.lines())
    for copy in fetch:
        copy.wait()
    red = Reduce(here, *rs)

    def fill(j, core):
        zc = here.zs[j] * 2 + core

        def columns(n, carry):
            cols = pl.ds(pl.multiple_of(n * ROWS, ROWS), ROWS)
            rows = nn(o_ref[zc], wo[:, cols]) + nn(m_ref[zc], wd[:, cols])
            red.part[j, core, :, :, :, cols] = rows.reshape(4, 2, HALF, ROWS)
            return carry

        lax.fori_loop(0, dim // ROWS, columns, 0)

    def finish(t, lo, rows):
        x = (x_ref[t, lo : lo + 16].astype(F32) + rows).astype(BF16)
        x_out[t, lo : lo + 16] = x
        h_out[t, lo : lo + 16] = normed(x, gain_ref[...])

    red.run(fill, finish)


def head_kernel(h_ref, emb_hbm, out_hbm, every, emb, ready, sem, out_sem, send, recv):
    here = Here()
    vocab, dim = emb_hbm.shape
    whole = vocab // ROWS * ROWS
    scale = dim**-0.5
    (fetch,) = load([(emb_hbm, emb)], sem)
    meet(here.lines())
    gather = Gather(here, h_ref, lambda z, c, y, x: every.at[z, :, y, x, c], send, recv)

    def meanwhile():
        every[here.z, :, here.y, here.x, here.c] = h_ref[...]
        fetch.wait()

    stores = []

    def use(j):
        z = here.zs[j]
        slot = len(stores) % 2
        if len(stores) >= 2:
            stores[-2].wait()

        for t in range(2):
            rows = every[z, t].reshape(ROWS, dim)

            def part(lo, n):
                ready[slot, pl.ds(lo, n), t, :] = nt(emb[pl.ds(lo, n)], rows) * scale

            def tile(i, carry):
                part(pl.multiple_of(i * ROWS, ROWS), ROWS)
                return carry

            lax.fori_loop(0, whole // ROWS, tile, 0)
            part(whole, vocab - whole)
        cols = pl.ds(pl.multiple_of(z * ROWS, ROWS), ROWS)
        copy = pltpu.make_async_copy(ready.at[slot], out_hbm.at[:, :, cols], out_sem.at[slot])
        copy.start()
        stores.append(copy)

    gather.run(meanwhile, use)
    stores[-2].wait()
    stores[-1].wait()


def params(index, mib):
    return pltpu.CompilerParams(collective_id=index, has_side_effects=True, vmem_limit_bytes=mib << 20)


def solution(mesh):
    def device_fn(tokens, lengths, embedding, ln_scale, w_q, w_kv, w_o, w_gate, w_up, w_down, final_scale, k_cache, v_cache):
        me = lax.axis_index("tp")
        steps, batch = tokens.shape
        vocab, dim = embedding.shape
        layers, seqs, length, width = k_cache.shape
        hidden = w_gate.shape[-1]
        half = width // 2
        block = jax.ShapeDtypeStruct((2, HALF, dim), BF16)

        def ordered(rows):
            return rows.reshape(2, 4, 2, 2, 2, HALF).transpose(1, 4, 2, 3, 0, 5).reshape(8, ROWS)

        positions = lengths[None, :] + jnp.arange(steps, dtype=jnp.int32)[:, None]
        own_len = lax.dynamic_slice_in_dim(lengths, me * seqs, seqs)
        own_pos = own_len[None, :] + jnp.arange(steps, dtype=jnp.int32)[:, None]
        inv_freq = 10000.0 ** (-jnp.arange(half, dtype=F32) / half)
        angles = ordered(positions)[:, None, :].astype(F32) * inv_freq[None, :, None]
        own_angles = own_pos.reshape(1, BLOCK).astype(F32) * inv_freq[:, None]
        turns = jnp.cos(angles), jnp.sin(angles), jnp.cos(own_angles), jnp.sin(own_angles)
        gains = [ln_scale[l][None] for l in range(layers)] + [final_scale[None]]

        x, h = pl.pallas_call(
            embed_kernel,
            out_shape=(block, block),
            in_specs=[VMEM, ANY, VMEM],
            out_specs=(VMEM, VMEM),
            scratch_shapes=[pltpu.VMEM((vocab, dim), BF16), pltpu.VMEM((LANES, dim), BF16), DMA((1,)), *Reduce.scratch(dim, BF16)],
            compiler_params=params(0, 60),
            name="embed",
        )(ordered(tokens)[:, :, None], embedding, gains[0])

        wg_t, wu_t, wkv_t = (w.transpose(0, 2, 1) for w in (w_gate, w_up, w_kv))
        wq_t = w_q.transpose(0, 2, 3, 1).reshape(layers, width, dim)
        wo = w_o.reshape(layers, width, dim)
        k_t, v_t = k_cache.transpose(0, 1, 3, 2), v_cache.transpose(0, 1, 3, 2)
        fresh = []
        for l in range(layers):
            m, q, kv = pl.pallas_call(
                functools.partial(in_kernel, l),
                out_shape=(
                    jax.ShapeDtypeStruct((8, ROWS, hidden), BF16),
                    jax.ShapeDtypeStruct((HALF, BLOCK, LANES), BF16),
                    jax.ShapeDtypeStruct((ROWS, BLOCK), BF16),
                ),
                in_specs=[VMEM] * 5 + [ANY] * 4,
                out_specs=(VMEM, VMEM, VMEM),
                scratch_shapes=[
                    pltpu.VMEM((4, 2, 2, 2, 2, HALF, dim), BF16),
                    pltpu.VMEM((hidden, dim), BF16),
                    pltpu.VMEM((hidden, dim), BF16),
                    pltpu.VMEM((LANES, dim), BF16),
                    pltpu.VMEM((2 * width, dim), BF16),
                    pltpu.VMEM((4, 2, 4, BLOCK, LANES), BF16),
                    DMA((4,)),
                    DMA((Gather.COPIES,)),
                    DMA((Gather.COPIES,)),
                    DMA((HALF,)),
                    DMA((HALF,)),
                ],
                compiler_params=params(1 + 3 * l, 48),
                name=f"in{l}",
            )(h, *turns, wg_t, wu_t, wq_t, wkv_t)
            fresh.append(kv)
            o = pl.pallas_call(
                functools.partial(attend_kernel, l),
                out_shape=jax.ShapeDtypeStruct((HALF, BLOCK, LANES), BF16),
                in_specs=[SMEM, VMEM, VMEM, ANY, ANY],
                out_specs=VMEM,
                scratch_shapes=[
                    pltpu.VMEM((seqs, width, length), BF16),
                    pltpu.VMEM((seqs, width, length), BF16),
                    pltpu.VMEM((2048, LANES), F32),
                    pltpu.VMEM((2048, LANES), F32),
                    pltpu.VMEM((HALF, BLOCK, LANES), BF16),
                    DMA((2,)),
                    DMA((HALF,)),
                    DMA((HALF,)),
                ],
                compiler_params=params(2 + 3 * l, 40),
                name=f"attend{l}",
            )(own_len, q, kv, k_t, v_t)
            x, h = pl.pallas_call(
                functools.partial(out_kernel, l),
                out_shape=(block, block),
                in_specs=[VMEM] * 4 + [ANY] * 2,
                out_specs=(VMEM, VMEM),
                scratch_shapes=[pltpu.VMEM((hidden, dim), BF16), pltpu.VMEM((LANES, dim), BF16), DMA((2,)), *Reduce.scratch(dim, F32)],
                compiler_params=params(3 + 3 * l, 60),
                name=f"out{l}",
            )(m, o.reshape(8, ROWS, LANES), x, gains[l + 1], w_down, wo)

        logits = pl.pallas_call(
            head_kernel,
            out_shape=jax.ShapeDtypeStruct((vocab, 2, batch), F32),
            in_specs=[VMEM, ANY],
            out_specs=ANY,
            scratch_shapes=[
                pltpu.VMEM((4, 2, 2, 2, 2, HALF, dim), BF16),
                pltpu.VMEM((vocab, dim), BF16),
                pltpu.VMEM((2, vocab, 2, ROWS), F32),
                DMA((1,)),
                DMA((2,)),
                DMA((Gather.COPIES,)),
                DMA((Gather.COPIES,)),
            ],
            compiler_params=params(7, 60),
            name="head",
        )(h, embedding)

        row_ids = lax.broadcasted_iota(jnp.int32, (1, 1, length, 1), 2)
        new = jnp.stack(fresh)[:, :, None].reshape(layers, 2, LANES, 2, HALF)[:, :, :width]

        def written(cache, which):
            for t in range(steps):
                cache = jnp.where(
                    row_ids == own_pos[t][None, :, None, None], new[:, which, :, t].transpose(0, 2, 1)[:, :, None, :], cache
                )
            return cache

        return logits.transpose(1, 2, 0), written(k_cache, 0), written(v_cache, 1)

    cache_spec = P(None, "tp", None, None)
    in_specs = (P(), P(), P("tp", None), P(), P(None, None, "tp", None), P(), P(None, "tp", None, None), P(None, None, "tp"), P(None, None, "tp"), P(None, "tp", None), P(), cache_spec, cache_spec)
    out_specs = (P(None, None, "tp"), cache_spec, cache_spec)
    return jax.shard_map(device_fn, mesh=mesh, in_specs=in_specs, out_specs=out_specs, check_vma=False)
```

```python
import functools

import jax
import jax.numpy as jnp
from jax import lax
from jax.experimental import pallas as pl
from jax.experimental.pallas import tpu as pltpu
from jax.sharding import PartitionSpec as P

LN_EPS = 1e-6
MESH = pl.DeviceIdType.MESH
BF16, F32 = jnp.bfloat16, jnp.float32
ANY = pl.BlockSpec(memory_space=pl.ANY)
VMEM = pl.BlockSpec(memory_space=pltpu.VMEM)
SMEM = pl.BlockSpec(memory_space=pltpu.SMEM)
DMA = pltpu.SemaphoreType.DMA
FLIPS = [(a, b, e) for a in range(2) for b in range(2) for e in range(2)]
HALF, BLOCK, ROWS, LANES = 32, 64, 256, 128
SIDE = ROWS
ALL = (slice(None),) * 3
DIGITS = "0123456789"
REDUCE = ("fo3 fm3 fo2 ca3", "d3 fm2 fz3 fo1", "p3 q3 ca2 d2", "fz2 fm1 u3 fo0", "ca1 fz1 fm0 p2", "q2 d1 gz3 ca0", "fin u2 p1 q1", "d0 gz2 u1 gz1", "p0 q0 u0 end")
GATHER = ("zown sh0 zf1 sh1", "ty0 tx0 zf2 sh2", "zf3 ty1 cl0 fown", "tx1 um0 tx2 sh3", "uo0 us0 ff1 cl1", "ty2 ff2 um1 uo1", "us1 ff3 tx3 cl2", "ty3 um2 uo2 us2", "cl3 um3 uo3 us3")


class Here:
    def __init__(self):
        me = lax.axis_index("tp")
        self.c = lax.rem(me, 2)
        self.x = lax.rem(lax.div(me, 2), 2)
        self.y = lax.rem(lax.div(me, 4), 2)
        z = lax.div(me, 8)
        self.z = z
        inner = lax.rem(lax.div(z + 1, 2), 2)
        self.inner = inner == 1
        two, three = lax.rem(z + 2, 4), 3 - z
        self.zs = [z, z + 1 - 2 * lax.rem(z, 2), inner * three + (1 - inner) * two, inner * two + (1 - inner) * three]
        self.slot = ((z * 2 + self.c) * 2 + self.y) * 2 + self.x
        self.near, self.across = self.dev(self.zs[1]), self.dev(three)
        self.core, self.along_x, self.along_y = self.dev(z, a=1), self.dev(z, e=1), self.dev(z, b=1)

    def flip(self, v, on):
        return 1 - v if on else v

    def dev(self, z, a=0, b=0, e=0):
        y, x, c = self.flip(self.y, b), self.flip(self.x, e), self.flip(self.c, a)
        return ((z * 2 + y) * 2 + x) * 2 + c

    def apart(self, s):
        inner = lax.rem(lax.div(self.z + 1, 2), 2)
        return (0, 1, 2 + inner, 3 - inner)[s]

    def lines(self):
        return [self.near, self.dev(self.zs[2]), self.dev(self.zs[3]), self.core, self.along_x, self.along_y]

    def all(self):
        z = self.z
        zs = [z, self.zs[1], lax.rem(z + 2, 4), 3 - z]
        return [(8 * j + 4 * a + 2 * b + e, zs[j], (a, b, e)) for j in range(4) for a, b, e in FLIPS if j or a or b or e]


def meet(devices):
    sem = pltpu.get_barrier_semaphore()
    for d in devices:
        pl.semaphore_signal(sem, inc=1, device_id={"tp": d}, device_id_type=MESH)
    pl.semaphore_wait(sem, len(devices))


class Wires:
    def __init__(self, here, send, recv):
        self.here, self.send, self.recv = here, send, recv
        self.names, self.count = {}, 0
        self.started = {None: [], True: [], False: []}

    def copy(self, what, src, dst, device):
        k = self.names.setdefault(what, len(self.names))
        self.count += 1
        return pltpu.make_async_remote_copy(
            src_ref=src,
            dst_ref=dst,
            send_sem=self.send.at[self.count - 1],
            recv_sem=self.recv.at[k],
            device_id={"tp": device},
            device_id_type=MESH,
        )

    def go(self, what, src, dst, device, inner=None):
        copy = self.copy(what, src, dst, device)
        self.started[inner].append(copy)
        if inner is None:
            copy.start()
        else:
            pl.when(self.here.inner == inner)(copy.start)
        return copy

    def got(self, what, like):
        k = self.names.setdefault(what, len(self.names))
        pltpu.make_async_remote_copy(
            src_ref=like, dst_ref=like, send_sem=self.send.at[0], recv_sem=self.recv.at[k], device_id={"tp": self.here.core}, device_id_type=MESH
        ).wait_recv()

    def run(self, order):
        for word in " ".join(order).split():
            step = word.rstrip(DIGITS)
            getattr(self, step)(*(int(n) for n in word[len(step) :]))

    def drain(self):
        for copy in self.started[None]:
            copy.wait_send()
        for side in (True, False):

            @pl.when(self.here.inner == side)
            def _(copies=self.started[side]):
                for copy in copies:
                    copy.wait_send()


def nt(a, b):
    return lax.dot_general(a, b, (((1,), (1,)), ((), ())), preferred_element_type=F32)


def nn(a, b):
    return lax.dot_general(a, b, (((1,), (0,)), ((), ())), preferred_element_type=F32)


class Gather(Wires):
    COPIES = 48

    def __init__(self, here, own, plane, send, recv, use, used):
        super().__init__(here, send, recv)
        self.own, self.plane, self.use, self.used = own, plane, use, used
        dim = own.shape[-1]
        self.main, self.side, self.full = pl.ds(0, dim - SIDE), pl.ds(dim - SIDE, SIDE), pl.ds(0, dim)

    def at(self, s, b=0, e=0):
        h = self.here
        return self.plane(h.zs[s], h.c).at[h.flip(h.y, b), h.flip(h.x, e)].at[:, :, self.main if s else self.full]

    def fours(self, s):
        return self.plane(self.here.zs[s], self.here.c).at[:, :, :, :, self.side]

    def pass_on(self, what, s, ref):
        h = self.here
        self.go((what, 3 if s == 1 else s), ref, ref, h.across if s == 1 else h.near, True)

    def zown(self):
        h = self.here
        src, dst = self.own.at[:, :, self.main], self.at(0).at[:, :, self.main]
        self.go(("z", 1), src, dst, h.near)
        self.go(("z", 2), src, dst, h.across, True)

    def zf(self, s):
        self.got(("z", s), self.at(s))
        self.pass_on("z", s, self.at(s))

    def fown(self):
        h, ref = self.here, self.fours(0)
        self.go(("f", 1), ref, ref, h.near)
        self.go(("f", 2), ref, ref, h.across, True)

    def ff(self, s):
        ref = self.fours(s)
        self.got(("f", s), ref)
        self.pass_on("f", s, ref)
        self.go(("cf", s), ref, ref, self.here.core)

    def sh(self, s):
        h, dst = self.here, self.at(s)
        src = dst if s else self.own
        self.go(("x", s), src, dst, h.along_x)
        self.go(("y", s), src, dst, h.along_y)
        self.go(("c", s), src, dst, h.core)

    def tx(self, s):
        ref = self.at(s, e=1)
        self.got(("x", s), ref)
        self.go(("xy", s), ref.at[0], ref.at[0], self.here.along_y)
        self.go(("cx", s), ref, ref, self.here.core)

    def ty(self, s):
        ref = self.at(s, b=1)
        self.got(("y", s), ref)
        self.go(("yx", s), ref.at[1], ref.at[1], self.here.along_x)
        self.go(("cy", s), ref, ref, self.here.core)

    def cl(self, s):
        ref = self.at(s, 1, 1)
        self.got(("xy", s), ref.at[0])
        self.got(("yx", s), ref.at[1])
        self.go(("cd", s), ref, ref, self.here.core)

    def um(self, s):
        self.use(s, self.here.c)

    def uo(self, s):
        for what in ("c", "cx", "cy", "cd"):
            self.got((what, s), self.at(s))
        if s:
            self.got(("cf", s), self.fours(s))
        self.use(s, 1 - self.here.c)

    def us(self, s):
        self.used(s)


class Reduce(Wires):
    COPIES = 48

    @staticmethod
    def scratch(rows, dim, dtype):
        return [
            pltpu.VMEM((4, 4, 2, rows, dim), dtype),
            pltpu.VMEM((2, 4, 2, rows, dim), dtype),
            pltpu.VMEM((4, 4, 2, rows, dim), dtype),
            pltpu.VMEM((4, 2, rows, dim), dtype),
            pltpu.VMEM((4, 2, rows, dim), dtype),
            pltpu.VMEM((4, 2, rows, dim), dtype),
            pltpu.VMEM((6, 2, rows, dim - SIDE), dtype),
            pltpu.VMEM((6, 4, 2, rows, SIDE), dtype),
            DMA((Reduce.COPIES,)),
            DMA((Reduce.COPIES,)),
        ]

    def __init__(self, here, fill, finish, part, sib, core_in, diag_in, x_in, y_in, z_in, side_in, send, recv):
        super().__init__(here, send, recv)
        self.fill, self.finish = fill, finish
        self.part, self.sib, self.core_in, self.diag_in = part, sib, core_in, diag_in
        self.x_in, self.y_in, self.z_in, self.side_in = x_in, y_in, z_in, side_in
        dim = part.shape[-1]
        self.main, self.side, self.full = pl.ds(0, dim - SIDE), pl.ds(dim - SIDE, SIDE), pl.ds(0, dim)
        self.lent = []

    def quad(self, b, e):
        h = self.here
        return h.flip(h.y, b) * 2 + h.flip(h.x, e)

    def piece(self, buf, s, *where):
        return buf, (s, *where, slice(None), self.main if s else self.full)

    def add(self, ref, *more):
        buf, index = ref
        total = buf[index]
        for other, where in more:
            total = total + other[where]
        buf[index] = total

    def fo(self, s):
        n = len(self.lent)
        if n > 1:
            self.lent[n - 2].wait_send()
            self.started[None].remove(self.lent[n - 2])
        self.fill(s, 1 - self.here.c, self.sib.at[n % 2])
        self.lent.append(self.go(("c", s), self.sib.at[n % 2], self.core_in.at[s], self.here.core))

    def fm(self, s):
        self.fill(s, self.here.c, self.part.at[s])

    def ca(self, s):
        self.got(("c", s), self.core_in.at[s])
        for t in range(2):

            def add(i, carry):
                self.add((self.part, (s, i, t)), (self.core_in, (s, i, t)))
                return carry

            lax.fori_loop(0, 4, add, 0)

    def along_z(self, what, s, ref, landing):
        h = self.here
        k = 5 if s == 1 else s
        to = 1 if s == 1 else s + 2

        @pl.when(h.inner)
        def _():
            self.got((what, k), landing.at[k])
            self.add(ref, (landing, k))

        self.go((what, to), ref[0].at[ref[1]], landing.at[to], h.near if s == 1 else h.across, True)
        self.go((what, s), ref[0].at[ref[1]], landing.at[s], h.near, False)

    def last_z(self, what, ref, landing):
        self.got((what, 1), landing.at[1])
        self.add(ref, (landing, 1))

        @pl.when(self.here.inner)
        def _():
            self.got((what, 4), landing.at[4])
            self.add(ref, (landing, 4))

    def fz(self, s):
        self.along_z("f", s, (self.part, (s, *ALL, self.side)), self.side_in)

    def fin(self):
        self.last_z("f", (self.part, (0, *ALL, self.side)), self.side_in)

    def d(self, s):
        h, part = self.here, self.part
        far = self.quad(1, 1)
        self.pass_on("dy", s, self.piece(part, s, far, 0), self.piece(self.diag_in, s, 0), h.along_y)
        self.pass_on("dx", s, self.piece(part, s, far, 1), self.piece(self.diag_in, s, 1), h.along_x)
        self.pass_on("x1", s, self.piece(part, s, self.quad(0, 1), 1), self.piece(self.x_in, s, 1), h.along_x)
        self.pass_on("y0", s, self.piece(part, s, self.quad(1, 0), 0), self.piece(self.y_in, s, 0), h.along_y)

    def pass_on(self, what, s, src, dst, device):
        self.go((what, s), src[0].at[src[1]], dst[0].at[dst[1]], device)

    def came(self, what, s, ref):
        self.got((what, s), ref[0].at[ref[1]])

    def p(self, s):
        ref = self.piece(self.part, s, self.quad(0, 1), 0)
        self.came("dy", s, ref)
        self.add(ref, self.piece(self.diag_in, s, 0))
        self.pass_on("x0", s, ref, self.piece(self.x_in, s, 0), self.here.along_x)

    def q(self, s):
        ref = self.piece(self.part, s, self.quad(1, 0), 1)
        self.came("dx", s, ref)
        self.add(ref, self.piece(self.diag_in, s, 1))
        self.pass_on("y1", s, ref, self.piece(self.y_in, s, 1), self.here.along_y)

    def u(self, s):
        for t in range(2):
            ref = self.piece(self.part, s, self.quad(0, 0), t)
            self.came(f"x{t}", s, ref)
            self.came(f"y{t}", s, ref)
            self.add(ref, self.piece(self.x_in, s, t), self.piece(self.y_in, s, t))

    def gz(self, s):
        self.along_z("g", s, (self.part, (s, self.quad(0, 0), *ALL[:2], self.main)), self.z_in)

    def end(self):
        mine = self.quad(0, 0)
        self.last_z("g", (self.part, (0, mine, *ALL[:2], self.main)), self.z_in)
        for t in range(2):
            for lo in range(0, self.part.shape[3], 16):
                self.finish(t, lo, self.part[0, mine, t, lo : lo + 16])


def normed(x, gain):
    rows = x.astype(F32)
    centred = rows - jnp.mean(rows, axis=-1, keepdims=True)
    var = jnp.mean(centred * centred, axis=-1, keepdims=True)
    return (centred * lax.rsqrt(var + LN_EPS) * gain).astype(BF16)


def load(pairs, sems):
    copies = [pltpu.make_async_copy(src, dst, sems.at[i]) for i, (src, dst) in enumerate(pairs)]
    for copy in copies:
        copy.start()
    return copies


def embed_kernel(tok_ref, emb_hbm, gain_ref, x_ref, h_ref, emb, tail, sem, *rs):
    here = Here()
    vocab, dim = emb_hbm.shape
    whole = vocab // ROWS * ROWS
    rest = vocab - whole
    (fetch,) = load([(emb_hbm, emb)], sem)
    meet(here.lines())
    fetch.wait()
    tail[...] = jnp.zeros_like(tail)
    tail[0:rest] = emb[whole:vocab]
    base = lax.axis_index("tp") * vocab

    def fill(s, core, ref):
        tok = tok_ref[here.zs[s] * 2 + core] - base
        hot = (tok == lax.broadcasted_iota(jnp.int32, (ROWS, whole), 1)).astype(F32).astype(BF16)
        hot_tail = (tok == lax.broadcasted_iota(jnp.int32, (ROWS, LANES), 1) + whole).astype(F32).astype(BF16)

        def columns(n, carry):
            cols = pl.ds(pl.multiple_of(n * ROWS, ROWS), ROWS)
            rows = nn(hot, emb[0:whole, cols]) + nn(hot_tail, tail[:, cols])
            ref[:, :, :, cols] = rows.astype(BF16).reshape(4, 2, HALF, ROWS)
            return carry

        lax.fori_loop(0, dim // ROWS, columns, 0)

    def finish(t, lo, rows):
        x_ref[t, lo : lo + 16] = rows
        h_ref[t, lo : lo + 16] = normed(rows, gain_ref[...])

    red = Reduce(here, fill, finish, *rs)
    red.run(REDUCE)
    red.drain()


def in_kernel(layer, h_ref, cos_ref, sin_ref, cos_own, sin_own, wg_hbm, wu_hbm, wq_hbm, wkv_hbm, m_ref, q_ref, kv_ref,
              every, wg, wu, wq, wkv, q_out, sem, send, recv, q_send, q_recv):
    here = Here()
    dim = h_ref.shape[-1]
    half = cos_ref.shape[1]
    width = 2 * half
    fetch = load([(wkv_hbm.at[layer], wkv), (wg_hbm.at[layer], wg), (wu_hbm.at[layer], wu), (wq_hbm.at[layer], wq.at[0:width])], sem)
    meet([here.dev(z, *f) for _, z, f in here.all()])
    def turned(rows, cos, sin):
        lo, hi = rows[0:half], rows[half:width]
        return lo * cos - hi * sin, lo * sin + hi * cos

    every[here.z, here.c, here.y, here.x] = h_ref[...]
    sent = []

    def use(s, core):
        z = here.zs[s]
        rows = every[z, core].reshape(ROWS, dim)
        q = nt(wq[...], rows)
        lo, hi = turned(q, cos_ref[z * 2 + core], sin_ref[z * 2 + core])
        q = jnp.concatenate([lo, hi, jnp.zeros((LANES - width, ROWS), F32)], 0)
        q_out[z, core] = q.T.astype(BF16).reshape(4, BLOCK, LANES)
        gate = nt(rows, wg[...])
        up = nt(rows, wu[...])
        m_ref[z * 2 + core] = (gate * jax.nn.sigmoid(gate) * up).astype(BF16)

    def used(s):
        z = here.zs[s]
        for a, b, e in FLIPS:
            core, quad = here.flip(here.c, a), here.flip(here.y, b) * 2 + here.flip(here.x, e)
            if s == a == b == e == 0:
                q_ref[here.slot] = q_out[z, core, quad]
                continue
            j = 0 if s == 0 else here.apart(s)
            r = j * 8 + (a * 4 + b * 2 + e)
            copy = pltpu.make_async_remote_copy(
                q_out.at[z, core, quad], q_ref.at[here.slot], q_send.at[r], q_recv.at[r], device_id={"tp": here.dev(z, a, b, e)}, device_id_type=MESH
            )
            copy.start()
            sent.append(copy)

    gather = Gather(here, h_ref, lambda z, c: every.at[z, c], send, recv, use, used)

    def kv():
        fetch[0].wait()
        rows = nt(wkv[...], h_ref[...].reshape(BLOCK, dim))
        blank = jnp.zeros((LANES - width, BLOCK), BF16)
        lo, hi = turned(rows, cos_own[...], sin_own[...])
        kv_ref[...] = jnp.concatenate([jnp.concatenate([lo, hi], 0).astype(BF16), blank, rows[width:].astype(BF16), blank], 0)
        wq[width:LANES] = jnp.zeros((LANES - width, dim), BF16)
        for copy in fetch[1:]:
            copy.wait()

    gather.run(GATHER[:1])
    kv()
    gather.run(GATHER[1:])
    gather.drain()
    for copy in sent:
        copy.wait_recv()
    for copy in sent:
        copy.wait_send()


def attend_kernel(layer, pos_ref, q_ref, kv_ref, k_hbm, v_hbm, o_ref, keys, values, q_rows, o_rows, o_out, sem, send, recv):
    here = Here()
    seqs, width, length = keys.shape
    fetch = load([(k_hbm.at[layer], keys), (v_hbm.at[layer], values)], sem)
    q_rows[...] = q_ref[...].reshape(2048, LANES).astype(F32)
    meet([here.dev(z, *f) for _, z, f in here.all()])
    for copy in fetch:
        copy.wait()
    row = lax.broadcasted_iota(jnp.int32, (BLOCK, length), 0)
    col = lax.broadcasted_iota(jnp.int32, (BLOCK, length), 1)
    cols = lax.broadcasted_iota(jnp.int32, (LANES, length), 1)
    blank = jnp.zeros((LANES - width, length), BF16)

    def one(s):
        pos = pos_ref[s]
        place = ((row == s) & (col == pos)) | ((row == s + HALF) & (col == pos + 1))
        new = nn(kv_ref[...], place.astype(F32).astype(BF16)).astype(BF16)
        fresh = (cols == pos) | (cols == pos + 1)
        k = jnp.where(fresh, new[0:LANES], jnp.concatenate([keys[s], blank], 0))
        v = jnp.where(fresh, new[LANES:ROWS], jnp.concatenate([values[s], blank], 0))
        q = q_rows[pl.ds(s, BLOCK, stride=HALF), :].astype(BF16)
        score = nn(q, k) * width**-0.5
        score = jnp.where(col <= pos + lax.rem(row, 2), score, -jnp.inf)
        weight = jnp.exp(score - jnp.max(score, axis=-1, keepdims=True))
        weight = (weight / jnp.sum(weight, axis=-1, keepdims=True)).astype(BF16)
        o_rows[pl.ds(s, BLOCK, stride=HALF), :] = nt(weight, v)

    def several(i, carry):
        for u in range(4):
            one(i * 4 + u)
        return carry

    lax.fori_loop(0, seqs // 4, several, 0)
    o_out[...] = o_rows[...].astype(BF16).reshape(HALF, BLOCK, LANES)
    o_ref[here.slot] = o_out[here.slot]
    sent = []
    for r, z, (a, b, e) in here.all():
        slot = ((z * 2 + here.flip(here.c, a)) * 2 + here.flip(here.y, b)) * 2 + here.flip(here.x, e)
        copy = pltpu.make_async_remote_copy(
            o_out.at[slot], o_ref.at[here.slot], send.at[r], recv.at[r], device_id={"tp": here.dev(z, a, b, e)}, device_id_type=MESH
        )
        copy.start()
        sent.append(copy)
    for copy in sent:
        copy.wait_recv()
    for copy in sent:
        copy.wait_send()


def out_kernel(layer, m_ref, o_ref, x_ref, gain_ref, wd_hbm, wo_hbm, x_out, h_out, wd, wo, sem, *rs):
    here = Here()
    dim = wd.shape[-1]
    width = wo_hbm.shape[1]
    fetch = load([(wd_hbm.at[layer], wd), (wo_hbm.at[layer], wo.at[0:width])], sem)
    wo[width:LANES] = jnp.zeros((LANES - width, dim), BF16)
    meet(here.lines())
    for copy in fetch:
        copy.wait()

    def fill(s, core, ref):
        zc = here.zs[s] * 2 + core

        def columns(n, carry):
            cols = pl.ds(pl.multiple_of(n * ROWS, ROWS), ROWS)
            rows = nn(o_ref[zc], wo[:, cols]) + nn(m_ref[zc], wd[:, cols])
            ref[:, :, :, cols] = rows.reshape(4, 2, HALF, ROWS)
            return carry

        lax.fori_loop(0, dim // ROWS, columns, 0)

    def finish(t, lo, rows):
        x = (x_ref[t, lo : lo + 16].astype(F32) + rows).astype(BF16)
        x_out[t, lo : lo + 16] = x
        h_out[t, lo : lo + 16] = normed(x, gain_ref[...])

    red = Reduce(here, fill, finish, *rs)
    red.run(REDUCE)
    red.drain()


def head_kernel(h_ref, emb_hbm, out_hbm, every, rows, emb, ready, sem, out_sem, send, recv):
    here = Here()
    vocab, dim = emb_hbm.shape
    whole = vocab // ROWS * ROWS
    scale = dim**-0.5
    (fetch,) = load([(emb_hbm, emb)], sem)
    meet(here.lines())
    every[here.z, here.c, here.y, here.x] = h_ref[...]
    stores = []

    def used(s):
        z = here.zs[s]
        slot = len(stores) % 2
        if len(stores) >= 2:
            stores[-2].wait()
        for t in range(2):
            for c in range(2):
                for y in range(2):
                    for x in range(2):
                        rows[pl.ds(((y * 2 + x) * 2 + c) * HALF, HALF)] = every[z, c, y, x, t]

            def part(lo, n):
                ready[slot, pl.ds(lo, n), t, :] = nt(emb[pl.ds(lo, n)], rows[...]) * scale

            def tile(i, carry):
                part(pl.multiple_of(i * ROWS, ROWS), ROWS)
                return carry

            lax.fori_loop(0, whole // ROWS, tile, 0)
            part(whole, vocab - whole)
        cols = pl.ds(pl.multiple_of(z * ROWS, ROWS), ROWS)
        copy = pltpu.make_async_copy(ready.at[slot], out_hbm.at[:, :, cols], out_sem.at[slot])
        copy.start()
        stores.append(copy)

    gather = Gather(here, h_ref, lambda z, c: every.at[z, c], send, recv, lambda s, core: None, used)
    gather.run(GATHER[:1])
    fetch.wait()
    gather.run(GATHER[1:])
    gather.drain()
    stores[-2].wait()
    stores[-1].wait()


def params(index, mib):
    return pltpu.CompilerParams(collective_id=index, has_side_effects=True, vmem_limit_bytes=mib << 20)


def solution(mesh):
    def device_fn(tokens, lengths, embedding, ln_scale, w_q, w_kv, w_o, w_gate, w_up, w_down, final_scale, k_cache, v_cache):
        me = lax.axis_index("tp")
        steps, batch = tokens.shape
        vocab, dim = embedding.shape
        layers, seqs, length, width = k_cache.shape
        hidden = w_gate.shape[-1]
        half = width // 2
        block = jax.ShapeDtypeStruct((2, HALF, dim), BF16)

        def ordered(rows):
            return rows.reshape(2, 4, 2, 2, 2, HALF).transpose(1, 4, 2, 3, 0, 5).reshape(8, ROWS)

        positions = lengths[None, :] + jnp.arange(steps, dtype=jnp.int32)[:, None]
        own_len = lax.dynamic_slice_in_dim(lengths, me * seqs, seqs)
        own_pos = own_len[None, :] + jnp.arange(steps, dtype=jnp.int32)[:, None]
        inv_freq = 10000.0 ** (-jnp.arange(half, dtype=F32) / half)
        angles = ordered(positions)[:, None, :].astype(F32) * inv_freq[None, :, None]
        own_angles = own_pos.reshape(1, BLOCK).astype(F32) * inv_freq[:, None]
        turns = jnp.cos(angles), jnp.sin(angles), jnp.cos(own_angles), jnp.sin(own_angles)
        gains = [ln_scale[l][None] for l in range(layers)] + [final_scale[None]]

        x, h = pl.pallas_call(
            embed_kernel,
            out_shape=(block, block),
            in_specs=[VMEM, ANY, VMEM],
            out_specs=(VMEM, VMEM),
            scratch_shapes=[pltpu.VMEM((vocab, dim), BF16), pltpu.VMEM((LANES, dim), BF16), DMA((1,)), *Reduce.scratch(HALF, dim, BF16)],
            compiler_params=params(0, 60),
            name="embed",
        )(ordered(tokens)[:, :, None], embedding, gains[0])

        wg_t, wu_t, wkv_t = (w.transpose(0, 2, 1) for w in (w_gate, w_up, w_kv))
        wq_t = w_q.transpose(0, 2, 3, 1).reshape(layers, width, dim)
        wo = w_o.reshape(layers, width, dim)
        k_t, v_t = k_cache.transpose(0, 1, 3, 2), v_cache.transpose(0, 1, 3, 2)
        fresh = []
        for l in range(layers):
            m, q, kv = pl.pallas_call(
                functools.partial(in_kernel, l),
                out_shape=(
                    jax.ShapeDtypeStruct((8, ROWS, hidden), BF16),
                    jax.ShapeDtypeStruct((HALF, BLOCK, LANES), BF16),
                    jax.ShapeDtypeStruct((ROWS, BLOCK), BF16),
                ),
                in_specs=[VMEM] * 5 + [ANY] * 4,
                out_specs=(VMEM, VMEM, VMEM),
                scratch_shapes=[
                    pltpu.VMEM((4, 2, 2, 2, 2, HALF, dim), BF16),
                    pltpu.VMEM((hidden, dim), BF16),
                    pltpu.VMEM((hidden, dim), BF16),
                    pltpu.VMEM((LANES, dim), BF16),
                    pltpu.VMEM((2 * width, dim), BF16),
                    pltpu.VMEM((4, 2, 4, BLOCK, LANES), BF16),
                    DMA((4,)),
                    DMA((Gather.COPIES,)),
                    DMA((Gather.COPIES,)),
                    DMA((HALF,)),
                    DMA((HALF,)),
                ],
                compiler_params=params(1 + 3 * l, 48),
                name=f"in{l}",
            )(h, *turns, wg_t, wu_t, wq_t, wkv_t)
            fresh.append(kv)
            o = pl.pallas_call(
                functools.partial(attend_kernel, l),
                out_shape=jax.ShapeDtypeStruct((HALF, BLOCK, LANES), BF16),
                in_specs=[SMEM, VMEM, VMEM, ANY, ANY],
                out_specs=VMEM,
                scratch_shapes=[
                    pltpu.VMEM((seqs, width, length), BF16),
                    pltpu.VMEM((seqs, width, length), BF16),
                    pltpu.VMEM((2048, LANES), F32),
                    pltpu.VMEM((2048, LANES), F32),
                    pltpu.VMEM((HALF, BLOCK, LANES), BF16),
                    DMA((2,)),
                    DMA((HALF,)),
                    DMA((HALF,)),
                ],
                compiler_params=params(2 + 3 * l, 40),
                name=f"attend{l}",
            )(own_len, q, kv, k_t, v_t)
            x, h = pl.pallas_call(
                functools.partial(out_kernel, l),
                out_shape=(block, block),
                in_specs=[VMEM] * 4 + [ANY] * 2,
                out_specs=(VMEM, VMEM),
                scratch_shapes=[pltpu.VMEM((hidden, dim), BF16), pltpu.VMEM((LANES, dim), BF16), DMA((2,)), *Reduce.scratch(HALF, dim, F32)],
                compiler_params=params(3 + 3 * l, 60),
                name=f"out{l}",
            )(m, o.reshape(8, ROWS, LANES), x, gains[l + 1], w_down, wo)

        logits = pl.pallas_call(
            head_kernel,
            out_shape=jax.ShapeDtypeStruct((vocab, 2, batch), F32),
            in_specs=[VMEM, ANY],
            out_specs=ANY,
            scratch_shapes=[
                pltpu.VMEM((4, 2, 2, 2, 2, HALF, dim), BF16),
                pltpu.VMEM((ROWS, dim), BF16),
                pltpu.VMEM((vocab, dim), BF16),
                pltpu.VMEM((2, vocab, 2, ROWS), F32),
                DMA((1,)),
                DMA((2,)),
                DMA((Gather.COPIES,)),
                DMA((Gather.COPIES,)),
            ],
            compiler_params=params(7, 60),
            name="head",
        )(h, embedding)

        row_ids = lax.broadcasted_iota(jnp.int32, (1, 1, length, 1), 2)
        new = jnp.stack(fresh)[:, :, None].reshape(layers, 2, LANES, 2, HALF)[:, :, :width]

        def written(cache, which):
            for t in range(steps):
                cache = jnp.where(
                    row_ids == own_pos[t][None, :, None, None], new[:, which, :, t].transpose(0, 2, 1)[:, :, None, :], cache
                )
            return cache

        return logits.transpose(1, 2, 0), written(k_cache, 0), written(v_cache, 1)

    cache_spec = P(None, "tp", None, None)
    in_specs = (P(), P(), P("tp", None), P(), P(None, None, "tp", None), P(), P(None, "tp", None, None), P(None, None, "tp"), P(None, None, "tp"), P(None, "tp", None), P(), cache_spec, cache_spec)
    out_specs = (P(None, None, "tp"), cache_spec, cache_spec)
    return jax.shard_map(device_fn, mesh=mesh, in_specs=in_specs, out_specs=out_specs, check_vma=False)
```

```python
import functools

import jax
import jax.numpy as jnp
from jax import lax
from jax.experimental import pallas as pl
from jax.experimental.pallas import tpu as pltpu
from jax.sharding import PartitionSpec as P

LN_EPS = 1e-6
MESH = pl.DeviceIdType.MESH
BF16, F32 = jnp.bfloat16, jnp.float32
ANY = pl.BlockSpec(memory_space=pl.ANY)
VMEM = pl.BlockSpec(memory_space=pltpu.VMEM)
SMEM = pl.BlockSpec(memory_space=pltpu.SMEM)
DMA = pltpu.SemaphoreType.DMA
FLIPS = [(a, b, e) for a in range(2) for b in range(2) for e in range(2)]
HALF, BLOCK, ROWS, LANES = 32, 64, 256, 128
SIDE = ROWS
ALL = (slice(None),) * 3
DIGITS = "0123456789"
REDUCE = ("fo3 fm3 fo2 ca3", "d3 fm2 fz3 fo1", "p3 q3 ca2 d2", "fz2 fm1 u3 fo0", "ca1 fz1 fm0 p2", "q2 d1 gz3 ca0", "fin u2 p1 q1", "d0 gz2 u1 gz1", "p0 q0 u0 end")
GATHER = ("zown sh0 zf1 sh1", "ty0 tx0 zf2 sh2", "zf3 ty1 cl0 fown", "tx1 um0 tx2 sh3", "uo0 us0 ff1 cl1", "ty2 ff2 um1 uo1", "us1 ff3 tx3 cl2", "ty3 um2 uo2 us2", "cl3 um3 uo3 us3")


class Here:
    def __init__(self):
        me = lax.axis_index("tp")
        self.c = lax.rem(me, 2)
        self.x = lax.rem(lax.div(me, 2), 2)
        self.y = lax.rem(lax.div(me, 4), 2)
        z = lax.div(me, 8)
        self.z = z
        inner = lax.rem(lax.div(z + 1, 2), 2)
        self.inner = inner == 1
        two, three = lax.rem(z + 2, 4), 3 - z
        self.zs = [z, z + 1 - 2 * lax.rem(z, 2), inner * three + (1 - inner) * two, inner * two + (1 - inner) * three]
        self.slot = ((z * 2 + self.c) * 2 + self.y) * 2 + self.x
        self.near, self.across = self.dev(self.zs[1]), self.dev(three)
        self.core, self.along_x, self.along_y = self.dev(z, a=1), self.dev(z, e=1), self.dev(z, b=1)

    def flip(self, v, on):
        return 1 - v if on else v

    def dev(self, z, a=0, b=0, e=0):
        y, x, c = self.flip(self.y, b), self.flip(self.x, e), self.flip(self.c, a)
        return ((z * 2 + y) * 2 + x) * 2 + c

    def apart(self, s):
        inner = lax.rem(lax.div(self.z + 1, 2), 2)
        return (0, 1, 2 + inner, 3 - inner)[s]

    def lines(self):
        return [self.near, self.dev(self.zs[2]), self.dev(self.zs[3]), self.core, self.along_x, self.along_y]

    def all(self):
        z = self.z
        zs = [z, self.zs[1], lax.rem(z + 2, 4), 3 - z]
        return [(8 * j + 4 * a + 2 * b + e, zs[j], (a, b, e)) for j in range(4) for a, b, e in FLIPS if j or a or b or e]


def meet(devices):
    sem = pltpu.get_barrier_semaphore()
    for d in devices:
        pl.semaphore_signal(sem, inc=1, device_id={"tp": d}, device_id_type=MESH)
    pl.semaphore_wait(sem, len(devices))


class Wires:
    def __init__(self, here, send, recv):
        self.here, self.send, self.recv = here, send, recv
        self.names, self.count = {}, 0
        self.started = {None: [], True: [], False: []}

    def copy(self, what, src, dst, device):
        k = self.names.setdefault(what, len(self.names))
        self.count += 1
        return pltpu.make_async_remote_copy(
            src_ref=src,
            dst_ref=dst,
            send_sem=self.send.at[self.count - 1],
            recv_sem=self.recv.at[k],
            device_id={"tp": device},
            device_id_type=MESH,
        )

    def go(self, what, src, dst, device, inner=None):
        copy = self.copy(what, src, dst, device)
        self.started[inner].append(copy)
        if inner is None:
            copy.start()
        else:
            pl.when(self.here.inner == inner)(copy.start)
        return copy

    def got(self, what, like):
        k = self.names.setdefault(what, len(self.names))
        pltpu.make_async_remote_copy(
            src_ref=like, dst_ref=like, send_sem=self.send.at[0], recv_sem=self.recv.at[k], device_id={"tp": self.here.core}, device_id_type=MESH
        ).wait_recv()

    def run(self, order):
        for word in " ".join(order).split():
            step = word.rstrip(DIGITS)
            getattr(self, step)(*(int(n) for n in word[len(step) :]))

    def drain(self):
        for copy in self.started[None]:
            copy.wait_send()
        for side in (True, False):

            @pl.when(self.here.inner == side)
            def _(copies=self.started[side]):
                for copy in copies:
                    copy.wait_send()


def nt(a, b):
    return lax.dot_general(a, b, (((1,), (1,)), ((), ())), preferred_element_type=F32)


def nn(a, b):
    return lax.dot_general(a, b, (((1,), (0,)), ((), ())), preferred_element_type=F32)


class Gather(Wires):
    COPIES = 48

    def __init__(self, here, own, plane, send, recv, use, used):
        super().__init__(here, send, recv)
        self.own, self.plane, self.use, self.used = own, plane, use, used
        dim = own.shape[-1]
        self.main, self.side, self.full = pl.ds(0, dim - SIDE), pl.ds(dim - SIDE, SIDE), pl.ds(0, dim)

    def at(self, s, b=0, e=0):
        h = self.here
        return self.plane(h.zs[s], h.c).at[h.flip(h.y, b), h.flip(h.x, e)].at[:, :, self.main if s else self.full]

    def fours(self, s):
        return self.plane(self.here.zs[s], self.here.c).at[:, :, :, :, self.side]

    def pass_on(self, what, s, ref):
        h = self.here
        self.go((what, 3 if s == 1 else s), ref, ref, h.across if s == 1 else h.near, True)

    def zown(self):
        h = self.here
        src, dst = self.own.at[:, :, self.main], self.at(0).at[:, :, self.main]
        self.go(("z", 1), src, dst, h.near)
        self.go(("z", 2), src, dst, h.across, True)

    def zf(self, s):
        self.got(("z", s), self.at(s))
        self.pass_on("z", s, self.at(s))

    def fown(self):
        h, ref = self.here, self.fours(0)
        self.go(("f", 1), ref, ref, h.near)
        self.go(("f", 2), ref, ref, h.across, True)

    def ff(self, s):
        ref = self.fours(s)
        self.got(("f", s), ref)
        self.pass_on("f", s, ref)
        self.go(("cf", s), ref, ref, self.here.core)

    def sh(self, s):
        h, dst = self.here, self.at(s)
        src = dst if s else self.own
        self.go(("x", s), src, dst, h.along_x)
        self.go(("y", s), src, dst, h.along_y)
        self.go(("c", s), src, dst, h.core)

    def tx(self, s):
        ref = self.at(s, e=1)
        self.got(("x", s), ref)
        self.go(("xy", s), ref.at[0], ref.at[0], self.here.along_y)
        self.go(("cx", s), ref, ref, self.here.core)

    def ty(self, s):
        ref = self.at(s, b=1)
        self.got(("y", s), ref)
        self.go(("yx", s), ref.at[1], ref.at[1], self.here.along_x)
        self.go(("cy", s), ref, ref, self.here.core)

    def cl(self, s):
        ref = self.at(s, 1, 1)
        self.got(("xy", s), ref.at[0])
        self.got(("yx", s), ref.at[1])
        self.go(("cd", s), ref, ref, self.here.core)

    def um(self, s):
        self.use(s, self.here.c)

    def uo(self, s):
        for what in ("c", "cx", "cy", "cd"):
            self.got((what, s), self.at(s))
        if s:
            self.got(("cf", s), self.fours(s))
        self.use(s, 1 - self.here.c)

    def us(self, s):
        self.used(s)


class Reduce(Wires):
    COPIES = 48

    @staticmethod
    def scratch(rows, dim, dtype):
        return [
            pltpu.VMEM((4, 4, 2, rows, dim), dtype),
            pltpu.VMEM((2, 4, 2, rows, dim), dtype),
            pltpu.VMEM((4, 4, 2, rows, dim), dtype),
            pltpu.VMEM((4, 2, rows, dim), dtype),
            pltpu.VMEM((4, 2, rows, dim), dtype),
            pltpu.VMEM((4, 2, rows, dim), dtype),
            pltpu.VMEM((6, 2, rows, dim - SIDE), dtype),
            pltpu.VMEM((6, 4, 2, rows, SIDE), dtype),
            DMA((Reduce.COPIES,)),
            DMA((Reduce.COPIES,)),
        ]

    def __init__(self, here, fill, finish, part, sib, core_in, diag_in, x_in, y_in, z_in, side_in, send, recv):
        super().__init__(here, send, recv)
        self.fill, self.finish = fill, finish
        self.part, self.sib, self.core_in, self.diag_in = part, sib, core_in, diag_in
        self.x_in, self.y_in, self.z_in, self.side_in = x_in, y_in, z_in, side_in
        dim = part.shape[-1]
        self.main, self.side, self.full = pl.ds(0, dim - SIDE), pl.ds(dim - SIDE, SIDE), pl.ds(0, dim)
        self.lent = []

    def quad(self, b, e):
        h = self.here
        return h.flip(h.y, b) * 2 + h.flip(h.x, e)

    def piece(self, buf, s, *where):
        return buf, (s, *where, slice(None), self.main if s else self.full)

    def add(self, ref, *more):
        buf, index = ref
        total = buf[index]
        for other, where in more:
            total = total + other[where]
        buf[index] = total

    def fo(self, s):
        n = len(self.lent)
        if n > 1:
            self.lent[n - 2].wait_send()
            self.started[None].remove(self.lent[n - 2])
        self.fill(s, 1 - self.here.c, self.sib.at[n % 2])
        self.lent.append(self.go(("c", s), self.sib.at[n % 2], self.core_in.at[s], self.here.core))

    def fm(self, s):
        self.fill(s, self.here.c, self.part.at[s])

    def ca(self, s):
        self.got(("c", s), self.core_in.at[s])
        for t in range(2):

            def add(i, carry):
                self.add((self.part, (s, i, t)), (self.core_in, (s, i, t)))
                return carry

            lax.fori_loop(0, 4, add, 0)

    def along_z(self, what, s, ref, landing):
        h = self.here
        k = 5 if s == 1 else s
        to = 1 if s == 1 else s + 2

        @pl.when(h.inner)
        def _():
            self.got((what, k), landing.at[k])
            self.add(ref, (landing, k))

        self.go((what, to), ref[0].at[ref[1]], landing.at[to], h.near if s == 1 else h.across, True)
        self.go((what, s), ref[0].at[ref[1]], landing.at[s], h.near, False)

    def last_z(self, what, ref, landing):
        self.got((what, 1), landing.at[1])
        self.add(ref, (landing, 1))

        @pl.when(self.here.inner)
        def _():
            self.got((what, 4), landing.at[4])
            self.add(ref, (landing, 4))

    def fz(self, s):
        self.along_z("f", s, (self.part, (s, *ALL, self.side)), self.side_in)

    def fin(self):
        self.last_z("f", (self.part, (0, *ALL, self.side)), self.side_in)

    def d(self, s):
        h, part = self.here, self.part
        far = self.quad(1, 1)
        self.pass_on("dy", s, self.piece(part, s, far, 0), self.piece(self.diag_in, s, 0), h.along_y)
        self.pass_on("dx", s, self.piece(part, s, far, 1), self.piece(self.diag_in, s, 1), h.along_x)
        self.pass_on("x1", s, self.piece(part, s, self.quad(0, 1), 1), self.piece(self.x_in, s, 1), h.along_x)
        self.pass_on("y0", s, self.piece(part, s, self.quad(1, 0), 0), self.piece(self.y_in, s, 0), h.along_y)

    def pass_on(self, what, s, src, dst, device):
        self.go((what, s), src[0].at[src[1]], dst[0].at[dst[1]], device)

    def came(self, what, s, ref):
        self.got((what, s), ref[0].at[ref[1]])

    def p(self, s):
        ref = self.piece(self.part, s, self.quad(0, 1), 0)
        self.came("dy", s, ref)
        self.add(ref, self.piece(self.diag_in, s, 0))
        self.pass_on("x0", s, ref, self.piece(self.x_in, s, 0), self.here.along_x)

    def q(self, s):
        ref = self.piece(self.part, s, self.quad(1, 0), 1)
        self.came("dx", s, ref)
        self.add(ref, self.piece(self.diag_in, s, 1))
        self.pass_on("y1", s, ref, self.piece(self.y_in, s, 1), self.here.along_y)

    def u(self, s):
        for t in range(2):
            ref = self.piece(self.part, s, self.quad(0, 0), t)
            self.came(f"x{t}", s, ref)
            self.came(f"y{t}", s, ref)
            self.add(ref, self.piece(self.x_in, s, t), self.piece(self.y_in, s, t))

    def gz(self, s):
        self.along_z("g", s, (self.part, (s, self.quad(0, 0), *ALL[:2], self.main)), self.z_in)

    def end(self):
        mine = self.quad(0, 0)
        self.last_z("g", (self.part, (0, mine, *ALL[:2], self.main)), self.z_in)
        for t in range(2):
            for lo in range(0, self.part.shape[3], 16):
                self.finish(t, lo, self.part[0, mine, t, lo : lo + 16])


def normed(x, gain):
    rows = x.astype(F32)
    centred = rows - jnp.mean(rows, axis=-1, keepdims=True)
    var = jnp.mean(centred * centred, axis=-1, keepdims=True)
    return (centred * lax.rsqrt(var + LN_EPS) * gain).astype(BF16)


def load(pairs, sems):
    copies = [pltpu.make_async_copy(src, dst, sems.at[i]) for i, (src, dst) in enumerate(pairs)]
    for copy in copies:
        copy.start()
    return copies


def embed_kernel(tok_ref, emb_hbm, gain_ref, x_ref, h_ref, emb, tail, sem, *rs):
    here = Here()
    vocab, dim = emb_hbm.shape
    whole = vocab // ROWS * ROWS
    rest = vocab - whole
    (fetch,) = load([(emb_hbm, emb)], sem)
    meet(here.lines())
    fetch.wait()
    tail[...] = jnp.zeros_like(tail)
    tail[0:rest] = emb[whole:vocab]
    base = lax.axis_index("tp") * vocab

    def fill(s, core, ref):
        tok = tok_ref[here.zs[s] * 2 + core] - base
        hot = (tok == lax.broadcasted_iota(jnp.int32, (ROWS, whole), 1)).astype(F32).astype(BF16)
        hot_tail = (tok == lax.broadcasted_iota(jnp.int32, (ROWS, LANES), 1) + whole).astype(F32).astype(BF16)

        def columns(n, carry):
            cols = pl.ds(pl.multiple_of(n * ROWS, ROWS), ROWS)
            rows = nn(hot, emb[0:whole, cols]) + nn(hot_tail, tail[:, cols])
            ref[:, :, :, cols] = rows.astype(BF16).reshape(4, 2, HALF, ROWS)
            return carry

        lax.fori_loop(0, dim // ROWS, columns, 0)

    def finish(t, lo, rows):
        x_ref[t, lo : lo + 16] = rows
        h_ref[t, lo : lo + 16] = normed(rows, gain_ref[...])

    red = Reduce(here, fill, finish, *rs)
    red.run(REDUCE)
    red.drain()


def in_kernel(layer, h_ref, cos_ref, sin_ref, cos_own, sin_own, wg_hbm, wu_hbm, wq_hbm, wkv_hbm, m_ref, q_ref, kv_ref,
              every, wide, wq, wkv, ready, q_out, sem, send, recv, q_send, q_recv):
    here = Here()
    dim = h_ref.shape[-1]
    half = cos_ref.shape[1]
    width = 2 * half
    hidden = m_ref.shape[-1]
    up_at = wide.shape[0] // 2
    pairs = [(wkv_hbm, wkv), (wg_hbm, wide.at[0:hidden]), (wu_hbm, wide.at[up_at : up_at + hidden]), (wq_hbm, wq.at[0:width])]
    fetch = load([(src.at[layer], dst) for src, dst in pairs], sem)
    meet([here.dev(z, *f) for _, z, f in here.all()])
    def turned(rows, cos, sin):
        lo, hi = rows[0:half], rows[half:width]
        return lo * cos - hi * sin, lo * sin + hi * cos

    every[here.z, here.c, here.y, here.x] = h_ref[...]
    sent = []

    def use(s, core):
        z = here.zs[s]
        rows = every[z, core].reshape(ROWS, dim)
        q = nt(wq[...], rows)
        lo, hi = turned(q, cos_ref[z * 2 + core], sin_ref[z * 2 + core])
        q = jnp.concatenate([lo, hi, jnp.zeros((LANES - width, ROWS), F32)], 0)
        q_out[z, core] = q.T.astype(BF16).reshape(4, BLOCK, LANES)

        def tile(n, carry):
            cols = pl.ds(pl.multiple_of(n * ROWS, ROWS), ROWS)
            ready[:, cols] = nt(every[z, core].reshape(ROWS, dim), wide[cols])
            return carry

        lax.fori_loop(0, wide.shape[0] // ROWS, tile, 0)

        def gated(n, carry):
            some = pl.ds(pl.multiple_of(n * HALF, HALF), HALF)
            gate, up = ready[some, 0:hidden], ready[some, up_at : up_at + hidden]
            m_ref[z * 2 + core, some] = (gate * jax.nn.sigmoid(gate) * up).astype(BF16)
            return carry

        lax.fori_loop(0, 8, gated, 0)

    def used(s):
        z = here.zs[s]
        for a, b, e in FLIPS:
            core, quad = here.flip(here.c, a), here.flip(here.y, b) * 2 + here.flip(here.x, e)
            if s == a == b == e == 0:
                q_ref[here.slot] = q_out[z, core, quad]
                continue
            j = 0 if s == 0 else here.apart(s)
            r = j * 8 + (a * 4 + b * 2 + e)
            copy = pltpu.make_async_remote_copy(
                q_out.at[z, core, quad], q_ref.at[here.slot], q_send.at[r], q_recv.at[r], device_id={"tp": here.dev(z, a, b, e)}, device_id_type=MESH
            )
            copy.start()
            sent.append(copy)

    gather = Gather(here, h_ref, lambda z, c: every.at[z, c], send, recv, use, used)

    def kv():
        fetch[0].wait()
        rows = nt(wkv[...], h_ref[...].reshape(BLOCK, dim))
        blank = jnp.zeros((LANES - width, BLOCK), BF16)
        lo, hi = turned(rows, cos_own[...], sin_own[...])
        kv_ref[...] = jnp.concatenate([jnp.concatenate([lo, hi], 0).astype(BF16), blank, rows[width:].astype(BF16), blank], 0)
        wq[width:LANES] = jnp.zeros((LANES - width, dim), BF16)
        for at in (0, up_at):
            wide[at + hidden : at + up_at] = jnp.zeros((up_at - hidden, dim), BF16)
        for copy in fetch[1:]:
            copy.wait()

    gather.run(GATHER[:1])
    kv()
    gather.run(GATHER[1:])
    gather.drain()
    for copy in sent:
        copy.wait_recv()
    for copy in sent:
        copy.wait_send()


def attend_kernel(layer, pos_ref, q_ref, kv_ref, k_hbm, v_hbm, o_ref, keys, values, q_rows, o_rows, o_out, sem, send, recv):
    here = Here()
    seqs, width, length = keys.shape
    fetch = load([(k_hbm.at[layer], keys), (v_hbm.at[layer], values)], sem)
    q_rows[...] = q_ref[...].reshape(2048, LANES).astype(F32)
    meet([here.dev(z, *f) for _, z, f in here.all()])
    for copy in fetch:
        copy.wait()
    row = lax.broadcasted_iota(jnp.int32, (BLOCK, length), 0)
    col = lax.broadcasted_iota(jnp.int32, (BLOCK, length), 1)
    cols = lax.broadcasted_iota(jnp.int32, (LANES, length), 1)
    blank = jnp.zeros((LANES - width, length), BF16)

    def one(s):
        pos = pos_ref[s]
        place = ((row == s) & (col == pos)) | ((row == s + HALF) & (col == pos + 1))
        new = nn(kv_ref[...], place.astype(F32).astype(BF16)).astype(BF16)
        fresh = (cols == pos) | (cols == pos + 1)
        k = jnp.where(fresh, new[0:LANES], jnp.concatenate([keys[s], blank], 0))
        v = jnp.where(fresh, new[LANES:ROWS], jnp.concatenate([values[s], blank], 0))
        q = q_rows[pl.ds(s, BLOCK, stride=HALF), :].astype(BF16)
        score = nn(q, k) * width**-0.5
        score = jnp.where(col <= pos + lax.rem(row, 2), score, -jnp.inf)
        weight = jnp.exp(score - jnp.max(score, axis=-1, keepdims=True))
        weight = (weight / jnp.sum(weight, axis=-1, keepdims=True)).astype(BF16)
        o_rows[pl.ds(s, BLOCK, stride=HALF), :] = nt(weight, v)

    def several(i, carry):
        for u in range(4):
            one(i * 4 + u)
        return carry

    lax.fori_loop(0, seqs // 4, several, 0)
    o_out[...] = o_rows[...].astype(BF16).reshape(HALF, BLOCK, LANES)
    o_ref[here.slot] = o_out[here.slot]
    sent = []
    for r, z, (a, b, e) in here.all():
        slot = ((z * 2 + here.flip(here.c, a)) * 2 + here.flip(here.y, b)) * 2 + here.flip(here.x, e)
        copy = pltpu.make_async_remote_copy(
            o_out.at[slot], o_ref.at[here.slot], send.at[r], recv.at[r], device_id={"tp": here.dev(z, a, b, e)}, device_id_type=MESH
        )
        copy.start()
        sent.append(copy)
    for copy in sent:
        copy.wait_recv()
    for copy in sent:
        copy.wait_send()


def out_kernel(layer, m_ref, o_ref, x_ref, gain_ref, wd_hbm, wo_hbm, x_out, h_out, wd, wo, sem, *rs):
    here = Here()
    dim = wd.shape[-1]
    width = wo_hbm.shape[1]
    fetch = load([(wd_hbm.at[layer], wd), (wo_hbm.at[layer], wo.at[0:width])], sem)
    wo[width:LANES] = jnp.zeros((LANES - width, dim), BF16)
    meet(here.lines())
    for copy in fetch:
        copy.wait()

    def fill(s, core, ref):
        zc = here.zs[s] * 2 + core

        def columns(n, carry):
            cols = pl.ds(pl.multiple_of(n * ROWS, ROWS), ROWS)
            rows = nn(o_ref[zc], wo[:, cols]) + nn(m_ref[zc], wd[:, cols])
            ref[:, :, :, cols] = rows.reshape(4, 2, HALF, ROWS)
            return carry

        lax.fori_loop(0, dim // ROWS, columns, 0)

    def finish(t, lo, rows):
        x = (x_ref[t, lo : lo + 16].astype(F32) + rows).astype(BF16)
        x_out[t, lo : lo + 16] = x
        h_out[t, lo : lo + 16] = normed(x, gain_ref[...])

    red = Reduce(here, fill, finish, *rs)
    red.run(REDUCE)
    red.drain()


def head_kernel(h_ref, emb_hbm, out_hbm, every, rows, emb, ready, sem, out_sem, send, recv):
    here = Here()
    vocab, dim = emb_hbm.shape
    whole = vocab // ROWS * ROWS
    scale = dim**-0.5
    (fetch,) = load([(emb_hbm, emb)], sem)
    meet(here.lines())
    every[here.z, here.c, here.y, here.x] = h_ref[...]
    stores = []

    def used(s):
        z = here.zs[s]
        slot = len(stores) % 2
        if len(stores) >= 2:
            stores[-2].wait()

        def step(t, carry):
            for b in range(8):
                c, y, x = b % 2, b // 4, b // 2 % 2
                rows[b * HALF : b * HALF + HALF] = every[z, c, y, x, t]

            def part(lo, n):
                ready[slot, pl.ds(lo, n), t, :] = nt(emb[pl.ds(lo, n)], rows[...]) * scale

            def tile(i, carry):
                part(pl.multiple_of(i * ROWS, ROWS), ROWS)
                return carry

            lax.fori_loop(0, whole // ROWS, tile, 0)
            part(whole, vocab - whole)
            return carry

        lax.fori_loop(0, 2, step, 0)
        cols = pl.ds(pl.multiple_of(z * ROWS, ROWS), ROWS)
        copy = pltpu.make_async_copy(ready.at[slot], out_hbm.at[:, :, cols], out_sem.at[slot])
        copy.start()
        stores.append(copy)

    gather = Gather(here, h_ref, lambda z, c: every.at[z, c], send, recv, lambda s, core: None, used)
    gather.run(GATHER[:1])
    fetch.wait()
    gather.run(GATHER[1:])
    gather.drain()
    stores[-2].wait()
    stores[-1].wait()


def params(index, mib):
    return pltpu.CompilerParams(collective_id=index, has_side_effects=True, vmem_limit_bytes=mib << 20)


def solution(mesh):
    def device_fn(tokens, lengths, embedding, ln_scale, w_q, w_kv, w_o, w_gate, w_up, w_down, final_scale, k_cache, v_cache):
        me = lax.axis_index("tp")
        steps, batch = tokens.shape
        vocab, dim = embedding.shape
        layers, seqs, length, width = k_cache.shape
        hidden = w_gate.shape[-1]
        half = width // 2
        up_at = pl.cdiv(hidden, LANES) * LANES
        block = jax.ShapeDtypeStruct((2, HALF, dim), BF16)

        def ordered(rows):
            return rows.reshape(2, 4, 2, 2, 2, HALF).transpose(1, 4, 2, 3, 0, 5).reshape(8, ROWS)

        positions = lengths[None, :] + jnp.arange(steps, dtype=jnp.int32)[:, None]
        own_len = lax.dynamic_slice_in_dim(lengths, me * seqs, seqs)
        own_pos = own_len[None, :] + jnp.arange(steps, dtype=jnp.int32)[:, None]
        inv_freq = 10000.0 ** (-jnp.arange(half, dtype=F32) / half)
        angles = ordered(positions)[:, None, :].astype(F32) * inv_freq[None, :, None]
        own_angles = own_pos.reshape(1, BLOCK).astype(F32) * inv_freq[:, None]
        turns = jnp.cos(angles), jnp.sin(angles), jnp.cos(own_angles), jnp.sin(own_angles)
        gains = [ln_scale[l][None] for l in range(layers)] + [final_scale[None]]

        x, h = pl.pallas_call(
            embed_kernel,
            out_shape=(block, block),
            in_specs=[VMEM, ANY, VMEM],
            out_specs=(VMEM, VMEM),
            scratch_shapes=[pltpu.VMEM((vocab, dim), BF16), pltpu.VMEM((LANES, dim), BF16), DMA((1,)), *Reduce.scratch(HALF, dim, BF16)],
            compiler_params=params(0, 60),
            name="embed",
        )(ordered(tokens)[:, :, None], embedding, gains[0])

        wg_t, wu_t, wkv_t = (w.transpose(0, 2, 1) for w in (w_gate, w_up, w_kv))
        wq_t = w_q.transpose(0, 2, 3, 1).reshape(layers, width, dim)
        wo = w_o.reshape(layers, width, dim)
        k_t, v_t = k_cache.transpose(0, 1, 3, 2), v_cache.transpose(0, 1, 3, 2)
        fresh = []
        for l in range(layers):
            m, q, kv = pl.pallas_call(
                functools.partial(in_kernel, l),
                out_shape=(
                    jax.ShapeDtypeStruct((8, ROWS, hidden), BF16),
                    jax.ShapeDtypeStruct((HALF, BLOCK, LANES), BF16),
                    jax.ShapeDtypeStruct((ROWS, BLOCK), BF16),
                ),
                in_specs=[VMEM] * 5 + [ANY] * 4,
                out_specs=(VMEM, VMEM, VMEM),
                scratch_shapes=[
                    pltpu.VMEM((4, 2, 2, 2, 2, HALF, dim), BF16),
                    pltpu.VMEM((2 * up_at, dim), BF16),
                    pltpu.VMEM((LANES, dim), BF16),
                    pltpu.VMEM((2 * width, dim), BF16),
                    pltpu.VMEM((ROWS, 2 * up_at), F32),
                    pltpu.VMEM((4, 2, 4, BLOCK, LANES), BF16),
                    DMA((4,)),
                    DMA((Gather.COPIES,)),
                    DMA((Gather.COPIES,)),
                    DMA((HALF,)),
                    DMA((HALF,)),
                ],
                compiler_params=params(1 + 3 * l, 48),
                name=f"in{l}",
            )(h, *turns, wg_t, wu_t, wq_t, wkv_t)
            fresh.append(kv)
            o = pl.pallas_call(
                functools.partial(attend_kernel, l),
                out_shape=jax.ShapeDtypeStruct((HALF, BLOCK, LANES), BF16),
                in_specs=[SMEM, VMEM, VMEM, ANY, ANY],
                out_specs=VMEM,
                scratch_shapes=[
                    pltpu.VMEM((seqs, width, length), BF16),
                    pltpu.VMEM((seqs, width, length), BF16),
                    pltpu.VMEM((2048, LANES), F32),
                    pltpu.VMEM((2048, LANES), F32),
                    pltpu.VMEM((HALF, BLOCK, LANES), BF16),
                    DMA((2,)),
                    DMA((HALF,)),
                    DMA((HALF,)),
                ],
                compiler_params=params(2 + 3 * l, 40),
                name=f"attend{l}",
            )(own_len, q, kv, k_t, v_t)
            x, h = pl.pallas_call(
                functools.partial(out_kernel, l),
                out_shape=(block, block),
                in_specs=[VMEM] * 4 + [ANY] * 2,
                out_specs=(VMEM, VMEM),
                scratch_shapes=[pltpu.VMEM((hidden, dim), BF16), pltpu.VMEM((LANES, dim), BF16), DMA((2,)), *Reduce.scratch(HALF, dim, F32)],
                compiler_params=params(3 + 3 * l, 60),
                name=f"out{l}",
            )(m, o.reshape(8, ROWS, LANES), x, gains[l + 1], w_down, wo)

        logits = pl.pallas_call(
            head_kernel,
            out_shape=jax.ShapeDtypeStruct((vocab, 2, batch), F32),
            in_specs=[VMEM, ANY],
            out_specs=ANY,
            scratch_shapes=[
                pltpu.VMEM((4, 2, 2, 2, 2, HALF, dim), BF16),
                pltpu.VMEM((ROWS, dim), BF16),
                pltpu.VMEM((vocab, dim), BF16),
                pltpu.VMEM((2, vocab, 2, ROWS), F32),
                DMA((1,)),
                DMA((2,)),
                DMA((Gather.COPIES,)),
                DMA((Gather.COPIES,)),
            ],
            compiler_params=params(7, 60),
            name="head",
        )(h, embedding)

        row_ids = lax.broadcasted_iota(jnp.int32, (1, 1, length, 1), 2)
        new = jnp.stack(fresh)[:, :, None].reshape(layers, 2, LANES, 2, HALF)[:, :, :width]

        def written(cache, which):
            for t in range(steps):
                cache = jnp.where(
                    row_ids == own_pos[t][None, :, None, None], new[:, which, :, t].transpose(0, 2, 1)[:, :, None, :], cache
                )
            return cache

        return logits.transpose(1, 2, 0), written(k_cache, 0), written(v_cache, 1)

    cache_spec = P(None, "tp", None, None)
    in_specs = (P(), P(), P("tp", None), P(), P(None, None, "tp", None), P(), P(None, "tp", None, None), P(None, None, "tp"), P(None, None, "tp"), P(None, "tp", None), P(), cache_spec, cache_spec)
    out_specs = (P(None, None, "tp"), cache_spec, cache_spec)
    return jax.shard_map(device_fn, mesh=mesh, in_specs=in_specs, out_specs=out_specs, check_vma=False)
```

```python
import functools

import jax
import jax.numpy as jnp
from jax import lax
from jax.experimental import pallas as pl
from jax.experimental.pallas import tpu as pltpu
from jax.sharding import PartitionSpec as P

LN_EPS = 1e-6
MESH = pl.DeviceIdType.MESH
BF16, F32 = jnp.bfloat16, jnp.float32
ANY = pl.BlockSpec(memory_space=pl.ANY)
VMEM = pl.BlockSpec(memory_space=pltpu.VMEM)
SMEM = pl.BlockSpec(memory_space=pltpu.SMEM)
DMA = pltpu.SemaphoreType.DMA
FLIPS = [(a, b, e) for a in range(2) for b in range(2) for e in range(2)]
HALF, BLOCK, ROWS, LANES = 32, 64, 256, 128
SIDE = ROWS
ALL = (slice(None),) * 3
DIGITS = "0123456789"
REDUCE = ("fo3 fm3 fo2 ca3", "d3 fm2 fz3 fo1", "p3 q3 ca2 d2", "fz2 fm1 u3 fo0", "ca1 fz1 fm0 p2", "q2 d1 gz3 ca0", "fin u2 p1 q1", "d0 gz2 u1 gz1", "p0 q0 u0 end")
TAIL = 40
ORDER = (
    "Ash0 Bsh0 Azown Bzown", "Aty0 Atx0 Azf1 Ash1", "Azf2 Bzf1 Bsh1 Btx0", "Bty0 Bzf2 Bsh2 Atx1", "Acl0 Ash2 Afown Bzf3",
    "Bty1 Btx1 Azf3 Aty1", "Bcl0 Bfown Bsh3 Aty2", "Ash3 Aff2 Bff2 Aff1", "Bty2 Atx2 Btx2 Bff1", "Aff3 Bff3 Bcl1 Btx3",
    "Acl1 Aty3 Acl2 Bty3", "Atx3 Bus1 Aus2 Bus0", "Acl3 Bcl3 Aus1 Bcl2", "Aus3 Aus0 Bus2 Bus3", "Jatt Katt Rfo2 Rfm2",
    "Rfo0 Rfm0 Rca2 Rd2", "Rfo3 Sfo2 Rfm3 Sfm2", "Rp2 Rq2 Rca3 Sfo3", "Rd3 Sca2 Sd2 Sfz2", "Rfo1 Rfm1 Rfz3 Ru2",
    "Rca0 Sfm3 Rca1 Sfo0", "Sca3 Sd3 Sfz3 Rfz1", "Rp3 Sfo1 Rq3 Rd1", "Sp2 Sfm1 Rfz2 Sq2", "Rgz2 Rfin Sca1 Ru3",
    "Rd0 Sp3 Sfm0 Sca0", "Rp1 Sq3 Sfz1 Rq1", "Rgz3 Sd1 Rp0 Su2", "Rq0 Sgz2 Sfin Sd0", "Su3 Sgz3 Ru1 Rgz1",
    "Ru0 Sp1 Sq1 Sp0", "Rend Czown Sq0 Su1", "Csh0 Sgz1 Czf1 Csh1", "Su0 Czf2 Csh2 Cty0", "Ctx0 Send Dsh0 Dzown",
    "Ctx2 Ccl0 Cty1 Czf3", "Ctx1 Csh3 Cfown Cff2", "Dtx0 Cty2 Dzf1 Dzf2", "Dty0 Ctx3 Cus0 Cty3", "Ccl2 Dzf3 Dsh3 Ccl1",
    "Dsh2 Dcl0 Cff1 Dfown", "Cus2 Ccl3 Dsh1 Cff3", "Cus1 Cus3 Dff1 Dty3", "Dff2 Dus0 Dty2 Dtx3", "Dtx1 Dtx2 Dty1 Latt",
    "Dcl1 Dcl3 Dcl2 Dus2", "Dff3 Tfo2 Dus1 Dus3", "Tfm2 Tca2 Tfo3 Tfo0", "Td2 Tfm3 Tfo1 Matt", "Tfm1 Tq2 Tca1 Tp2",
    "Tca3 Td3 Ufo2 Ufm2", "Tu2 Tfm0 Tp3 Uca2", "Ud2 Tq3 Tfz2 Tca0", "Td1 Ufo3 Ufz2 Ufo0", "Ufm3 Tfz3 Uca3 Ud3",
    "Ufo1 Ufm1 Ufz3 Ufm0", "Uq2 Up2 Tfz1 Uca1", "Tu3 Tgz3 Tp1 Ufz1", "Tq1 Uq3 Up3 Uca0", "Tfin Td0 Tgz2 Ufin",
    "Uu2 Ud0 Ugz2 Tu1", "Uu3 Tgz1 Tp0 Tq0", "Ud1 Ugz3 Tu0 Tend", "Ezown Uq1 Up1 Esh0", "Ezf1 Uu1 Ugz1 Esh1",
    "Ety0 Etx0 Uq0 Up0", "Ety1 Ezf2 Esh2 Ecl0", "Ezf3 Etx1 Uu0 Efown", "Esh3 Uend Fzown Ety2", "Etx2 Fsh0 Ecl1 Eus0",
    "Ety3 Etx3 Eff2 Fzf2", "Eff1 Ecl2 Fsh2 Fzf1", "Fty0 Ftx0 Eus2 Fsh1", "Eus1 Fty2 Ftx2 Fzf3", "Ecl3 Fcl0 Ffown Ftx1",
    "Fty1 Eff3 Fsh3 Fus0", "Fcl2 Eus3 Fcl1 Fff1", "Fff2 Fty3 Ftx3 Fus1", "Fff3 Fcl3 Fus2 Fus3",
)


class Here:
    def __init__(self):
        me = lax.axis_index("tp")
        self.c = lax.rem(me, 2)
        self.x = lax.rem(lax.div(me, 2), 2)
        self.y = lax.rem(lax.div(me, 4), 2)
        z = lax.div(me, 8)
        self.z = z
        self.against = {id(v): 1 - v for v in (self.c, self.x, self.y)}
        inner = lax.rem(lax.div(z + 1, 2), 2)
        self.inner = inner == 1
        two, three = lax.rem(z + 2, 4), 3 - z
        self.zs = [z, z + 1 - 2 * lax.rem(z, 2), inner * three + (1 - inner) * two, inner * two + (1 - inner) * three]
        self.slot = ((z * 2 + self.c) * 2 + self.y) * 2 + self.x
        self.near, self.across = self.dev(self.zs[1]), self.dev(three)
        self.core, self.along_x, self.along_y = self.dev(z, a=1), self.dev(z, e=1), self.dev(z, b=1)

    def flip(self, v, on):
        return self.against[id(v)] if on else v

    def dev(self, z, a=0, b=0, e=0):
        y, x, c = self.flip(self.y, b), self.flip(self.x, e), self.flip(self.c, a)
        return ((z * 2 + y) * 2 + x) * 2 + c

    def apart(self, s):
        inner = lax.rem(lax.div(self.z + 1, 2), 2)
        return (0, 1, 2 + inner, 3 - inner)[s]

    def partner(self, s, f):
        a, b, e = lax.div(f, 4), lax.rem(lax.div(f, 2), 2), lax.rem(f, 2)
        c, y, x = (on + v - 2 * on * v for on, v in ((a, self.c), (b, self.y), (e, self.x)))
        return self.apart(s) * 8 + f, c, y * 2 + x, ((self.zs[s] * 2 + y) * 2 + x) * 2 + c

    def lines(self):
        return [self.near, self.dev(self.zs[2]), self.dev(self.zs[3]), self.core, self.along_x, self.along_y]

    def all(self):
        z = self.z
        zs = [z, self.zs[1], lax.rem(z + 2, 4), 3 - z]
        return [(8 * j + 4 * a + 2 * b + e, zs[j], (a, b, e)) for j in range(4) for a, b, e in FLIPS if j or a or b or e]


def meet(devices):
    sem = pltpu.get_barrier_semaphore()
    for d in devices:
        pl.semaphore_signal(sem, inc=1, device_id={"tp": d}, device_id_type=MESH)
    pl.semaphore_wait(sem, len(devices))


class Wires:
    def __init__(self, here, send, recv, sizes):
        self.here, self.send, self.recv = here, send, recv
        self.names, self.first, self.started, at = {}, {}, {}, 0
        for kind, count in sizes.items():
            self.first[kind], self.started[kind] = at, []
            at += count

    def go(self, what, src, dst, device, inner=None):
        kind = tuple(src.shape), inner
        k = self.names.setdefault(what, len(self.names))
        copy = pltpu.make_async_remote_copy(
            src_ref=src,
            dst_ref=dst,
            send_sem=self.send.at[self.first[kind] + len(self.started[kind])],
            recv_sem=self.recv.at[k],
            device_id={"tp": device},
            device_id_type=MESH,
        )
        self.started[kind].append(src)
        if inner is None:
            copy.start()
        else:
            pl.when(self.here.inner == inner)(copy.start)

    def got(self, what, like):
        k = self.names.setdefault(what, len(self.names))
        pltpu.make_async_copy(like, like, self.recv.at[k]).wait()

    def run(self, order):
        for word in " ".join(order).split():
            step = word.rstrip(DIGITS)
            getattr(self, step)(*(int(n) for n in word[len(step) :]))

    def drain(self):
        for (kind, inner), copies in self.started.items():

            def wait(ref=copies[0], first=self.first[kind, inner], count=len(copies)):
                def one(i, carry):
                    pltpu.make_async_copy(ref, ref, self.send.at[first + i]).wait()
                    return carry

                lax.fori_loop(0, count, one, 0)

            if inner is None:
                wait()
            else:
                pl.when(self.here.inner == inner)(wait)


def nt(a, b):
    return lax.dot_general(a, b, (((1,), (1,)), ((), ())), preferred_element_type=F32)


def nn(a, b):
    return lax.dot_general(a, b, (((1,), (0,)), ((), ())), preferred_element_type=F32)


class Gather(Wires):
    COPIES = 48

    def __init__(self, here, own, plane, send, recv, use):
        rows, dim = own.shape[1:]
        main, four = ((2, rows, dim - SIDE)), (2, 2, 2, rows, SIDE)
        sizes = {(main, None): 19, (main, True): 4, ((2, rows, dim), None): 6, (four, None): 4, (four, True): 4}
        super().__init__(here, send, recv, sizes | {(main[1:], None): 6, ((rows, dim), None): 2})
        self.own, self.plane, self.use = own, plane, use
        self.main, self.side, self.full = pl.ds(0, dim - SIDE), pl.ds(dim - SIDE, SIDE), pl.ds(0, dim)

    def at(self, s, b=0, e=0):
        h = self.here
        return self.plane(h.zs[s], h.c).at[h.flip(h.y, b), h.flip(h.x, e)].at[:, :, self.main if s else self.full]

    def fours(self, s):
        return self.plane(self.here.zs[s], self.here.c).at[:, :, :, :, self.side]

    def pass_on(self, what, s, ref):
        h = self.here
        self.go((what, 3 if s == 1 else s), ref, ref, h.across if s == 1 else h.near, True)

    def zown(self):
        h = self.here
        src, dst = self.own.at[:, :, self.main], self.at(0).at[:, :, self.main]
        self.go(("z", 1), src, dst, h.near)
        self.go(("z", 2), src, dst, h.across, True)

    def zf(self, s):
        self.got(("z", s), self.at(s))
        self.pass_on("z", s, self.at(s))

    def fown(self):
        h, ref = self.here, self.fours(0)
        self.go(("f", 1), ref, ref, h.near)
        self.go(("f", 2), ref, ref, h.across, True)

    def ff(self, s):
        ref = self.fours(s)
        self.got(("f", s), ref)
        self.pass_on("f", s, ref)
        self.go(("cf", s), ref, ref, self.here.core)

    def sh(self, s):
        h, dst = self.here, self.at(s)
        src = dst if s else self.own
        self.go(("x", s), src, dst, h.along_x)
        self.go(("y", s), src, dst, h.along_y)
        self.go(("c", s), src, dst, h.core)

    def tx(self, s):
        ref = self.at(s, e=1)
        self.got(("x", s), ref)
        self.go(("xy", s), ref.at[0], ref.at[0], self.here.along_y)
        self.go(("cx", s), ref, ref, self.here.core)

    def ty(self, s):
        ref = self.at(s, b=1)
        self.got(("y", s), ref)
        self.go(("yx", s), ref.at[1], ref.at[1], self.here.along_x)
        self.go(("cy", s), ref, ref, self.here.core)

    def cl(self, s):
        ref = self.at(s, 1, 1)
        self.got(("xy", s), ref.at[0])
        self.got(("yx", s), ref.at[1])
        self.go(("cd", s), ref, ref, self.here.core)

    def us(self, s):
        for what in ("c", "cx", "cy", "cd"):
            self.got((what, s), self.at(s))
        if s:
            self.got(("cf", s), self.fours(s))
        self.use(s)


class Loans:
    def __init__(self, here, send, free):
        self.here, self.send, self.free = here, send, free
        self.lent, self.out = [], set()

    def take(self, s):
        if s in self.out:
            pl.semaphore_wait(self.free.at[s], 1)
        self.out.add(s)

    def give(self, s):
        pl.semaphore_signal(self.free.at[s], inc=1, device_id={"tp": self.here.core}, device_id_type=MESH)

    def settle(self):
        for copy in self.lent[-2:]:
            copy.wait_send()
        for s in self.out:
            pl.semaphore_wait(self.free.at[s], 1)


class Reduce(Wires):
    COPIES = 48

    @staticmethod
    def scratch(rows, dim, dtype):
        return [
            pltpu.VMEM((4, 4, 2, rows, dim), dtype),
            pltpu.VMEM((2, 4, 2, rows, dim), dtype),
            pltpu.VMEM((4, 4, 2, rows, dim), dtype),
            pltpu.VMEM((4, 2, rows, dim), dtype),
            pltpu.VMEM((4, 2, rows, dim), dtype),
            pltpu.VMEM((4, 2, rows, dim), dtype),
            pltpu.VMEM((5, 2, rows, dim - SIDE), dtype),
            pltpu.VMEM((5, 4, 2, rows, SIDE), dtype),
            DMA((Reduce.COPIES,)),
            DMA((Reduce.COPIES,)),
            DMA((2,)),
            pltpu.SemaphoreType.REGULAR((4,)),
        ]

    def __init__(self, here, fill, finish, loans, part, sib, core_in, diag_in, x_in, y_in, z_in, side_in, send, recv):
        rows, dim = part.shape[3:]
        main, four = (2, rows, dim - SIDE), (4, 2, rows, SIDE)
        sizes = {(main[1:], None): 18, ((rows, dim), None): 6, (four, True): 3, (four, False): 3, (main, True): 3, (main, False): 3}
        super().__init__(here, send, recv, sizes)
        self.fill, self.finish, self.loans = fill, finish, loans
        self.part, self.sib, self.core_in, self.diag_in = part, sib, core_in, diag_in
        self.x_in, self.y_in, self.z_in, self.side_in = x_in, y_in, z_in, side_in
        dim = part.shape[-1]
        self.main, self.side, self.full = pl.ds(0, dim - SIDE), pl.ds(dim - SIDE, SIDE), pl.ds(0, dim)

    def quad(self, b, e):
        h = self.here
        return h.flip(h.y, b) * 2 + h.flip(h.x, e)

    def piece(self, buf, s, *where):
        return buf, (s, *where, slice(None), self.main if s else self.full)

    def add(self, ref, *more):
        buf, index = ref
        total = buf[index]
        for other, where in more:
            total = total + other[where]
        buf[index] = total

    def fo(self, s):
        loans, n = self.loans, len(self.loans.lent)
        if n > 1:
            loans.lent[n - 2].wait_send()
        self.fill(s, self.here.flip(self.here.c, 1), self.sib.at[n % 2])
        loans.take(s)
        k = self.names.setdefault(("c", s), len(self.names))
        copy = pltpu.make_async_remote_copy(
            src_ref=self.sib.at[n % 2],
            dst_ref=self.core_in.at[s],
            send_sem=loans.send.at[n % 2],
            recv_sem=self.recv.at[k],
            device_id={"tp": self.here.core},
            device_id_type=MESH,
        )
        copy.start()
        loans.lent.append(copy)

    def fm(self, s):
        self.fill(s, self.here.c, self.part.at[s])

    def ca(self, s):
        self.got(("c", s), self.core_in.at[s])
        for t in range(2):

            def add(i, carry):
                self.add((self.part, (s, i, t)), (self.core_in, (s, i, t)))
                return carry

            lax.fori_loop(0, 4, add, 0)
        self.loans.give(s)

    def along_z(self, what, s, ref, landing):
        h = self.here
        k = 5 if s == 1 else s
        to = 1 if s == 1 else s + 2

        @pl.when(h.inner)
        def _():
            self.got((what, k), landing.at[k - 1])
            self.add(ref, (landing, k - 1))

        self.go((what, to), ref[0].at[ref[1]], landing.at[to - 1], h.near if s == 1 else h.across, True)
        self.go((what, s), ref[0].at[ref[1]], landing.at[s - 1], h.near, False)

    def last_z(self, what, ref, landing):
        self.got((what, 1), landing.at[0])
        self.add(ref, (landing, 0))

        @pl.when(self.here.inner)
        def _():
            self.got((what, 4), landing.at[3])
            self.add(ref, (landing, 3))

    def fz(self, s):
        self.along_z("f", s, (self.part, (s, *ALL, self.side)), self.side_in)

    def fin(self):
        self.last_z("f", (self.part, (0, *ALL, self.side)), self.side_in)

    def d(self, s):
        h, part = self.here, self.part
        far = self.quad(1, 1)
        self.pass_on("dy", s, self.piece(part, s, far, 0), self.piece(self.diag_in, s, 0), h.along_y)
        self.pass_on("dx", s, self.piece(part, s, far, 1), self.piece(self.diag_in, s, 1), h.along_x)
        self.pass_on("x1", s, self.piece(part, s, self.quad(0, 1), 1), self.piece(self.x_in, s, 1), h.along_x)
        self.pass_on("y0", s, self.piece(part, s, self.quad(1, 0), 0), self.piece(self.y_in, s, 0), h.along_y)

    def pass_on(self, what, s, src, dst, device):
        self.go((what, s), src[0].at[src[1]], dst[0].at[dst[1]], device)

    def came(self, what, s, ref):
        self.got((what, s), ref[0].at[ref[1]])

    def p(self, s):
        ref = self.piece(self.part, s, self.quad(0, 1), 0)
        self.came("dy", s, ref)
        self.add(ref, self.piece(self.diag_in, s, 0))
        self.pass_on("x0", s, ref, self.piece(self.x_in, s, 0), self.here.along_x)

    def q(self, s):
        ref = self.piece(self.part, s, self.quad(1, 0), 1)
        self.came("dx", s, ref)
        self.add(ref, self.piece(self.diag_in, s, 1))
        self.pass_on("y1", s, ref, self.piece(self.y_in, s, 1), self.here.along_y)

    def u(self, s):
        for t in range(2):
            ref = self.piece(self.part, s, self.quad(0, 0), t)
            self.came(f"x{t}", s, ref)
            self.came(f"y{t}", s, ref)
            self.add(ref, self.piece(self.x_in, s, t), self.piece(self.y_in, s, t))

    def gz(self, s):
        self.along_z("g", s, (self.part, (s, self.quad(0, 0), *ALL[:2], self.main)), self.z_in)

    def end(self):
        mine = self.quad(0, 0)
        self.last_z("g", (self.part, (0, mine, *ALL[:2], self.main)), self.z_in)
        for t in range(2):
            for lo in range(0, self.part.shape[3], 16):
                self.finish(t, lo, self.part[0, mine, t, lo : lo + 16])


def normed(x, gain):
    rows = x.astype(F32)
    centred = rows - jnp.mean(rows, axis=-1, keepdims=True)
    var = jnp.mean(centred * centred, axis=-1, keepdims=True)
    return (centred * lax.rsqrt(var + LN_EPS) * gain).astype(BF16)


def load(pairs, sems):
    copies = [pltpu.make_async_copy(src, dst, sems.at[i]) for i, (src, dst) in enumerate(pairs)]
    for copy in copies:
        copy.start()
    return copies


def embed_kernel(tok_ref, emb_hbm, gain_ref, x_ref, h_ref, emb, tail, sem, *scratch):
    here = Here()
    vocab, dim = emb_hbm.shape
    whole = vocab // ROWS * ROWS
    rest = vocab - whole
    (fetch,) = load([(emb_hbm, emb)], sem)
    meet(here.lines())
    fetch.wait()
    tail[...] = jnp.zeros_like(tail)
    tail[0:rest] = emb[whole:vocab]
    base = lax.axis_index("tp") * vocab

    def fill(s, core, ref):
        tok = tok_ref[here.zs[s] * 2 + core] - base
        hot = (tok == lax.broadcasted_iota(jnp.int32, (ROWS, whole), 1)).astype(F32).astype(BF16)
        hot_tail = (tok == lax.broadcasted_iota(jnp.int32, (ROWS, LANES), 1) + whole).astype(F32).astype(BF16)

        def columns(n, carry):
            cols = pl.ds(pl.multiple_of(n * ROWS, ROWS), ROWS)
            rows = nn(hot, emb[0:whole, cols]) + nn(hot_tail, tail[:, cols])
            ref[:, :, :, cols] = rows.astype(BF16).reshape(4, 2, HALF, ROWS)
            return carry

        lax.fori_loop(0, dim // ROWS, columns, 0)

    def finish(t, lo, rows):
        x_ref[t, lo : lo + 16] = rows
        h_ref[t, lo : lo + 16] = normed(rows, gain_ref[...])

    *rs, lent, free = scratch
    loans = Loans(here, lent, free)
    red = Reduce(here, fill, finish, loans, *rs)
    red.run(REDUCE)
    red.drain()
    loans.settle()


class Layers:
    INPUTS = ("lengths", "x_ref", "h_ref", "gains", "cos", "sin", "cos_own", "sin_own", "emb_tail", "wg_hbm", "wu_hbm")
    INPUTS += ("wq_hbm", "wkv_hbm", "wd_hbm", "wo_hbm", "k_hbm", "v_hbm", "emb_hbm", "out_hbm", "kv_out")

    @staticmethod
    def scratch(dim, hidden, width, seqs, length):
        up_at = pl.cdiv(hidden, LANES) * LANES
        return {
            "x": pltpu.VMEM((2, 2, 16, dim), BF16),
            "h": pltpu.VMEM((2, 2, 16, dim), BF16),
            "every": pltpu.VMEM((2, 4, 2, 2, 2, 2, 16, dim), BF16),
            "wide": pltpu.VMEM((2 * up_at, dim), BF16),
            "wq": pltpu.VMEM((LANES, dim), BF16),
            "wkv": pltpu.VMEM((2 * width, dim), BF16),
            "wd": pltpu.VMEM((hidden, dim), BF16),
            "wo": pltpu.VMEM((LANES, dim), BF16),
            "ready": pltpu.VMEM((ROWS, 2 * up_at), F32),
            "m": pltpu.VMEM((2, 4, ROWS, hidden), BF16),
            "q_out": pltpu.VMEM((2, 4, 2, 4, HALF, LANES), BF16),
            "q_in": pltpu.VMEM((2, 8, 4, HALF, LANES), BF16),
            "o_out": pltpu.VMEM((2, 8, 4, HALF, LANES), BF16),
            "o_in": pltpu.VMEM((2, 8, 4, HALF, LANES), BF16),
            "q_rows": pltpu.VMEM((1024, LANES), F32),
            "o_rows": pltpu.VMEM((1024, LANES), F32),
            "keys": pltpu.VMEM((seqs, width, length), BF16),
            "values": pltpu.VMEM((seqs, width, length), BF16),
            "tiles": pltpu.VMEM((2, ROWS, dim), BF16),
            "logits": pltpu.VMEM((2, ROWS, ROWS), F32),
            "last": pltpu.VMEM((TAIL, ROWS), F32),
            "w_sem": DMA((8,)),
            "tile_sem": DMA((2,)),
            "logit_sem": DMA((3,)),
            "q_send": DMA((2, HALF)),
            "q_recv": DMA((2, HALF)),
            "o_send": DMA((2, HALF)),
            "o_recv": DMA((2, HALF)),
            "g_send": DMA((2, Gather.COPIES)),
            "g_recv": DMA((2, Gather.COPIES)),
            "part": pltpu.VMEM((2, 4, 4, 2, 16, dim), F32),
            "sib": pltpu.VMEM((2, 4, 2, 16, dim), F32),
            "core_in": pltpu.VMEM((4, 4, 2, 16, dim), F32),
            "diag_in": pltpu.VMEM((2, 4, 2, 16, dim), F32),
            "x_in": pltpu.VMEM((2, 4, 2, 16, dim), F32),
            "y_in": pltpu.VMEM((2, 4, 2, 16, dim), F32),
            "z_in": pltpu.VMEM((2, 5, 2, 16, dim - SIDE), F32),
            "side_in": pltpu.VMEM((2, 5, 4, 2, 16, SIDE), F32),
            "r_send": DMA((2, Reduce.COPIES)),
            "r_recv": DMA((2, Reduce.COPIES)),
            "lent": DMA((2,)),
            "free": pltpu.SemaphoreType.REGULAR((4,)),
        }

    def __init__(self, layers, names, *refs):
        for name, ref in zip(self.INPUTS + names, refs, strict=True):
            setattr(self, name, ref)
        here = self.here = Here()
        self.count = layers
        self.dim, self.hidden, self.width = self.h.shape[-1], self.m.shape[-1], self.keys.shape[1]
        self.up_at = self.wide.shape[0] // 2
        self.whole = self.emb_hbm.shape[0] // ROWS * ROWS
        self.loads, self.answered, self.heads, self.fills = {}, set(), 0, 0
        self.stream = {}
        self.loans = Loans(here, self.lent, self.free)
        letters = iter("ABCDEFRSTUJKLM")
        for l in range(layers + 1):
            for t in range(2):
                use = functools.partial(self.project if l < layers else self.head, l, t)
                if l < layers:
                    plane = functools.partial(lambda t, z, c: self.every.at[t, z, c], t)
                else:
                    plane = functools.partial(lambda t, z, c: self.every.at[t, z, :, :, c], t)
                self.stream[next(letters)] = Gather(here, self.h.at[t], plane, self.g_send.at[t], self.g_recv.at[t], use)
        for l in range(layers):
            for t in range(2):
                fill, finish = functools.partial(self.fill, l, t), functools.partial(self.finish, l, t)
                mine = [ref.at[t] for ref in (self.diag_in, self.x_in, self.y_in, self.z_in, self.side_in, self.r_send, self.r_recv)]
                reduce = Reduce(here, fill, finish, self.loans, self.part.at[t], self.sib, self.core_in, *mine)
                reduce.stream = t
                self.stream[next(letters)] = reduce
        for l in range(layers):
            for t in range(2):
                self.stream[next(letters)] = (l, t)

    def load(self, name, l):
        groups = {
            "in": [(self.wg_hbm, self.wide.at[0 : self.hidden]), (self.wu_hbm, self.wide.at[self.up_at : self.up_at + self.hidden]),
                   (self.wq_hbm, self.wq.at[0 : self.width])],
            "out": [(self.wd_hbm, self.wd), (self.wo_hbm, self.wo.at[0 : self.width])],
            "kv": [(self.wkv_hbm, self.wkv), (self.k_hbm, self.keys), (self.v_hbm, self.values)],
        }
        first = {"in": 0, "out": 3, "kv": 5}[name]
        copies = [pltpu.make_async_copy(src.at[l], dst, self.w_sem.at[first + i]) for i, (src, dst) in enumerate(groups[name])]
        for copy in copies:
            copy.start()
        self.loads[name] = copies

    def ready_for(self, name):
        for copy in self.loads.pop(name, ()):
            copy.wait()

    def turned(self, rows, cos, sin):
        half = self.width // 2
        lo, hi = rows[0:half], rows[half : self.width]
        return lo * cos - hi * sin, lo * sin + hi * cos

    def each(self, s, body, own=None):
        if s == 0 and own:
            own(self.here.c, self.here.y * 2 + self.here.x)

        def one(f, carry):
            body(*self.here.partner(s, f))
            return carry

        lax.fori_loop(0 if s else 1, 8, one, 0)

    def trip(self, kind, t, r, src, dst, device):
        sends, recvs = (self.q_send, self.q_recv) if kind == "q" else (self.o_send, self.o_recv)
        return pltpu.make_async_remote_copy(
            src_ref=src, dst_ref=dst, send_sem=sends.at[t, r], recv_sem=recvs.at[t, r], device_id={"tp": device}, device_id_type=MESH
        )

    def arrived(self, sems, t, r):
        ref = self.q_in.at[t, 0, 0]
        pltpu.make_async_copy(ref, ref, sems.at[t, r]).wait()

    def all_arrived(self, t, *sems):
        def one(r, carry):
            for sem in sems:
                self.arrived(sem, t, r)
            return carry

        lax.fori_loop(1, HALF, one, 0)

    def mine(self):
        h = self.here
        return h.z * 2 + h.c, h.y * 2 + h.x

    def project(self, l, t, s):
        self.ready_for("in")
        z, dim = self.here.zs[s], self.dim

        def rows():
            return self.every[t, z].reshape(ROWS, dim)

        q = nt(self.wq[...], rows())
        lo, hi = self.turned(q, self.cos[t, z], self.sin[t, z])
        q = jnp.concatenate([lo, hi, jnp.zeros((LANES - self.width, ROWS), F32)], 0)
        self.q_out[t, z] = q.T.astype(BF16).reshape(2, 4, HALF, LANES)
        zc, quad = self.mine()

        def ask(r, core, four, device):
            self.trip("q", t, r, self.q_out.at[t, z, core, four], self.q_in.at[t, zc, quad], device).start()

        def keep(core, four):
            self.q_in[t, zc, quad] = self.q_out[t, z, core, four]

        self.each(s, ask, keep)

        def tile(n, carry):
            cols = pl.ds(pl.multiple_of(n * ROWS, ROWS), ROWS)
            self.ready[:, cols] = nt(rows(), self.wide[cols])
            return carry

        lax.fori_loop(0, self.wide.shape[0] // ROWS, tile, 0)

        def gated(n, carry):
            some = pl.ds(pl.multiple_of(n * HALF, HALF), HALF)
            gate, up = self.ready[some, 0 : self.hidden], self.ready[some, self.up_at : self.up_at + self.hidden]
            self.m[t, z, some] = (gate * jax.nn.sigmoid(gate) * up).astype(BF16)
            return carry

        lax.fori_loop(0, 8, gated, 0)

    def attend(self, l, t):
        width, half = self.width, self.width // 2
        length = self.keys.shape[-1]
        self.ready_for("kv")
        self.stream["ABCD"[2 * l + t]].drain()
        self.all_arrived(t, self.q_recv, self.q_send)
        rows = nt(self.wkv[...], self.h[t].reshape(HALF, self.dim))
        lo, hi = self.turned(rows, self.cos_own[t], self.sin_own[t])
        blank = jnp.zeros((LANES - width, HALF), BF16)
        new = jnp.concatenate([jnp.concatenate([lo, hi], 0).astype(BF16), blank, rows[width:].astype(BF16), blank], 0)
        self.kv_out[l, t] = new
        self.q_rows[...] = self.q_in[t].reshape(1024, LANES).astype(F32)
        row = lax.broadcasted_iota(jnp.int32, (HALF, length), 0)
        col = lax.broadcasted_iota(jnp.int32, (HALF, length), 1)
        cols = lax.broadcasted_iota(jnp.int32, (width, length), 1)
        blank = jnp.zeros((LANES - width, length), BF16)

        def one(s):
            pos = self.lengths[s] + t
            place = (row == s) & (col == pos)
            at_pos = nn(self.kv_out[l, t], place.astype(F32).astype(BF16)).astype(BF16)
            k = jnp.where(cols == pos, at_pos[0:width], self.keys[s])
            v = jnp.where(cols == pos, at_pos[LANES : LANES + width], self.values[s])
            if t == 0:
                self.keys[s] = k
                self.values[s] = v
            q = self.q_rows[pl.ds(s, HALF, stride=HALF), :].astype(BF16)
            score = nn(q, jnp.concatenate([k, blank], 0)) * width**-0.5
            score = jnp.where(col <= pos, score, -jnp.inf)
            weight = jnp.exp(score - jnp.max(score, axis=-1, keepdims=True))
            weight = (weight / jnp.sum(weight, axis=-1, keepdims=True)).astype(BF16)
            self.o_rows[pl.ds(s, HALF, stride=HALF), :] = nt(weight, jnp.concatenate([v, blank], 0))

        def several(i, carry):
            for u in range(4):
                one(i * 4 + u)
            return carry

        lax.fori_loop(0, 8, several, 0)
        self.o_out[t] = self.o_rows[...].astype(BF16).reshape(8, 4, HALF, LANES)
        zc, quad = self.mine()
        for s in range(4):
            z = self.here.zs[s]

            def answer(r, core, four, device, z=z):
                self.trip("o", t, r, self.o_out.at[t, z * 2 + core, four], self.o_in.at[t, zc, quad], device).start()

            def keep(core, four, z=z):
                self.o_in[t, zc, quad] = self.o_out[t, z * 2 + core, four]

            self.each(s, answer, keep)
        if t and l + 1 < self.count:
            self.load("in", l + 1)
            self.load("kv", l + 1)

    def fill(self, l, t, s, core, ref):
        self.ready_for("out")
        if (l, t, s) not in self.answered:
            self.answered.add((l, t, s))
            self.each(s, lambda r, core, four, device: self.arrived(self.o_recv, t, r))
        z = self.here.zs[s]
        some = pl.ds(pl.multiple_of(core * LANES, LANES), LANES)

        def columns(n, carry):
            cols = pl.ds(pl.multiple_of(n * ROWS, ROWS), ROWS)
            rows = nn(self.o_in[t, z * 2 + core].reshape(LANES, LANES), self.wo[:, cols]) + nn(self.m[t, z, some], self.wd[:, cols])
            ref[:, :, :, cols] = rows.reshape(4, 2, 16, ROWS)
            return carry

        lax.fori_loop(0, self.dim // ROWS, columns, 0)
        self.fills += 1
        if self.fills == 16 * (l + 1) and l + 1 < self.count:
            self.load("out", l + 1)

    def finish(self, l, t, half, lo, rows):
        x = (self.x[t, half].astype(F32) + rows).astype(BF16)
        self.x[t, half] = x
        self.h[t, half] = normed(x, self.gains[pl.ds(l, 1)])

    def tile(self, i):
        at = lax.rem(i, 2)
        return pltpu.make_async_copy(self.emb_hbm.at[pl.ds(pl.multiple_of(i * ROWS, ROWS), ROWS)], self.tiles.at[at], self.tile_sem.at[at])

    def store(self, t, z, i):
        at = lax.rem(i, 2)
        rows, cols = pl.ds(pl.multiple_of(i * ROWS, ROWS), ROWS), pl.ds(pl.multiple_of(z * ROWS, ROWS), ROWS)
        return pltpu.make_async_copy(self.logits.at[at], self.out_hbm.at[t, rows, cols], self.logit_sem.at[at])

    def store_last(self, t, z):
        rows, cols = pl.ds(self.whole, TAIL), pl.ds(pl.multiple_of(z * ROWS, ROWS), ROWS)
        return pltpu.make_async_copy(self.last, self.out_hbm.at[t, rows, cols], self.logit_sem.at[2])

    def head(self, l, t, s):
        z, dim, count = self.here.zs[s], self.dim, self.whole // ROWS
        first, final = self.heads == 0, self.heads == 7
        self.heads += 1

        def rows():
            return self.every[t, z].reshape(ROWS, dim)

        if not first:
            self.store_last(t, z).wait()
        self.last[...] = nt(self.emb_tail[...], rows()) * dim**-0.5
        self.store_last(t, z).start()

        def one(i, carry):
            more = lax.rem(i + 1, count)

            @pl.when((i + 1 < count) if final else (i >= 0))
            def _():
                self.tile(more).start()

            self.tile(i).wait()

            @pl.when((i >= 2) if first else (i >= 0))
            def _():
                self.store(t, z, i).wait()

            self.logits[lax.rem(i, 2)] = nt(self.tiles[lax.rem(i, 2)], rows()) * dim**-0.5
            self.store(t, z, i).start()
            return carry

        lax.fori_loop(0, count, one, 0)
        if final:
            self.store(t, z, 0).wait()
            self.store(t, z, 1).wait()
            self.store_last(t, z).wait()

    def run(self, order):
        h = self.here
        for name in ("in", "kv", "out"):
            self.load(name, 0)
        self.tile(0).start()
        self.h[...] = self.h_ref[...].reshape(self.h.shape)
        self.x[...] = self.x_ref[...].reshape(self.x.shape)
        self.wq[self.width : LANES] = jnp.zeros((LANES - self.width, self.dim), BF16)
        self.wo[self.width : LANES] = jnp.zeros((LANES - self.width, self.dim), BF16)
        for at in (0, self.up_at):
            self.wide[at + self.hidden : at + self.up_at] = jnp.zeros((self.up_at - self.hidden, self.dim), BF16)
        meet([h.dev(z, *f) for _, z, f in h.all()])
        placed = set()
        for word in " ".join(order).split():
            who, step = self.stream[word[0]], word[1:].rstrip(DIGITS)
            if step == "att":
                self.attend(*who)
                continue
            if isinstance(who, Gather) and who not in placed:
                placed.add(who)
                t = "ABCDEF".index(word[0]) % 2
                self.every[(t, h.z, *((h.y, h.x, h.c) if word[0] in "EF" else (h.c, h.y, h.x)))] = self.h[t]
            getattr(who, step)(*(int(n) for n in word[1 + len(step) :]))
            if step == "end":
                who.drain()
                self.all_arrived(who.stream, self.o_send)
        for letter in "EF":
            self.stream[letter].drain()
        self.loans.settle()


def layers_kernel(layers, names, *refs):
    Layers(layers, names, *refs).run(ORDER)


def relayout_kernel(in_ref, out_ref):
    for t in range(2):
        out_ref[:, t, :] = in_ref[t]


def params(index, mib):
    return pltpu.CompilerParams(collective_id=index, has_side_effects=True, vmem_limit_bytes=mib << 20)


def solution(mesh):
    def device_fn(tokens, lengths, embedding, ln_scale, w_q, w_kv, w_o, w_gate, w_up, w_down, final_scale, k_cache, v_cache):
        me = lax.axis_index("tp")
        steps, batch = tokens.shape
        vocab, dim = embedding.shape
        layers, seqs, length, width = k_cache.shape
        hidden = w_gate.shape[-1]
        half = width // 2
        block = jax.ShapeDtypeStruct((2, HALF, dim), BF16)

        def ordered(rows):
            return rows.reshape(2, 4, 2, 2, 2, HALF).transpose(0, 1, 4, 2, 3, 5).reshape(2, 4, 2, LANES)

        positions = lengths[None, :] + jnp.arange(steps, dtype=jnp.int32)[:, None]
        own_len = lax.dynamic_slice_in_dim(lengths, me * seqs, seqs)
        own_pos = own_len[None, :] + jnp.arange(steps, dtype=jnp.int32)[:, None]
        inv_freq = 10000.0 ** (-jnp.arange(half, dtype=F32) / half)
        angles = ordered(positions).reshape(2, 4, 1, ROWS).astype(F32) * inv_freq[None, None, :, None]
        own_angles = own_pos[:, None, :].astype(F32) * inv_freq[None, :, None]
        tok = ordered(tokens).reshape(2, 4, 2, 4, HALF).transpose(1, 2, 3, 0, 4).reshape(8, ROWS, 1)
        turns = jnp.cos(angles), jnp.sin(angles), jnp.cos(own_angles), jnp.sin(own_angles)
        gains = jnp.concatenate([ln_scale[1:], final_scale[None]], 0)

        x, h = pl.pallas_call(
            embed_kernel,
            out_shape=(block, block),
            in_specs=[VMEM, ANY, VMEM],
            out_specs=(VMEM, VMEM),
            scratch_shapes=[pltpu.VMEM((vocab, dim), BF16), pltpu.VMEM((LANES, dim), BF16), DMA((1,)), *Reduce.scratch(HALF, dim, BF16)],
            compiler_params=params(0, 60),
            name="embed",
        )(tok, embedding, ln_scale[:1])

        wg_t, wu_t, wkv_t = (w.transpose(0, 2, 1) for w in (w_gate, w_up, w_kv))
        wq_t = w_q.transpose(0, 2, 3, 1).reshape(layers, width, dim)
        wo = w_o.reshape(layers, width, dim)
        k_t, v_t = k_cache.transpose(0, 1, 3, 2), v_cache.transpose(0, 1, 3, 2)
        padded = pl.cdiv(vocab, 8) * 8
        tail = jnp.pad(embedding[vocab // ROWS * ROWS :], ((0, padded - vocab), (0, 0)))
        scratch = Layers.scratch(dim, hidden, width, seqs, length)
        logits, fresh = pl.pallas_call(
            functools.partial(layers_kernel, layers, tuple(scratch)),
            out_shape=(jax.ShapeDtypeStruct((2, padded, batch), F32), jax.ShapeDtypeStruct((layers, 2, ROWS, HALF), BF16)),
            in_specs=[SMEM] + [VMEM] * 8 + [ANY] * 9,
            out_specs=(ANY, VMEM),
            scratch_shapes=list(scratch.values()),
            compiler_params=params(1, 63),
            name="layers",
        )(own_len, x, h, gains, *turns, tail, wg_t, wu_t, wq_t, wkv_t, w_down, wo, k_t, v_t, embedding)
        logits = pl.pallas_call(
            relayout_kernel,
            grid=(pl.cdiv(vocab, LANES),),
            out_shape=jax.ShapeDtypeStruct((vocab, 2, batch), F32),
            in_specs=[pl.BlockSpec((2, LANES, batch), lambda i: (0, i, 0))],
            out_specs=pl.BlockSpec((LANES, 2, batch), lambda i: (i, 0, 0)),
            name="relayout",
        )(logits)

        row_ids = lax.broadcasted_iota(jnp.int32, (1, 1, length, 1), 2)
        new = fresh.reshape(layers, 2, 2, LANES, HALF)[:, :, :, :width]

        def written(cache, which):
            for t in range(steps):
                cache = jnp.where(
                    row_ids == own_pos[t][None, :, None, None], new[:, t, which].transpose(0, 2, 1)[:, :, None, :], cache
                )
            return cache

        return logits.transpose(1, 2, 0), written(k_cache, 0), written(v_cache, 1)

    cache_spec = P(None, "tp", None, None)
    in_specs = (P(), P(), P("tp", None), P(), P(None, None, "tp", None), P(), P(None, "tp", None, None), P(None, None, "tp"), P(None, None, "tp"), P(None, "tp", None), P(), cache_spec, cache_spec)
    out_specs = (P(None, None, "tp"), cache_spec, cache_spec)
    return jax.shard_map(device_fn, mesh=mesh, in_specs=in_specs, out_specs=out_specs, check_vma=False)
```

```python
import functools

import jax
import jax.numpy as jnp
from jax import lax
from jax.experimental import pallas as pl
from jax.experimental.pallas import tpu as pltpu
from jax.sharding import PartitionSpec as P

LN_EPS = 1e-6
TWO, FOUR = 2, 4
HALF, BLOCK, ROWS, LANES = 32, 64, 256, 128
MESH = pl.DeviceIdType.MESH
BF16, F32 = jnp.bfloat16, jnp.float32
ANY = pl.BlockSpec(memory_space=pl.ANY)
VMEM = pl.BlockSpec(memory_space=pltpu.VMEM)
SMEM = pl.BlockSpec(memory_space=pltpu.SMEM)
DMA = pltpu.SemaphoreType.DMA
FLIPS = [(a, b, e) for a in range(TWO) for b in range(TWO) for e in range(TWO)]
SIDE = 512
ALL = (slice(None),) * 3
CODES = "0123456789abcdefghijklmnopqrstuvwxyz"
STREAMS = "ABCDEFRSTUJKLM"


def numbered(words, slots):
    return tuple(f"{word}{s}" for word in words for s in slots)


TAIL = 40
WIDE = 512
SHEET = 264
REDUCE = "372bfu6ae1tnj59sd0mi48rxylhqcwpvgkoz"
ORDER = (
    "A0AqBqB0AkA1A8AlBlA4B8B4A5BkA2B1AmA3AcA9ArBmB2AaBcBrA6B9AoAn",
    "AdB3B5A7BoAhBnBaAbB6AeBgApAiB7BdBpAfAgBeBbAjBiBfBhBjJ0K0R2R6",
    "RaReS2R3R7S6SaRiRmSeRtRbRfS3S7R1RuSbR5SfR0StRnR9RjRdS1S5SuR4",
    "SiR8SmSnSjRqS9SdRsRwSsS0S4RlSrRyRhRrRcRxSqS8ShSlSxSyRpRgRkSc",
    "SwRvSpRoSvSgSkRzCqC0ClC2CkC1SoSzC8C4DqD0DlCcCrC9C5D2D8D4DkCa",
    "CdC6D1CmCoD6DcC3CnDrD5DaD9DmCeD3ChCiC7CbCgDoDdCpDgDnCfDbD7De",
    "DhCjDfDiDpDjL0T2M0T6TaTeT3T7U2TbTmTfTtTiU6UaUeU3TuU7T1TnUbTj",
    "T0UuUfT4T5T9T8U1TsU5TqTdU0U9UtUiUjUsThUnUmU4UdTyTwTrTlTcUhTx",
    "UrUqUlU8UxUyTgTkUcTpUwTvUpUvToUkUgTzEqE0UoElE2UzEkE8FqE4F0Ec",
    "E1E6EmErEaEgF8FkF4EoE3E5FlE9F1FcFmEeF2FrEbE7F3EnEdFgF5EiEpEf",
    "F6F9FaEhF7FbFoFnFdEjFeFfFhFpFiFj",
)


class Here:
    def __init__(self):
        me = lax.axis_index("tp")
        self.c = lax.rem(me, TWO)
        self.x = lax.rem(lax.div(me, TWO), TWO)
        self.y = lax.rem(lax.div(me, FOUR), TWO)
        z = lax.div(me, 8)
        self.z = z
        self.against = {id(v): 1 - v for v in (self.c, self.x, self.y)}
        inner = lax.rem(lax.div(z + 1, TWO), TWO)
        self.inner = inner == 1
        two, three = lax.rem(z + TWO, FOUR), 3 - z
        self.zs = [z, z + 1 - TWO * lax.rem(z, TWO), inner * three + (1 - inner) * two, inner * two + (1 - inner) * three]
        self.slot = ((z * TWO + self.c) * TWO + self.y) * TWO + self.x
        self.near, self.across = self.dev(self.zs[1]), self.dev(three)
        self.core, self.along_x, self.along_y = self.dev(z, a=1), self.dev(z, e=1), self.dev(z, b=1)

    def flip(self, v, on):
        return self.against[id(v)] if on else v

    def dev(self, z, a=0, b=0, e=0):
        y, x, c = self.flip(self.y, b), self.flip(self.x, e), self.flip(self.c, a)
        return ((z * TWO + y) * TWO + x) * TWO + c

    def apart(self, s):
        inner = lax.rem(lax.div(self.z + 1, TWO), TWO)
        return (0, 1, TWO + inner, 3 - inner)[s]

    def partner(self, s, f):
        a, b, e = lax.div(f, FOUR), lax.rem(lax.div(f, TWO), TWO), lax.rem(f, TWO)
        c, y, x = (on + v - TWO * on * v for on, v in ((a, self.c), (b, self.y), (e, self.x)))
        return self.apart(s) * 8 + f, c, y * TWO + x, ((self.zs[s] * TWO + y) * TWO + x) * TWO + c

    def lines(self):
        return [self.near, self.dev(self.zs[TWO]), self.dev(self.zs[3]), self.core, self.along_x, self.along_y]

    def all(self):
        z = self.z
        zs = [z, self.zs[1], lax.rem(z + TWO, FOUR), 3 - z]
        return [(8 * j + FOUR * a + TWO * b + e, zs[j], (a, b, e)) for j in range(FOUR) for a, b, e in FLIPS if j or a or b or e]


def meet(devices):
    sem = pltpu.get_barrier_semaphore()
    for d in devices:
        pl.semaphore_signal(sem, inc=1, device_id={"tp": d}, device_id_type=MESH)
    pl.semaphore_wait(sem, len(devices))


class Wires:
    def __init__(self, here, send, recv, sizes):
        self.here, self.send, self.recv = here, send, recv
        self.names, self.first, self.started, at = {}, {}, {}, 0
        for kind, count in sizes.items():
            self.first[kind], self.started[kind] = at, []
            at += count

    def go(self, what, src, dst, device, inner=None):
        kind = tuple(src.shape), inner
        k = self.names.setdefault(what, len(self.names))
        copy = pltpu.make_async_remote_copy(
            src_ref=src,
            dst_ref=dst,
            send_sem=self.send.at[self.first[kind] + len(self.started[kind])],
            recv_sem=self.recv.at[k],
            device_id={"tp": device},
            device_id_type=MESH,
        )
        self.started[kind].append(src)
        if inner is None:
            copy.start()
        else:
            pl.when(self.here.inner == inner)(copy.start)

    def got(self, what, like):
        k = self.names.setdefault(what, len(self.names))
        pltpu.make_async_copy(like, like, self.recv.at[k]).wait()

    def step(self, code):
        name = self.STEPS[CODES.index(code)]
        word = name.rstrip(CODES[:FOUR])
        getattr(self, word)(*map(int, name[len(word) :]))

    def run(self, order):
        for code in "".join(order):
            self.step(code)

    def drain(self):
        for (kind, inner), copies in self.started.items():

            def wait(ref=copies[0], first=self.first[kind, inner], count=len(copies)):
                def one(i, carry):
                    pltpu.make_async_copy(ref, ref, self.send.at[first + i]).wait()
                    return carry

                lax.fori_loop(0, count, one, 0)

            if inner is None:
                wait()
            else:
                pl.when(self.here.inner == inner)(wait)


def nt(a, b):
    return lax.dot_general(a, b, (((1,), (1,)), ((), ())), preferred_element_type=F32)


def nn(a, b):
    return lax.dot_general(a, b, (((1,), (0,)), ((), ())), preferred_element_type=F32)


class Gather(Wires):
    COPIES = 48
    STEPS = numbered(("sh", "tx", "ty", "cl", "us"), range(FOUR)) + numbered(("zf", "ff"), range(1, FOUR)) + ("zown", "fown")

    def __init__(self, here, own, plane, send, recv, use):
        rows, dim = own.shape[1:]
        main, four = ((TWO, rows, dim - SIDE)), (TWO, TWO, TWO, rows, SIDE)
        sizes = {(main, None): 19, (main, True): FOUR, ((TWO, rows, dim), None): 6, (four, None): FOUR, (four, True): FOUR}
        super().__init__(here, send, recv, sizes | {(main[1:], None): 6, ((rows, dim), None): TWO})
        self.own, self.plane, self.use = own, plane, use
        self.main, self.side, self.full = pl.ds(0, dim - SIDE), pl.ds(dim - SIDE, SIDE), pl.ds(0, dim)

    def at(self, s, b=0, e=0):
        h = self.here
        return self.plane(h.zs[s], h.c).at[h.flip(h.y, b), h.flip(h.x, e)].at[:, :, self.main if s else self.full]

    def fours(self, s):
        return self.plane(self.here.zs[s], self.here.c).at[:, :, :, :, self.side]

    def pass_on(self, what, s, ref):
        h = self.here
        self.go((what, 3 if s == 1 else s), ref, ref, h.across if s == 1 else h.near, True)

    def zown(self):
        h = self.here
        src, dst = self.own.at[:, :, self.main], self.at(0).at[:, :, self.main]
        self.go(("z", 1), src, dst, h.near)
        self.go(("z", TWO), src, dst, h.across, True)

    def zf(self, s):
        self.got(("z", s), self.at(s))
        self.pass_on("z", s, self.at(s))

    def fown(self):
        h, ref = self.here, self.fours(0)
        self.go(("f", 1), ref, ref, h.near)
        self.go(("f", TWO), ref, ref, h.across, True)

    def ff(self, s):
        ref = self.fours(s)
        self.got(("f", s), ref)
        self.pass_on("f", s, ref)
        self.go(("cf", s), ref, ref, self.here.core)

    def sh(self, s):
        h, dst = self.here, self.at(s)
        src = dst if s else self.own
        self.go(("x", s), src, dst, h.along_x)
        self.go(("y", s), src, dst, h.along_y)
        self.go(("c", s), src, dst, h.core)

    def tx(self, s):
        ref = self.at(s, e=1)
        self.got(("x", s), ref)
        self.go(("xy", s), ref.at[0], ref.at[0], self.here.along_y)
        self.go(("cx", s), ref, ref, self.here.core)

    def ty(self, s):
        ref = self.at(s, b=1)
        self.got(("y", s), ref)
        self.go(("yx", s), ref.at[1], ref.at[1], self.here.along_x)
        self.go(("cy", s), ref, ref, self.here.core)

    def cl(self, s):
        ref = self.at(s, 1, 1)
        self.got(("xy", s), ref.at[0])
        self.got(("yx", s), ref.at[1])
        self.go(("cd", s), ref, ref, self.here.core)

    def us(self, s):
        for what in ("c", "cx", "cy", "cd"):
            self.got((what, s), self.at(s))
        if s:
            self.got(("cf", s), self.fours(s))
        self.use(s)


class Loans:
    def __init__(self, here, send, free):
        self.here, self.send, self.free = here, send, free
        self.lent, self.out = [], set()

    def take(self, s):
        if s in self.out:
            pl.semaphore_wait(self.free.at[s], 1)
        self.out.add(s)

    def give(self, s):
        pl.semaphore_signal(self.free.at[s], inc=1, device_id={"tp": self.here.core}, device_id_type=MESH)

    def settle(self):
        for copy in self.lent[-TWO:]:
            copy.wait_send()
        for s in self.out:
            pl.semaphore_wait(self.free.at[s], 1)


class Reduce(Wires):
    COPIES = 48
    STEPS = numbered(("fo", "fm", "ca", *"dpqu"), range(FOUR)) + numbered(("fz", "gz"), range(1, FOUR)) + ("fin", "end")

    @staticmethod
    def scratch(rows, dim, dtype):
        return [
            pltpu.VMEM((FOUR, FOUR, TWO, rows, dim), dtype),
            pltpu.VMEM((TWO, FOUR, TWO, rows, dim), dtype),
            pltpu.VMEM((FOUR, FOUR, TWO, rows, dim), dtype),
            pltpu.VMEM((FOUR, TWO, rows, dim), dtype),
            pltpu.VMEM((FOUR, TWO, rows, dim), dtype),
            pltpu.VMEM((FOUR, TWO, rows, dim), dtype),
            pltpu.VMEM((5, TWO, rows, dim - SIDE), dtype),
            pltpu.VMEM((5, FOUR, TWO, rows, SIDE), dtype),
            DMA((Reduce.COPIES,)),
            DMA((Reduce.COPIES,)),
            DMA((TWO,)),
            pltpu.SemaphoreType.REGULAR((FOUR,)),
        ]

    def __init__(self, here, fill, finish, loans, part, sib, core_in, diag_in, x_in, y_in, z_in, side_in, send, recv):
        rows, dim = part.shape[3:]
        main, four = (TWO, rows, dim - SIDE), (FOUR, TWO, rows, SIDE)
        sizes = {(main[1:], None): 18, ((rows, dim), None): 6, (four, True): 3, (four, False): 3, (main, True): 3, (main, False): 3}
        super().__init__(here, send, recv, sizes)
        self.fill, self.finish, self.loans = fill, finish, loans
        self.part, self.sib, self.core_in, self.diag_in = part, sib, core_in, diag_in
        self.x_in, self.y_in, self.z_in, self.side_in = x_in, y_in, z_in, side_in
        dim = part.shape[-1]
        self.main, self.side, self.full = pl.ds(0, dim - SIDE), pl.ds(dim - SIDE, SIDE), pl.ds(0, dim)

    def quad(self, b, e):
        h = self.here
        return h.flip(h.y, b) * TWO + h.flip(h.x, e)

    def piece(self, buf, s, *where):
        return buf, (s, *where, slice(None), self.main if s else self.full)

    def add(self, ref, *more):
        buf, index = ref
        total = buf[index]
        for other, where in more:
            total = total + other[where]
        buf[index] = total

    def fo(self, s):
        loans, n = self.loans, len(self.loans.lent)
        if n > 1:
            loans.lent[n - TWO].wait_send()
        self.fill(s, self.here.flip(self.here.c, 1), self.sib.at[n % TWO])
        loans.take(s)
        k = self.names.setdefault(("c", s), len(self.names))
        copy = pltpu.make_async_remote_copy(
            src_ref=self.sib.at[n % TWO],
            dst_ref=self.core_in.at[s],
            send_sem=loans.send.at[n % TWO],
            recv_sem=self.recv.at[k],
            device_id={"tp": self.here.core},
            device_id_type=MESH,
        )
        copy.start()
        loans.lent.append(copy)

    def fm(self, s):
        self.fill(s, self.here.c, self.part.at[s])

    def ca(self, s):
        self.got(("c", s), self.core_in.at[s])
        for t in range(TWO):

            def add(i, carry):
                self.add((self.part, (s, i, t)), (self.core_in, (s, i, t)))
                return carry

            lax.fori_loop(0, FOUR, add, 0)
        self.loans.give(s)

    def along_z(self, what, s, ref, landing):
        h = self.here
        k = 5 if s == 1 else s
        to = 1 if s == 1 else s + TWO

        @pl.when(h.inner)
        def _():
            self.got((what, k), landing.at[k - 1])
            self.add(ref, (landing, k - 1))

        self.go((what, to), ref[0].at[ref[1]], landing.at[to - 1], h.near if s == 1 else h.across, True)
        self.go((what, s), ref[0].at[ref[1]], landing.at[s - 1], h.near, False)

    def last_z(self, what, ref, landing):
        self.got((what, 1), landing.at[0])
        self.add(ref, (landing, 0))

        @pl.when(self.here.inner)
        def _():
            self.got((what, FOUR), landing.at[3])
            self.add(ref, (landing, 3))

    def fz(self, s):
        self.along_z("f", s, (self.part, (s, *ALL, self.side)), self.side_in)

    def fin(self):
        self.last_z("f", (self.part, (0, *ALL, self.side)), self.side_in)

    def d(self, s):
        h, part = self.here, self.part
        far = self.quad(1, 1)
        self.pass_on("dy", s, self.piece(part, s, far, 0), self.piece(self.diag_in, s, 0), h.along_y)
        self.pass_on("dx", s, self.piece(part, s, far, 1), self.piece(self.diag_in, s, 1), h.along_x)
        self.pass_on("x1", s, self.piece(part, s, self.quad(0, 1), 1), self.piece(self.x_in, s, 1), h.along_x)
        self.pass_on("y0", s, self.piece(part, s, self.quad(1, 0), 0), self.piece(self.y_in, s, 0), h.along_y)

    def pass_on(self, what, s, src, dst, device):
        self.go((what, s), src[0].at[src[1]], dst[0].at[dst[1]], device)

    def came(self, what, s, ref):
        self.got((what, s), ref[0].at[ref[1]])

    def p(self, s):
        ref = self.piece(self.part, s, self.quad(0, 1), 0)
        self.came("dy", s, ref)
        self.add(ref, self.piece(self.diag_in, s, 0))
        self.pass_on("x0", s, ref, self.piece(self.x_in, s, 0), self.here.along_x)

    def q(self, s):
        ref = self.piece(self.part, s, self.quad(1, 0), 1)
        self.came("dx", s, ref)
        self.add(ref, self.piece(self.diag_in, s, 1))
        self.pass_on("y1", s, ref, self.piece(self.y_in, s, 1), self.here.along_y)

    def u(self, s):
        for t in range(TWO):
            ref = self.piece(self.part, s, self.quad(0, 0), t)
            self.came(f"x{t}", s, ref)
            self.came(f"y{t}", s, ref)
            self.add(ref, self.piece(self.x_in, s, t), self.piece(self.y_in, s, t))

    def gz(self, s):
        self.along_z("g", s, (self.part, (s, self.quad(0, 0), *ALL[:TWO], self.main)), self.z_in)

    def end(self):
        mine = self.quad(0, 0)
        self.last_z("g", (self.part, (0, mine, *ALL[:TWO], self.main)), self.z_in)
        for t in range(TWO):
            for lo in range(0, self.part.shape[3], 16):
                self.finish(t, lo, self.part[0, mine, t, lo : lo + 16])


def normed(x, gain):
    rows = x.astype(F32)
    centred = rows - jnp.mean(rows, axis=-1, keepdims=True)
    var = jnp.mean(centred * centred, axis=-1, keepdims=True)
    return (centred * lax.rsqrt(var + LN_EPS) * gain).astype(BF16)


def load(pairs, sems):
    copies = [pltpu.make_async_copy(src, dst, sems.at[i]) for i, (src, dst) in enumerate(pairs)]
    for copy in copies:
        copy.start()
    return copies


def embed_kernel(tok_ref, emb_hbm, gain_ref, x_ref, h_ref, emb, tail, sem, *scratch):
    here = Here()
    vocab, dim = emb_hbm.shape
    whole = vocab // ROWS * ROWS
    rest = vocab - whole
    (fetch,) = load([(emb_hbm, emb)], sem)
    meet(here.lines())
    fetch.wait()
    tail[...] = jnp.zeros_like(tail)
    tail[0:rest] = emb[whole:vocab]
    base = lax.axis_index("tp") * vocab

    def fill(s, core, ref):
        tok = tok_ref[here.zs[s] * TWO + core] - base
        hot = (tok == lax.broadcasted_iota(jnp.int32, (ROWS, whole), 1)).astype(F32).astype(BF16)
        hot_tail = (tok == lax.broadcasted_iota(jnp.int32, (ROWS, LANES), 1) + whole).astype(F32).astype(BF16)

        def columns(n, carry):
            cols = pl.ds(pl.multiple_of(n * ROWS, ROWS), ROWS)
            rows = nn(hot, emb[0:whole, cols]) + nn(hot_tail, tail[:, cols])
            ref[:, :, :, cols] = rows.astype(BF16).reshape(FOUR, TWO, HALF, ROWS)
            return carry

        lax.fori_loop(0, dim // ROWS, columns, 0)

    def finish(t, lo, rows):
        x_ref[t, lo : lo + 16] = rows
        h_ref[t, lo : lo + 16] = normed(rows, gain_ref[...])

    *rs, lent, free = scratch
    loans = Loans(here, lent, free)
    red = Reduce(here, fill, finish, loans, *rs)
    red.run(REDUCE)
    red.drain()
    loans.settle()


class Layers:
    @staticmethod
    def scratch(dim, hidden, width, seqs, length):
        up_at = pl.cdiv(hidden, LANES) * LANES
        return dict(
            x=pltpu.VMEM((TWO, TWO, 16, dim), BF16),
            h=pltpu.VMEM((TWO, TWO, 16, dim), BF16),
            every=pltpu.VMEM((TWO, FOUR, TWO, TWO, TWO, TWO, 16, dim), BF16),
            wide=pltpu.VMEM((TWO * up_at, dim), BF16),
            wq=pltpu.VMEM((LANES, dim), BF16),
            wkv=pltpu.VMEM((TWO * width, dim), BF16),
            wd=pltpu.VMEM((hidden, dim), BF16),
            wo=pltpu.VMEM((LANES, dim), BF16),
            ready=pltpu.VMEM((ROWS, TWO * up_at), F32),
            m=pltpu.VMEM((TWO, FOUR, ROWS, hidden), BF16),
            q_out=pltpu.VMEM((TWO, FOUR, TWO, FOUR, HALF, LANES), BF16),
            q_in=pltpu.VMEM((TWO, 8, FOUR, HALF, LANES), BF16),
            o_out=pltpu.VMEM((TWO, 8, FOUR, HALF, LANES), BF16),
            o_in=pltpu.VMEM((TWO, 8, FOUR, HALF, LANES), BF16),
            q_rows=pltpu.VMEM((1024, LANES), F32),
            o_rows=pltpu.VMEM((1024, LANES), F32),
            keys=pltpu.VMEM((seqs, width, length), BF16),
            values=pltpu.VMEM((seqs, width, length), BF16),
            tiles=pltpu.VMEM((TWO, ROWS, dim), BF16),
            logits=pltpu.VMEM((TWO, ROWS, ROWS), F32),
            last=pltpu.VMEM((TAIL, ROWS), F32),
            w_sem=DMA((8,)),
            tile_sem=DMA((TWO,)),
            logit_sem=DMA((3,)),
            q_send=DMA((TWO, HALF)),
            q_recv=DMA((TWO, HALF)),
            o_send=DMA((TWO, HALF)),
            o_recv=DMA((TWO, HALF)),
            g_send=DMA((TWO, Gather.COPIES)),
            g_recv=DMA((TWO, Gather.COPIES)),
            part=pltpu.VMEM((TWO, FOUR, FOUR, TWO, 16, dim), F32),
            sib=pltpu.VMEM((TWO, FOUR, TWO, 16, dim), F32),
            core_in=pltpu.VMEM((FOUR, FOUR, TWO, 16, dim), F32),
            diag_in=pltpu.VMEM((TWO, FOUR, TWO, 16, dim), F32),
            x_in=pltpu.VMEM((TWO, FOUR, TWO, 16, dim), F32),
            y_in=pltpu.VMEM((TWO, FOUR, TWO, 16, dim), F32),
            z_in=pltpu.VMEM((TWO, 5, TWO, 16, dim - SIDE), F32),
            side_in=pltpu.VMEM((TWO, 5, FOUR, TWO, 16, SIDE), F32),
            r_send=DMA((TWO, Reduce.COPIES)),
            r_recv=DMA((TWO, Reduce.COPIES)),
            lent=DMA((TWO,)),
            free=pltpu.SemaphoreType.REGULAR((FOUR,)),
        )

    def __init__(self, layers, **refs):
        self.__dict__.update(refs)
        here = self.here = Here()
        self.count = layers
        self.dim, self.hidden, self.width = self.h.shape[-1], self.m.shape[-1], self.keys.shape[1]
        self.up_at = self.wide.shape[0] // TWO
        self.whole = self.emb_hbm.shape[0] // ROWS * ROWS
        self.loads, self.answered, self.heads, self.fills = {}, set(), 0, 0
        self.stream = {}
        self.loans = Loans(here, self.lent, self.free)
        letters = iter(STREAMS)
        for l in range(layers + 1):
            for t in range(TWO):
                use = functools.partial(self.project if l < layers else self.head, l, t)
                if l < layers:
                    plane = functools.partial(lambda t, z, c: self.every.at[t, z, c], t)
                else:
                    plane = functools.partial(lambda t, z, c: self.every.at[t, z, :, :, c], t)
                self.stream[next(letters)] = Gather(here, self.h.at[t], plane, self.g_send.at[t], self.g_recv.at[t], use)
        for l in range(layers):
            for t in range(TWO):
                fill, finish = functools.partial(self.fill, l, t), functools.partial(self.finish, l, t)
                mine = [ref.at[t] for ref in (self.diag_in, self.x_in, self.y_in, self.z_in, self.side_in, self.r_send, self.r_recv)]
                reduce = Reduce(here, fill, finish, self.loans, self.part.at[t], self.sib, self.core_in, *mine)
                self.stream[next(letters)] = reduce
        for l in range(layers):
            for t in range(TWO):
                self.stream[next(letters)] = (l, t)

    def load(self, name, l):
        groups = {
            "in": [(self.wg_hbm, self.wide.at[0 : self.hidden]), (self.wu_hbm, self.wide.at[self.up_at : self.up_at + self.hidden]),
                   (self.wq_hbm, self.wq.at[0 : self.width])],
            "out": [(self.wd_hbm, self.wd), (self.wo_hbm, self.wo.at[0 : self.width])],
            "kv": [(self.wkv_hbm, self.wkv), (self.k_hbm, self.keys), (self.v_hbm, self.values)],
        }
        first = {"in": 0, "out": 3, "kv": 5}[name]
        copies = [pltpu.make_async_copy(src.at[l], dst, self.w_sem.at[first + i]) for i, (src, dst) in enumerate(groups[name])]
        for copy in copies:
            copy.start()
        self.loads[name] = copies

    def ready_for(self, name):
        for copy in self.loads.pop(name, ()):
            copy.wait()

    def turned(self, rows, cos, sin):
        half = self.width // TWO
        lo, hi = rows[0:half], rows[half : self.width]
        return lo * cos - hi * sin, lo * sin + hi * cos

    def each(self, s, body, own=None):
        if s == 0 and own:
            own(self.here.c, self.here.y * TWO + self.here.x)

        def one(f, carry):
            body(*self.here.partner(s, f))
            return carry

        lax.fori_loop(0 if s else 1, 8, one, 0)

    def trip(self, kind, t, r, src, dst, device):
        sends, recvs = (self.q_send, self.q_recv) if kind == "q" else (self.o_send, self.o_recv)
        return pltpu.make_async_remote_copy(
            src_ref=src, dst_ref=dst, send_sem=sends.at[t, r], recv_sem=recvs.at[t, r], device_id={"tp": device}, device_id_type=MESH
        )

    def arrived(self, sems, t, r):
        ref = self.q_in.at[t, 0, 0]
        pltpu.make_async_copy(ref, ref, sems.at[t, r]).wait()

    def all_arrived(self, t, *sems):
        def one(r, carry):
            for sem in sems:
                self.arrived(sem, t, r)
            return carry

        lax.fori_loop(1, HALF, one, 0)

    def mine(self):
        h = self.here
        return h.z * TWO + h.c, h.y * TWO + h.x

    def project(self, l, t, s):
        self.ready_for("in")
        z, dim = self.here.zs[s], self.dim

        def rows():
            return self.every[t, z].reshape(ROWS, dim)

        q = nt(self.wq[...], rows())
        lo, hi = self.turned(q, self.cos[t, z], self.sin[t, z])
        q = jnp.concatenate([lo, hi, jnp.zeros((LANES - self.width, ROWS), F32)], 0)
        self.q_out[t, z] = q.T.astype(BF16).reshape(TWO, FOUR, HALF, LANES)
        zc, quad = self.mine()

        def ask(r, core, four, device):
            self.trip("q", t, r, self.q_out.at[t, z, core, four], self.q_in.at[t, zc, quad], device).start()

        def keep(core, four):
            self.q_in[t, zc, quad] = self.q_out[t, z, core, four]

        self.each(s, ask, keep)

        def tile(n, carry):
            cols = pl.ds(pl.multiple_of(n * ROWS, ROWS), ROWS)
            self.ready[:, cols] = nt(rows(), self.wide[cols])
            return carry

        lax.fori_loop(0, self.wide.shape[0] // ROWS, tile, 0)

        def gated(n, carry):
            some = pl.ds(pl.multiple_of(n * HALF, HALF), HALF)
            gate, up = self.ready[some, 0 : self.hidden], self.ready[some, self.up_at : self.up_at + self.hidden]
            self.m[t, z, some] = (gate * jax.nn.sigmoid(gate) * up).astype(BF16)
            return carry

        lax.fori_loop(0, 8, gated, 0)

    def attend(self, l, t):
        width, half = self.width, self.width // TWO
        length = self.keys.shape[-1]
        self.ready_for("kv")
        self.stream[STREAMS[TWO * l + t]].drain()
        self.all_arrived(t, self.q_recv, self.q_send)
        rows = nt(self.wkv[...], self.h[t].reshape(HALF, self.dim))
        lo, hi = self.turned(rows, self.cos_own[t], self.sin_own[t])
        blank = jnp.zeros((LANES - width, HALF), BF16)
        new = jnp.concatenate([jnp.concatenate([lo, hi], 0).astype(BF16), blank, rows[width:].astype(BF16), blank], 0)
        self.kv_out[l, t] = new
        self.q_rows[...] = self.q_in[t].reshape(1024, LANES).astype(F32)
        row = lax.broadcasted_iota(jnp.int32, (HALF, length), 0)
        col = lax.broadcasted_iota(jnp.int32, (HALF, length), 1)
        cols = lax.broadcasted_iota(jnp.int32, (width, length), 1)
        blank = jnp.zeros((LANES - width, length), BF16)

        def one(s):
            pos = self.lengths[s] + t
            place = (row == s) & (col == pos)
            at_pos = nn(self.kv_out[l, t], place.astype(F32).astype(BF16)).astype(BF16)
            k = jnp.where(cols == pos, at_pos[0:width], self.keys[s])
            v = jnp.where(cols == pos, at_pos[LANES : LANES + width], self.values[s])
            if t == 0:
                self.keys[s] = k
                self.values[s] = v
            q = self.q_rows[pl.ds(s, HALF, stride=HALF), :].astype(BF16)
            score = nn(q, jnp.concatenate([k, blank], 0)) * width**-0.5
            score = jnp.where(col <= pos, score, -jnp.inf)
            weight = jnp.exp(score - jnp.max(score, axis=-1, keepdims=True))
            weight = (weight / jnp.sum(weight, axis=-1, keepdims=True)).astype(BF16)
            self.o_rows[pl.ds(s, HALF, stride=HALF), :] = nt(weight, jnp.concatenate([v, blank], 0))

        def several(i, carry):
            for u in range(FOUR):
                one(i * FOUR + u)
            return carry

        lax.fori_loop(0, 8, several, 0)
        self.o_out[t] = self.o_rows[...].astype(BF16).reshape(8, FOUR, HALF, LANES)
        zc, quad = self.mine()
        for s in range(FOUR):
            z = self.here.zs[s]

            def answer(r, core, four, device, z=z):
                self.trip("o", t, r, self.o_out.at[t, z * TWO + core, four], self.o_in.at[t, zc, quad], device).start()

            def keep(core, four, z=z):
                self.o_in[t, zc, quad] = self.o_out[t, z * TWO + core, four]

            self.each(s, answer, keep)
        if t and l + 1 < self.count:
            self.load("in", l + 1)
            self.load("kv", l + 1)

    def fill(self, l, t, s, core, ref):
        self.ready_for("out")
        if (l, t, s) not in self.answered:
            self.answered.add((l, t, s))
            self.each(s, lambda r, core, four, device: self.arrived(self.o_recv, t, r))
        z = self.here.zs[s]
        some = pl.ds(pl.multiple_of(core * LANES, LANES), LANES)

        def columns(n, carry):
            cols = pl.ds(pl.multiple_of(n * WIDE, WIDE), WIDE)
            rows = nn(self.o_in[t, z * TWO + core].reshape(LANES, LANES), self.wo[:, cols]) + nn(self.m[t, z, some], self.wd[:, cols])
            ref[:, :, :, cols] = rows.reshape(FOUR, TWO, 16, WIDE)
            return carry

        lax.fori_loop(0, self.dim // WIDE, columns, 0)
        self.fills += 1
        if self.fills == 16 * (l + 1) and l + 1 < self.count:
            self.load("out", l + 1)

    def finish(self, l, t, half, lo, rows):
        x = (self.x[t, half].astype(F32) + rows).astype(BF16)
        self.x[t, half] = x
        self.h[t, half] = normed(x, self.gains[pl.ds(l, 1)])

    def tile(self, i):
        at = lax.rem(i, TWO)
        return pltpu.make_async_copy(self.emb_hbm.at[pl.ds(pl.multiple_of(i * ROWS, ROWS), ROWS)], self.tiles.at[at], self.tile_sem.at[at])

    def store(self, t, z, i):
        at = lax.rem(i, TWO)
        rows, cols = pl.ds(pl.multiple_of(i * ROWS, ROWS), ROWS), pl.ds(pl.multiple_of(z * ROWS, ROWS), ROWS)
        return pltpu.make_async_copy(self.logits.at[at], self.out_hbm.at[t, rows, cols], self.logit_sem.at[at])

    def store_last(self, t, z):
        rows, cols = pl.ds(self.whole, TAIL), pl.ds(pl.multiple_of(z * ROWS, ROWS), ROWS)
        return pltpu.make_async_copy(self.last, self.out_hbm.at[t, rows, cols], self.logit_sem.at[TWO])

    def head(self, l, t, s):
        z, dim, count = self.here.zs[s], self.dim, self.whole // ROWS
        first, final = self.heads == 0, self.heads == 7
        self.heads += 1

        def rows():
            return self.every[t, z].reshape(ROWS, dim)

        if not first:
            self.store_last(t, z).wait()
        self.last[...] = nt(self.emb_tail[...], rows()) * dim**-0.5
        self.store_last(t, z).start()

        def one(i, carry):
            more = lax.rem(i + 1, count)

            @pl.when((i + 1 < count) if final else (i >= 0))
            def _():
                self.tile(more).start()

            self.tile(i).wait()

            @pl.when((i >= TWO) if first else (i >= 0))
            def _():
                self.store(t, z, i).wait()

            self.logits[lax.rem(i, TWO)] = nt(self.tiles[lax.rem(i, TWO)], rows()) * dim**-0.5
            self.store(t, z, i).start()
            return carry

        lax.fori_loop(0, count, one, 0)
        if final:
            self.store(t, z, 0).wait()
            self.store(t, z, 1).wait()
            self.store_last(t, z).wait()

    def run(self, order):
        h = self.here
        for name in ("in", "kv", "out"):
            self.load(name, 0)
        self.tile(0).start()
        self.h[...] = self.h_ref[...].reshape(self.h.shape)
        self.x[...] = self.x_ref[...].reshape(self.x.shape)
        self.wq[self.width : LANES] = jnp.zeros((LANES - self.width, self.dim), BF16)
        self.wo[self.width : LANES] = jnp.zeros((LANES - self.width, self.dim), BF16)
        for at in (0, self.up_at):
            self.wide[at + self.hidden : at + self.up_at] = jnp.zeros((self.up_at - self.hidden, self.dim), BF16)
        meet([h.dev(z, *f) for _, z, f in h.all()])
        placed = set()
        order = "".join(order)
        for letter, code in zip(order[::TWO], order[1::TWO], strict=True):
            who, at = self.stream[letter], STREAMS.index(letter)
            if isinstance(who, tuple):
                self.attend(*who)
                continue
            if letter not in placed and isinstance(who, Gather):
                placed.add(letter)
                core_inner = (h.y, h.x, h.c) if letter in "EF" else (h.c, h.y, h.x)
                self.every[(at % TWO, h.z, *core_inner)] = self.h[at % TWO]
            who.step(code)
            if who.STEPS[CODES.index(code)] == "end":
                who.drain()
                self.all_arrived(at % TWO, self.o_send)
        for letter in "EF":
            self.stream[letter].drain()
        self.loans.settle()


def layers_kernel(layers, names, lengths, x_ref, h_ref, gains, cos, sin, cos_own, sin_own, emb_tail, wg_hbm, wu_hbm, wq_hbm, wkv_hbm,
                  wd_hbm, wo_hbm, k_hbm, v_hbm, emb_hbm, out_hbm, kv_out, *scratch):
    refs = dict(locals(), **dict(zip(names, scratch, strict=True)))
    del refs["names"], refs["scratch"]
    Layers(**refs).run(ORDER)


def relayout_kernel(in_ref, out_ref):
    for t in range(TWO):
        out_ref[:, t, :] = in_ref[t]


def params(index, mib):
    return pltpu.CompilerParams(collective_id=index, has_side_effects=True, vmem_limit_bytes=mib << 20)


def solution(mesh):
    def device_fn(tokens, lengths, embedding, ln_scale, w_q, w_kv, w_o, w_gate, w_up, w_down, final_scale, k_cache, v_cache):
        me = lax.axis_index("tp")
        steps, batch = tokens.shape
        vocab, dim = embedding.shape
        layers, seqs, length, width = k_cache.shape
        hidden = w_gate.shape[-1]
        half = width // TWO
        block = jax.ShapeDtypeStruct((TWO, HALF, dim), BF16)

        def ordered(rows):
            return rows.reshape(TWO, FOUR, TWO, TWO, TWO, HALF).transpose(0, 1, FOUR, TWO, 3, 5).reshape(TWO, FOUR, TWO, LANES)

        positions = lengths[None, :] + jnp.arange(steps, dtype=jnp.int32)[:, None]
        own_len = lax.dynamic_slice_in_dim(lengths, me * seqs, seqs)
        own_pos = own_len[None, :] + jnp.arange(steps, dtype=jnp.int32)[:, None]
        inv_freq = 10000.0 ** (-jnp.arange(half, dtype=F32) / half)
        angles = ordered(positions).reshape(TWO, FOUR, 1, ROWS).astype(F32) * inv_freq[None, None, :, None]
        own_angles = own_pos[:, None, :].astype(F32) * inv_freq[None, :, None]
        tok = ordered(tokens).reshape(TWO, FOUR, TWO, FOUR, HALF).transpose(1, TWO, 3, 0, FOUR).reshape(8, ROWS, 1)
        turns = jnp.cos(angles), jnp.sin(angles), jnp.cos(own_angles), jnp.sin(own_angles)
        gains = jnp.concatenate([ln_scale[1:], final_scale[None]], 0)

        x, h = pl.pallas_call(
            embed_kernel,
            out_shape=(block, block),
            in_specs=[VMEM, ANY, VMEM],
            out_specs=(VMEM, VMEM),
            scratch_shapes=[pltpu.VMEM((vocab, dim), BF16), pltpu.VMEM((LANES, dim), BF16), DMA((1,)), *Reduce.scratch(HALF, dim, BF16)],
            compiler_params=params(0, 60),
            name="embed",
        )(tok, embedding, ln_scale[:1])

        wg_t, wu_t, wkv_t = (w.transpose(0, TWO, 1) for w in (w_gate, w_up, w_kv))
        wq_t = w_q.transpose(0, TWO, 3, 1).reshape(layers, width, dim)
        wo = w_o.reshape(layers, width, dim)
        k_t, v_t = k_cache.transpose(0, 1, 3, TWO), v_cache.transpose(0, 1, 3, TWO)
        padded = pl.cdiv(vocab, 8) * 8
        tail = jnp.pad(embedding[vocab // ROWS * ROWS :], ((0, padded - vocab), (0, 0)))
        scratch = Layers.scratch(dim, hidden, width, seqs, length)
        logits, fresh = pl.pallas_call(
            functools.partial(layers_kernel, layers, tuple(scratch)),
            out_shape=(jax.ShapeDtypeStruct((TWO, padded, batch), F32), jax.ShapeDtypeStruct((layers, TWO, ROWS, HALF), BF16)),
            in_specs=[SMEM] + [VMEM] * 8 + [ANY] * 9,
            out_specs=(ANY, VMEM),
            scratch_shapes=list(scratch.values()),
            compiler_params=params(1, 63),
            name="layers",
        )(own_len, x, h, gains, *turns, tail, wg_t, wu_t, wq_t, wkv_t, w_down, wo, k_t, v_t, embedding)
        logits = pl.pallas_call(
            relayout_kernel,
            grid=(pl.cdiv(vocab, SHEET),),
            out_shape=jax.ShapeDtypeStruct((vocab, TWO, batch), F32),
            in_specs=[pl.BlockSpec((TWO, SHEET, batch), lambda i: (0, i, 0))],
            out_specs=pl.BlockSpec((SHEET, TWO, batch), lambda i: (i, 0, 0)),
            name="relayout",
        )(logits)

        row_ids = lax.broadcasted_iota(jnp.int32, (1, 1, length, 1), TWO)
        new = fresh.reshape(layers, TWO, TWO, LANES, HALF)[:, :, :, :width]

        def written(cache, which):
            for t in range(steps):
                cache = jnp.where(
                    row_ids == own_pos[t][None, :, None, None], new[:, t, which].transpose(0, TWO, 1)[:, :, None, :], cache
                )
            return cache

        return logits.transpose(1, TWO, 0), written(k_cache, 0), written(v_cache, 1)

    cache_spec = P(None, "tp", None, None)
    in_specs = (P(), P(), P("tp", None), P(), P(None, None, "tp", None), P(), P(None, "tp", None, None), P(None, None, "tp"), P(None, None, "tp"), P(None, "tp", None), P(), cache_spec, cache_spec)
    out_specs = (P(None, None, "tp"), cache_spec, cache_spec)
    return jax.shard_map(device_fn, mesh=mesh, in_specs=in_specs, out_specs=out_specs, check_vma=False)
```

```python
import functools

import jax
import jax.numpy as jnp
from jax import lax
from jax.experimental import pallas as pl
from jax.experimental.pallas import tpu as pltpu
from jax.sharding import PartitionSpec as P

LN_EPS = 1e-6
TWO, FOUR = 2, 4
HALF, BLOCK, ROWS, LANES = 32, 64, 256, 128
MESH = pl.DeviceIdType.MESH
BF16, F32 = jnp.bfloat16, jnp.float32
ANY = pl.BlockSpec(memory_space=pl.ANY)
VMEM = pl.BlockSpec(memory_space=pltpu.VMEM)
SMEM = pl.BlockSpec(memory_space=pltpu.SMEM)
DMA = pltpu.SemaphoreType.DMA
FLIPS = [(a, b, e) for a in range(TWO) for b in range(TWO) for e in range(TWO)]
SIDE = 512
ALL = (slice(None),) * 3
CODES = "0123456789abcdefghijklmnopqrstuvwxyz"
STREAMS = "ABCDEFRSTUJKLM"


def numbered(words, slots):
    return tuple(f"{word}{s}" for word in words for s in slots)


TAIL = 40
WIDE = 512
GROUP = 8
SHEET = 264
REDUCE = "372bfu6ae1tnj59sd0mi48rxylhqcwpvgkoz"
ORDER = (
    "A0B0AqBqAkA4A1AlA8A2BkBlB4B8AmA5A9B1AcB2A3ArBmBcA6BrAaAoB3B5",
    "B9AnAdB6BoAhBaAbBnA7AeBgApAiBbB7BdBpAfAgAjBeBhBfBiBjJ0K0R2R6",
    "RaReS2R3S6R7SaRmSeRiRtRbRfS3R0S7RuSbSfR1SiR5StR9S1RjRnRdSuRq",
    "R4R8S5SnS9SjRsSdRhRwRrRlS0S4SmSsS8RySrRcSlRxShSxRkSyRgSqScRp",
    "SwRvSgSpSkRoSvRzCqC0SoClC2SzDqC8CkC1C4D0CaCmDlC6CcC5C9D2CrD4",
    "DkD8CdCoD1CgC3DmDcDrCnD5D9D6CeD3DaChC7CbCiDdDgD7DoDnDeDbCpCf",
    "DhCjDfDpDiDjL0T2M0T6TaT3TeT7U2TbTfTtTmTiU6UaUeU3TuU7T1TjUbUf",
    "T0UuT5TnT9U1TqUiUmTsT4T8U5U9UsTdU0U4UjUnUdTwUqTyTlThTcUtTrTx",
    "UrU8UhUlUyUxTpTkTgUcUwTvUpUvUgUkToTzE0EqUoElE2EkE4E8UzFqF0Ea",
    "EmEcE6E1ErF4F8FlE3FkEgEoE5E9F1F2EeFcEnFmEbE7FrF3FgEdF5EiEpF9",
    "FaF6EfEhF7FoFbFnFdEjFeFhFfFpFiFj",
)


class Here:
    def __init__(self):
        me = lax.axis_index("tp")
        self.c = lax.rem(me, TWO)
        self.x = lax.rem(lax.div(me, TWO), TWO)
        self.y = lax.rem(lax.div(me, FOUR), TWO)
        z = lax.div(me, 8)
        self.z = z
        self.against = {id(v): 1 - v for v in (self.c, self.x, self.y)}
        inner = lax.rem(lax.div(z + 1, TWO), TWO)
        self.inner = inner == 1
        two, three = lax.rem(z + TWO, FOUR), 3 - z
        self.zs = [z, z + 1 - TWO * lax.rem(z, TWO), inner * three + (1 - inner) * two, inner * two + (1 - inner) * three]
        self.slot = ((z * TWO + self.c) * TWO + self.y) * TWO + self.x
        self.near, self.across = self.dev(self.zs[1]), self.dev(three)
        self.core, self.along_x, self.along_y = self.dev(z, a=1), self.dev(z, e=1), self.dev(z, b=1)

    def flip(self, v, on):
        return self.against[id(v)] if on else v

    def dev(self, z, a=0, b=0, e=0):
        y, x, c = self.flip(self.y, b), self.flip(self.x, e), self.flip(self.c, a)
        return ((z * TWO + y) * TWO + x) * TWO + c

    def apart(self, s):
        inner = lax.rem(lax.div(self.z + 1, TWO), TWO)
        return (0, 1, TWO + inner, 3 - inner)[s]

    def partner(self, s, f):
        a, b, e = lax.div(f, FOUR), lax.rem(lax.div(f, TWO), TWO), lax.rem(f, TWO)
        c, y, x = (on + v - TWO * on * v for on, v in ((a, self.c), (b, self.y), (e, self.x)))
        return self.apart(s) * 8 + f, c, y * TWO + x, ((self.zs[s] * TWO + y) * TWO + x) * TWO + c

    def lines(self):
        return [self.near, self.dev(self.zs[TWO]), self.dev(self.zs[3]), self.core, self.along_x, self.along_y]

    def all(self):
        z = self.z
        zs = [z, self.zs[1], lax.rem(z + TWO, FOUR), 3 - z]
        return [(8 * j + FOUR * a + TWO * b + e, zs[j], (a, b, e)) for j in range(FOUR) for a, b, e in FLIPS if j or a or b or e]


def meet(devices):
    sem = pltpu.get_barrier_semaphore()
    for d in devices:
        pl.semaphore_signal(sem, inc=1, device_id={"tp": d}, device_id_type=MESH)
    pl.semaphore_wait(sem, len(devices))


class Wires:
    def __init__(self, here, send, recv, sizes):
        self.here, self.send, self.recv = here, send, recv
        self.names, self.first, self.started, at = {}, {}, {}, 0
        for kind, count in sizes.items():
            self.first[kind], self.started[kind] = at, []
            at += count

    def go(self, what, src, dst, device, inner=None):
        kind = tuple(src.shape), inner
        k = self.names.setdefault(what, len(self.names))
        copy = pltpu.make_async_remote_copy(
            src_ref=src,
            dst_ref=dst,
            send_sem=self.send.at[self.first[kind] + len(self.started[kind])],
            recv_sem=self.recv.at[k],
            device_id={"tp": device},
            device_id_type=MESH,
        )
        self.started[kind].append(src)
        if inner is None:
            copy.start()
        else:
            pl.when(self.here.inner == inner)(copy.start)

    def got(self, what, like):
        k = self.names.setdefault(what, len(self.names))
        pltpu.make_async_copy(like, like, self.recv.at[k]).wait()

    def step(self, code):
        name = self.STEPS[CODES.index(code)]
        word = name.rstrip(CODES[:FOUR])
        getattr(self, word)(*map(int, name[len(word) :]))

    def run(self, order):
        for code in "".join(order):
            self.step(code)

    def drain(self):
        for (kind, inner), copies in self.started.items():

            def wait(ref=copies[0], first=self.first[kind, inner], count=len(copies)):
                def one(i, carry):
                    pltpu.make_async_copy(ref, ref, self.send.at[first + i]).wait()
                    return carry

                lax.fori_loop(0, count, one, 0)

            if inner is None:
                wait()
            else:
                pl.when(self.here.inner == inner)(wait)


def nt(a, b):
    return lax.dot_general(a, b, (((1,), (1,)), ((), ())), preferred_element_type=F32)


def nn(a, b):
    return lax.dot_general(a, b, (((1,), (0,)), ((), ())), preferred_element_type=F32)


class Gather(Wires):
    COPIES = 48
    STEPS = numbered(("sh", "tx", "ty", "cl", "us"), range(FOUR)) + numbered(("zf", "ff"), range(1, FOUR)) + ("zown", "fown")

    def __init__(self, here, own, plane, send, recv, use):
        rows, dim = own.shape[1:]
        main, four = ((TWO, rows, dim - SIDE)), (TWO, TWO, TWO, rows, SIDE)
        sizes = {(main, None): 19, (main, True): FOUR, ((TWO, rows, dim), None): 6, (four, None): FOUR, (four, True): FOUR}
        super().__init__(here, send, recv, sizes | {(main[1:], None): 6, ((rows, dim), None): TWO})
        self.own, self.plane, self.use = own, plane, use
        self.main, self.side, self.full = pl.ds(0, dim - SIDE), pl.ds(dim - SIDE, SIDE), pl.ds(0, dim)

    def at(self, s, b=0, e=0):
        h = self.here
        return self.plane(h.zs[s], h.c).at[h.flip(h.y, b), h.flip(h.x, e)].at[:, :, self.main if s else self.full]

    def fours(self, s):
        return self.plane(self.here.zs[s], self.here.c).at[:, :, :, :, self.side]

    def pass_on(self, what, s, ref):
        h = self.here
        self.go((what, 3 if s == 1 else s), ref, ref, h.across if s == 1 else h.near, True)

    def zown(self):
        h = self.here
        src, dst = self.own.at[:, :, self.main], self.at(0).at[:, :, self.main]
        self.go(("z", 1), src, dst, h.near)
        self.go(("z", TWO), src, dst, h.across, True)

    def zf(self, s):
        self.got(("z", s), self.at(s))
        self.pass_on("z", s, self.at(s))

    def fown(self):
        h, ref = self.here, self.fours(0)
        self.go(("f", 1), ref, ref, h.near)
        self.go(("f", TWO), ref, ref, h.across, True)

    def ff(self, s):
        ref = self.fours(s)
        self.got(("f", s), ref)
        self.pass_on("f", s, ref)
        self.go(("cf", s), ref, ref, self.here.core)

    def sh(self, s):
        h, dst = self.here, self.at(s)
        src = dst if s else self.own
        self.go(("x", s), src, dst, h.along_x)
        self.go(("y", s), src, dst, h.along_y)
        self.go(("c", s), src, dst, h.core)

    def tx(self, s):
        ref = self.at(s, e=1)
        self.got(("x", s), ref)
        self.go(("xy", s), ref.at[0], ref.at[0], self.here.along_y)
        self.go(("cx", s), ref, ref, self.here.core)

    def ty(self, s):
        ref = self.at(s, b=1)
        self.got(("y", s), ref)
        self.go(("yx", s), ref.at[1], ref.at[1], self.here.along_x)
        self.go(("cy", s), ref, ref, self.here.core)

    def cl(self, s):
        ref = self.at(s, 1, 1)
        self.got(("xy", s), ref.at[0])
        self.got(("yx", s), ref.at[1])
        self.go(("cd", s), ref, ref, self.here.core)

    def us(self, s):
        for what in ("c", "cx", "cy", "cd"):
            self.got((what, s), self.at(s))
        if s:
            self.got(("cf", s), self.fours(s))
        self.use(s)


class Loans:
    def __init__(self, here, send, free):
        self.here, self.send, self.free = here, send, free
        self.lent, self.out = [], set()

    def take(self, s):
        if s in self.out:
            pl.semaphore_wait(self.free.at[s], 1)
        self.out.add(s)

    def give(self, s):
        pl.semaphore_signal(self.free.at[s], inc=1, device_id={"tp": self.here.core}, device_id_type=MESH)

    def settle(self):
        for copy in self.lent[-TWO:]:
            copy.wait_send()
        for s in self.out:
            pl.semaphore_wait(self.free.at[s], 1)


class Reduce(Wires):
    COPIES = 48
    STEPS = numbered(("fo", "fm", "ca", *"dpqu"), range(FOUR)) + numbered(("fz", "gz"), range(1, FOUR)) + ("fin", "end")

    @staticmethod
    def scratch(rows, dim, dtype):
        return [
            pltpu.VMEM((FOUR, FOUR, TWO, rows, dim), dtype),
            pltpu.VMEM((TWO, FOUR, TWO, rows, dim), dtype),
            pltpu.VMEM((FOUR, FOUR, TWO, rows, dim), dtype),
            pltpu.VMEM((FOUR, TWO, rows, dim), dtype),
            pltpu.VMEM((FOUR, TWO, rows, dim), dtype),
            pltpu.VMEM((FOUR, TWO, rows, dim), dtype),
            pltpu.VMEM((5, TWO, rows, dim - SIDE), dtype),
            pltpu.VMEM((5, FOUR, TWO, rows, SIDE), dtype),
            DMA((Reduce.COPIES,)),
            DMA((Reduce.COPIES,)),
            DMA((TWO,)),
            pltpu.SemaphoreType.REGULAR((FOUR,)),
        ]

    def __init__(self, here, fill, finish, loans, part, sib, core_in, diag_in, x_in, y_in, z_in, side_in, send, recv):
        rows, dim = part.shape[3:]
        main, four = (TWO, rows, dim - SIDE), (FOUR, TWO, rows, SIDE)
        sizes = {(main[1:], None): 18, ((rows, dim), None): 6, (four, True): 3, (four, False): 3, (main, True): 3, (main, False): 3}
        super().__init__(here, send, recv, sizes)
        self.fill, self.finish, self.loans = fill, finish, loans
        self.part, self.sib, self.core_in, self.diag_in = part, sib, core_in, diag_in
        self.x_in, self.y_in, self.z_in, self.side_in = x_in, y_in, z_in, side_in
        dim = part.shape[-1]
        self.main, self.side, self.full = pl.ds(0, dim - SIDE), pl.ds(dim - SIDE, SIDE), pl.ds(0, dim)

    def quad(self, b, e):
        h = self.here
        return h.flip(h.y, b) * TWO + h.flip(h.x, e)

    def piece(self, buf, s, *where):
        return buf, (s, *where, slice(None), self.main if s else self.full)

    def add(self, ref, *more):
        buf, index = ref
        total = buf[index]
        for other, where in more:
            total = total + other[where]
        buf[index] = total

    def fo(self, s):
        loans, n = self.loans, len(self.loans.lent)
        if n > 1:
            loans.lent[n - TWO].wait_send()
        self.fill(s, self.here.flip(self.here.c, 1), self.sib.at[n % TWO])
        loans.take(s)
        k = self.names.setdefault(("c", s), len(self.names))
        copy = pltpu.make_async_remote_copy(
            src_ref=self.sib.at[n % TWO],
            dst_ref=self.core_in.at[s],
            send_sem=loans.send.at[n % TWO],
            recv_sem=self.recv.at[k],
            device_id={"tp": self.here.core},
            device_id_type=MESH,
        )
        copy.start()
        loans.lent.append(copy)

    def fm(self, s):
        self.fill(s, self.here.c, self.part.at[s])

    def ca(self, s):
        self.got(("c", s), self.core_in.at[s])
        for t in range(TWO):

            def add(i, carry):
                self.add((self.part, (s, i, t)), (self.core_in, (s, i, t)))
                return carry

            lax.fori_loop(0, FOUR, add, 0)
        self.loans.give(s)

    def along_z(self, what, s, ref, landing):
        h = self.here
        k = 5 if s == 1 else s
        to = 1 if s == 1 else s + TWO

        @pl.when(h.inner)
        def _():
            self.got((what, k), landing.at[k - 1])
            self.add(ref, (landing, k - 1))

        self.go((what, to), ref[0].at[ref[1]], landing.at[to - 1], h.near if s == 1 else h.across, True)
        self.go((what, s), ref[0].at[ref[1]], landing.at[s - 1], h.near, False)

    def last_z(self, what, ref, landing):
        self.got((what, 1), landing.at[0])
        self.add(ref, (landing, 0))

        @pl.when(self.here.inner)
        def _():
            self.got((what, FOUR), landing.at[3])
            self.add(ref, (landing, 3))

    def fz(self, s):
        self.along_z("f", s, (self.part, (s, *ALL, self.side)), self.side_in)

    def fin(self):
        self.last_z("f", (self.part, (0, *ALL, self.side)), self.side_in)

    def d(self, s):
        h, part = self.here, self.part
        far = self.quad(1, 1)
        self.pass_on("dy", s, self.piece(part, s, far, 0), self.piece(self.diag_in, s, 0), h.along_y)
        self.pass_on("dx", s, self.piece(part, s, far, 1), self.piece(self.diag_in, s, 1), h.along_x)
        self.pass_on("x1", s, self.piece(part, s, self.quad(0, 1), 1), self.piece(self.x_in, s, 1), h.along_x)
        self.pass_on("y0", s, self.piece(part, s, self.quad(1, 0), 0), self.piece(self.y_in, s, 0), h.along_y)

    def pass_on(self, what, s, src, dst, device):
        self.go((what, s), src[0].at[src[1]], dst[0].at[dst[1]], device)

    def came(self, what, s, ref):
        self.got((what, s), ref[0].at[ref[1]])

    def p(self, s):
        ref = self.piece(self.part, s, self.quad(0, 1), 0)
        self.came("dy", s, ref)
        self.add(ref, self.piece(self.diag_in, s, 0))
        self.pass_on("x0", s, ref, self.piece(self.x_in, s, 0), self.here.along_x)

    def q(self, s):
        ref = self.piece(self.part, s, self.quad(1, 0), 1)
        self.came("dx", s, ref)
        self.add(ref, self.piece(self.diag_in, s, 1))
        self.pass_on("y1", s, ref, self.piece(self.y_in, s, 1), self.here.along_y)

    def u(self, s):
        for t in range(TWO):
            ref = self.piece(self.part, s, self.quad(0, 0), t)
            self.came(f"x{t}", s, ref)
            self.came(f"y{t}", s, ref)
            self.add(ref, self.piece(self.x_in, s, t), self.piece(self.y_in, s, t))

    def gz(self, s):
        self.along_z("g", s, (self.part, (s, self.quad(0, 0), *ALL[:TWO], self.main)), self.z_in)

    def end(self):
        mine = self.quad(0, 0)
        self.last_z("g", (self.part, (0, mine, *ALL[:TWO], self.main)), self.z_in)
        for t in range(TWO):
            for lo in range(0, self.part.shape[3], 16):
                self.finish(t, lo, self.part[0, mine, t, lo : lo + 16])


def normed(x, gain):
    rows = x.astype(F32)
    centred = rows - jnp.mean(rows, axis=-1, keepdims=True)
    var = jnp.mean(centred * centred, axis=-1, keepdims=True)
    return (centred * lax.rsqrt(var + LN_EPS) * gain).astype(BF16)


def load(pairs, sems):
    copies = [pltpu.make_async_copy(src, dst, sems.at[i]) for i, (src, dst) in enumerate(pairs)]
    for copy in copies:
        copy.start()
    return copies


def embed_kernel(tok_ref, emb_hbm, gain_ref, x_ref, h_ref, emb, tail, sem, *scratch):
    here = Here()
    vocab, dim = emb_hbm.shape
    whole = vocab // ROWS * ROWS
    rest = vocab - whole
    (fetch,) = load([(emb_hbm, emb)], sem)
    meet(here.lines())
    fetch.wait()
    tail[...] = jnp.zeros_like(tail)
    tail[0:rest] = emb[whole:vocab]
    base = lax.axis_index("tp") * vocab

    def fill(s, core, ref):
        tok = tok_ref[here.zs[s] * TWO + core] - base
        hot = (tok == lax.broadcasted_iota(jnp.int32, (ROWS, whole), 1)).astype(F32).astype(BF16)
        hot_tail = (tok == lax.broadcasted_iota(jnp.int32, (ROWS, LANES), 1) + whole).astype(F32).astype(BF16)

        def columns(n, carry):
            cols = pl.ds(pl.multiple_of(n * ROWS, ROWS), ROWS)
            rows = nn(hot, emb[0:whole, cols]) + nn(hot_tail, tail[:, cols])
            ref[:, :, :, cols] = rows.astype(BF16).reshape(FOUR, TWO, HALF, ROWS)
            return carry

        lax.fori_loop(0, dim // ROWS, columns, 0)

    def finish(t, lo, rows):
        x_ref[t, lo : lo + 16] = rows
        h_ref[t, lo : lo + 16] = normed(rows, gain_ref[...])

    *rs, lent, free = scratch
    loans = Loans(here, lent, free)
    red = Reduce(here, fill, finish, loans, *rs)
    red.run(REDUCE)
    red.drain()
    loans.settle()


def attention(t, lengths, q_rows, fresh, keys, values, o_rows):
    seqs, width, length = keys.shape
    col = lax.broadcasted_iota(jnp.int32, (HALF, length), 1)
    blank = jnp.zeros((LANES - width, length), BF16)

    def several(i, carry):
        some = [i * GROUP + u for u in range(GROUP)]
        pos = [lengths[s] for s in some]
        q = [q_rows[pl.ds(s, HALF, stride=HALF), :] for s in some]
        new = [[fresh[step, pl.ds(s, 1), :] for step in range(t + 1)] for s in some]
        score = [nn(a.astype(BF16), jnp.concatenate([keys[s], blank], 0)) for a, s in zip(q, some)]
        own = [[jnp.sum(a * row[:, 0:LANES], axis=-1, keepdims=True) for row in rows] for a, rows in zip(q, new)]
        for u in range(GROUP):
            for step in range(t + 1):
                score[u] = jnp.where(col == pos[u] + step, own[u][step], score[u])
            score[u] = jnp.where(col <= pos[u] + t, score[u] * width**-0.5, -jnp.inf)
        top = [jnp.max(a, axis=-1, keepdims=True) for a in score]
        weight = [jnp.exp(a - b) for a, b in zip(score, top)]
        total = [jnp.sum(a, axis=-1, keepdims=True) for a in weight]
        weight = [(a / b).astype(BF16).astype(F32) for a, b in zip(weight, total)]
        at = [[col == p + step for step in range(t + 1)] for p in pos]
        mine = [[jnp.sum(jnp.where(hit, a, 0.0), axis=-1, keepdims=True) for hit in hits] for a, hits in zip(weight, at)]
        for u in range(GROUP):
            for hit in at[u]:
                weight[u] = jnp.where(hit, 0.0, weight[u])
        out = [nt(a.astype(BF16), jnp.concatenate([values[s], blank], 0)) for a, s in zip(weight, some)]
        for u in range(GROUP):
            for step in range(t + 1):
                out[u] = out[u] + mine[u][step] * new[u][step][:, LANES:ROWS]
            o_rows[pl.ds(some[u], HALF, stride=HALF), :] = out[u]
        return carry

    lax.fori_loop(0, seqs // GROUP, several, 0)


class Layers:
    @staticmethod
    def scratch(dim, hidden, width, seqs, length):
        up_at = pl.cdiv(hidden, LANES) * LANES
        return dict(
            x=pltpu.VMEM((TWO, TWO, 16, dim), BF16),
            h=pltpu.VMEM((TWO, TWO, 16, dim), BF16),
            every=pltpu.VMEM((TWO, FOUR, TWO, TWO, TWO, TWO, 16, dim), BF16),
            wide=pltpu.VMEM((TWO * up_at, dim), BF16),
            wq=pltpu.VMEM((LANES, dim), BF16),
            wkv=pltpu.VMEM((TWO * width, dim), BF16),
            wd=pltpu.VMEM((hidden, dim), BF16),
            wo=pltpu.VMEM((LANES, dim), BF16),
            ready=pltpu.VMEM((ROWS, TWO * up_at), F32),
            m=pltpu.VMEM((TWO, FOUR, ROWS, hidden), BF16),
            q_out=pltpu.VMEM((TWO, FOUR, TWO, FOUR, HALF, LANES), BF16),
            q_in=pltpu.VMEM((TWO, 8, FOUR, HALF, LANES), BF16),
            o_out=pltpu.VMEM((TWO, 8, FOUR, HALF, LANES), BF16),
            o_in=pltpu.VMEM((TWO, 8, FOUR, HALF, LANES), BF16),
            q_rows=pltpu.VMEM((1024, LANES), F32),
            o_rows=pltpu.VMEM((1024, LANES), F32),
            fresh=pltpu.VMEM((TWO, LANES, ROWS), F32),
            keys=pltpu.VMEM((seqs, width, length), BF16),
            values=pltpu.VMEM((seqs, width, length), BF16),
            tiles=pltpu.VMEM((TWO, ROWS, dim), BF16),
            logits=pltpu.VMEM((TWO, ROWS, ROWS), F32),
            last=pltpu.VMEM((TAIL, ROWS), F32),
            w_sem=DMA((8,)),
            tile_sem=DMA((TWO,)),
            logit_sem=DMA((3,)),
            q_send=DMA((TWO, HALF)),
            q_recv=DMA((TWO, HALF)),
            o_send=DMA((TWO, HALF)),
            o_recv=DMA((TWO, HALF)),
            g_send=DMA((TWO, Gather.COPIES)),
            g_recv=DMA((TWO, Gather.COPIES)),
            part=pltpu.VMEM((TWO, FOUR, FOUR, TWO, 16, dim), F32),
            sib=pltpu.VMEM((TWO, FOUR, TWO, 16, dim), F32),
            core_in=pltpu.VMEM((FOUR, FOUR, TWO, 16, dim), F32),
            diag_in=pltpu.VMEM((TWO, FOUR, TWO, 16, dim), F32),
            x_in=pltpu.VMEM((TWO, FOUR, TWO, 16, dim), F32),
            y_in=pltpu.VMEM((TWO, FOUR, TWO, 16, dim), F32),
            z_in=pltpu.VMEM((TWO, 5, TWO, 16, dim - SIDE), F32),
            side_in=pltpu.VMEM((TWO, 5, FOUR, TWO, 16, SIDE), F32),
            r_send=DMA((TWO, Reduce.COPIES)),
            r_recv=DMA((TWO, Reduce.COPIES)),
            lent=DMA((TWO,)),
            free=pltpu.SemaphoreType.REGULAR((FOUR,)),
        )

    def __init__(self, layers, **refs):
        self.__dict__.update(refs)
        here = self.here = Here()
        self.count = layers
        self.dim, self.hidden, self.width = self.h.shape[-1], self.m.shape[-1], self.keys.shape[1]
        self.up_at = self.wide.shape[0] // TWO
        self.whole = self.emb_hbm.shape[0] // ROWS * ROWS
        self.loads, self.answered, self.heads, self.fills = {}, set(), 0, 0
        self.stream = {}
        self.loans = Loans(here, self.lent, self.free)
        letters = iter(STREAMS)
        for l in range(layers + 1):
            for t in range(TWO):
                use = functools.partial(self.project if l < layers else self.head, l, t)
                if l < layers:
                    plane = functools.partial(lambda t, z, c: self.every.at[t, z, c], t)
                else:
                    plane = functools.partial(lambda t, z, c: self.every.at[t, z, :, :, c], t)
                self.stream[next(letters)] = Gather(here, self.h.at[t], plane, self.g_send.at[t], self.g_recv.at[t], use)
        for l in range(layers):
            for t in range(TWO):
                fill, finish = functools.partial(self.fill, l, t), functools.partial(self.finish, l, t)
                mine = [ref.at[t] for ref in (self.diag_in, self.x_in, self.y_in, self.z_in, self.side_in, self.r_send, self.r_recv)]
                reduce = Reduce(here, fill, finish, self.loans, self.part.at[t], self.sib, self.core_in, *mine)
                self.stream[next(letters)] = reduce
        for l in range(layers):
            for t in range(TWO):
                self.stream[next(letters)] = (l, t)

    def load(self, name, l):
        groups = {
            "in": [(self.wg_hbm, self.wide.at[0 : self.hidden]), (self.wu_hbm, self.wide.at[self.up_at : self.up_at + self.hidden]),
                   (self.wq_hbm, self.wq.at[0 : self.width])],
            "out": [(self.wd_hbm, self.wd), (self.wo_hbm, self.wo.at[0 : self.width])],
            "kv": [(self.wkv_hbm, self.wkv), (self.k_hbm, self.keys), (self.v_hbm, self.values)],
        }
        first = {"in": 0, "out": 3, "kv": 5}[name]
        copies = [pltpu.make_async_copy(src.at[l], dst, self.w_sem.at[first + i]) for i, (src, dst) in enumerate(groups[name])]
        for copy in copies:
            copy.start()
        self.loads[name] = copies

    def ready_for(self, name):
        for copy in self.loads.pop(name, ()):
            copy.wait()

    def turned(self, rows, cos, sin):
        half = self.width // TWO
        lo, hi = rows[0:half], rows[half : self.width]
        return lo * cos - hi * sin, lo * sin + hi * cos

    def each(self, s, body, own=None):
        if s == 0 and own:
            own(self.here.c, self.here.y * TWO + self.here.x)

        def one(f, carry):
            body(*self.here.partner(s, f))
            return carry

        lax.fori_loop(0 if s else 1, 8, one, 0)

    def trip(self, kind, t, r, src, dst, device):
        sends, recvs = (self.q_send, self.q_recv) if kind == "q" else (self.o_send, self.o_recv)
        return pltpu.make_async_remote_copy(
            src_ref=src, dst_ref=dst, send_sem=sends.at[t, r], recv_sem=recvs.at[t, r], device_id={"tp": device}, device_id_type=MESH
        )

    def arrived(self, sems, t, r):
        ref = self.q_in.at[t, 0, 0]
        pltpu.make_async_copy(ref, ref, sems.at[t, r]).wait()

    def all_arrived(self, t, *sems):
        def one(r, carry):
            for sem in sems:
                self.arrived(sem, t, r)
            return carry

        lax.fori_loop(1, HALF, one, 0)

    def mine(self):
        h = self.here
        return h.z * TWO + h.c, h.y * TWO + h.x

    def project(self, l, t, s):
        self.ready_for("in")
        z, dim = self.here.zs[s], self.dim

        def rows():
            return self.every[t, z].reshape(ROWS, dim)

        q = nt(self.wq[...], rows())
        lo, hi = self.turned(q, self.cos[t, z], self.sin[t, z])
        q = jnp.concatenate([lo, hi, jnp.zeros((LANES - self.width, ROWS), F32)], 0)
        self.q_out[t, z] = q.T.astype(BF16).reshape(TWO, FOUR, HALF, LANES)
        zc, quad = self.mine()

        def ask(r, core, four, device):
            self.trip("q", t, r, self.q_out.at[t, z, core, four], self.q_in.at[t, zc, quad], device).start()

        def keep(core, four):
            self.q_in[t, zc, quad] = self.q_out[t, z, core, four]

        self.each(s, ask, keep)

        def tile(n, carry):
            cols = pl.ds(pl.multiple_of(n * ROWS, ROWS), ROWS)
            self.ready[:, cols] = nt(rows(), self.wide[cols])
            return carry

        lax.fori_loop(0, self.wide.shape[0] // ROWS, tile, 0)

        def gated(n, carry):
            some = pl.ds(pl.multiple_of(n * HALF, HALF), HALF)
            gate, up = self.ready[some, 0 : self.hidden], self.ready[some, self.up_at : self.up_at + self.hidden]
            self.m[t, z, some] = (gate * jax.nn.sigmoid(gate) * up).astype(BF16)
            return carry

        lax.fori_loop(0, 8, gated, 0)

    def attend(self, l, t):
        width = self.width
        self.ready_for("kv")
        self.stream[STREAMS[TWO * l + t]].drain()
        self.all_arrived(t, self.q_recv, self.q_send)
        mine = jnp.concatenate([self.h[t].reshape(HALF, self.dim), jnp.zeros((LANES - HALF, self.dim), BF16)], 0)
        rows = nt(self.wkv[...], mine)
        lo, hi = self.turned(rows, self.cos_own[t], self.sin_own[t])
        blank = jnp.zeros((LANES - width, LANES), BF16)
        new = jnp.concatenate([jnp.concatenate([lo, hi], 0).astype(BF16), blank, rows[width:].astype(BF16), blank], 0)
        self.kv_out[l, t] = new[:, 0:HALF]
        self.fresh[t] = new.astype(F32).T
        self.q_rows[...] = self.q_in[t].reshape(1024, LANES).astype(F32)
        attention(t, self.lengths, self.q_rows, self.fresh, self.keys, self.values, self.o_rows)
        self.o_out[t] = self.o_rows[...].astype(BF16).reshape(8, FOUR, HALF, LANES)
        zc, quad = self.mine()
        for s in range(FOUR):
            z = self.here.zs[s]

            def answer(r, core, four, device, z=z):
                self.trip("o", t, r, self.o_out.at[t, z * TWO + core, four], self.o_in.at[t, zc, quad], device).start()

            def keep(core, four, z=z):
                self.o_in[t, zc, quad] = self.o_out[t, z * TWO + core, four]

            self.each(s, answer, keep)
        if t and l + 1 < self.count:
            self.load("in", l + 1)
            self.load("kv", l + 1)

    def fill(self, l, t, s, core, ref):
        self.ready_for("out")
        if (l, t, s) not in self.answered:
            self.answered.add((l, t, s))
            self.each(s, lambda r, core, four, device: self.arrived(self.o_recv, t, r))
        z = self.here.zs[s]
        some = pl.ds(pl.multiple_of(core * LANES, LANES), LANES)

        def columns(n, carry):
            cols = pl.ds(pl.multiple_of(n * WIDE, WIDE), WIDE)
            rows = nn(self.o_in[t, z * TWO + core].reshape(LANES, LANES), self.wo[:, cols]) + nn(self.m[t, z, some], self.wd[:, cols])
            ref[:, :, :, cols] = rows.reshape(FOUR, TWO, 16, WIDE)
            return carry

        lax.fori_loop(0, self.dim // WIDE, columns, 0)
        self.fills += 1
        if self.fills == 16 * (l + 1) and l + 1 < self.count:
            self.load("out", l + 1)

    def finish(self, l, t, half, lo, rows):
        x = (self.x[t, half].astype(F32) + rows).astype(BF16)
        self.x[t, half] = x
        self.h[t, half] = normed(x, self.gains[pl.ds(l, 1)])

    def tile(self, i):
        at = lax.rem(i, TWO)
        return pltpu.make_async_copy(self.emb_hbm.at[pl.ds(pl.multiple_of(i * ROWS, ROWS), ROWS)], self.tiles.at[at], self.tile_sem.at[at])

    def store(self, t, z, i):
        at = lax.rem(i, TWO)
        rows, cols = pl.ds(pl.multiple_of(i * ROWS, ROWS), ROWS), pl.ds(pl.multiple_of(z * ROWS, ROWS), ROWS)
        return pltpu.make_async_copy(self.logits.at[at], self.out_hbm.at[t, rows, cols], self.logit_sem.at[at])

    def store_last(self, t, z):
        rows, cols = pl.ds(self.whole, TAIL), pl.ds(pl.multiple_of(z * ROWS, ROWS), ROWS)
        return pltpu.make_async_copy(self.last, self.out_hbm.at[t, rows, cols], self.logit_sem.at[TWO])

    def head(self, l, t, s):
        z, dim, count = self.here.zs[s], self.dim, self.whole // ROWS
        first, final = self.heads == 0, self.heads == 7
        self.heads += 1

        def rows():
            return self.every[t, z].reshape(ROWS, dim)

        if not first:
            self.store_last(t, z).wait()
        self.last[...] = nt(self.emb_tail[...], rows()) * dim**-0.5
        self.store_last(t, z).start()

        def one(i, carry):
            more = lax.rem(i + 1, count)

            @pl.when((i + 1 < count) if final else (i >= 0))
            def _():
                self.tile(more).start()

            self.tile(i).wait()

            @pl.when((i >= TWO) if first else (i >= 0))
            def _():
                self.store(t, z, i).wait()

            self.logits[lax.rem(i, TWO)] = nt(self.tiles[lax.rem(i, TWO)], rows()) * dim**-0.5
            self.store(t, z, i).start()
            return carry

        lax.fori_loop(0, count, one, 0)
        if final:
            self.store(t, z, 0).wait()
            self.store(t, z, 1).wait()
            self.store_last(t, z).wait()

    def run(self, order):
        h = self.here
        for name in ("in", "kv", "out"):
            self.load(name, 0)
        self.tile(0).start()
        self.h[...] = self.h_ref[...].reshape(self.h.shape)
        self.x[...] = self.x_ref[...].reshape(self.x.shape)
        self.wq[self.width : LANES] = jnp.zeros((LANES - self.width, self.dim), BF16)
        self.wo[self.width : LANES] = jnp.zeros((LANES - self.width, self.dim), BF16)
        for at in (0, self.up_at):
            self.wide[at + self.hidden : at + self.up_at] = jnp.zeros((self.up_at - self.hidden, self.dim), BF16)
        meet([h.dev(z, *f) for _, z, f in h.all()])
        placed = set()
        order = "".join(order)
        for letter, code in zip(order[::TWO], order[1::TWO], strict=True):
            who, at = self.stream[letter], STREAMS.index(letter)
            if isinstance(who, tuple):
                self.attend(*who)
                continue
            if letter not in placed and isinstance(who, Gather):
                placed.add(letter)
                core_inner = (h.y, h.x, h.c) if letter in "EF" else (h.c, h.y, h.x)
                self.every[(at % TWO, h.z, *core_inner)] = self.h[at % TWO]
            who.step(code)
            if who.STEPS[CODES.index(code)] == "end":
                who.drain()
                self.all_arrived(at % TWO, self.o_send)
        for letter in "EF":
            self.stream[letter].drain()
        self.loans.settle()


def layers_kernel(layers, names, lengths, x_ref, h_ref, gains, cos, sin, cos_own, sin_own, emb_tail, wg_hbm, wu_hbm, wq_hbm, wkv_hbm,
                  wd_hbm, wo_hbm, k_hbm, v_hbm, emb_hbm, out_hbm, kv_out, *scratch):
    refs = dict(locals(), **dict(zip(names, scratch, strict=True)))
    del refs["names"], refs["scratch"]
    Layers(**refs).run(ORDER)


def relayout_kernel(in_ref, out_ref):
    for t in range(TWO):
        out_ref[:, t, :] = in_ref[t]


def params(index, mib):
    return pltpu.CompilerParams(collective_id=index, has_side_effects=True, vmem_limit_bytes=mib << 20)


def solution(mesh):
    def device_fn(tokens, lengths, embedding, ln_scale, w_q, w_kv, w_o, w_gate, w_up, w_down, final_scale, k_cache, v_cache):
        me = lax.axis_index("tp")
        steps, batch = tokens.shape
        vocab, dim = embedding.shape
        layers, seqs, length, width = k_cache.shape
        hidden = w_gate.shape[-1]
        half = width // TWO
        block = jax.ShapeDtypeStruct((TWO, HALF, dim), BF16)

        def ordered(rows):
            return rows.reshape(TWO, FOUR, TWO, TWO, TWO, HALF).transpose(0, 1, FOUR, TWO, 3, 5).reshape(TWO, FOUR, TWO, LANES)

        positions = lengths[None, :] + jnp.arange(steps, dtype=jnp.int32)[:, None]
        own_len = lax.dynamic_slice_in_dim(lengths, me * seqs, seqs)
        own_pos = own_len[None, :] + jnp.arange(steps, dtype=jnp.int32)[:, None]
        inv_freq = 10000.0 ** (-jnp.arange(half, dtype=F32) / half)
        angles = ordered(positions).reshape(TWO, FOUR, 1, ROWS).astype(F32) * inv_freq[None, None, :, None]
        own_angles = jnp.pad(own_pos, ((0, 0), (0, LANES - HALF)))[:, None, :].astype(F32) * inv_freq[None, :, None]
        tok = ordered(tokens).reshape(TWO, FOUR, TWO, FOUR, HALF).transpose(1, TWO, 3, 0, FOUR).reshape(8, ROWS, 1)
        turns = jnp.cos(angles), jnp.sin(angles), jnp.cos(own_angles), jnp.sin(own_angles)
        gains = jnp.concatenate([ln_scale[1:], final_scale[None]], 0)

        x, h = pl.pallas_call(
            embed_kernel,
            out_shape=(block, block),
            in_specs=[VMEM, ANY, VMEM],
            out_specs=(VMEM, VMEM),
            scratch_shapes=[pltpu.VMEM((vocab, dim), BF16), pltpu.VMEM((LANES, dim), BF16), DMA((1,)), *Reduce.scratch(HALF, dim, BF16)],
            compiler_params=params(0, 60),
            name="embed",
        )(tok, embedding, ln_scale[:1])

        wg_t, wu_t, wkv_t = (w.transpose(0, TWO, 1) for w in (w_gate, w_up, w_kv))
        wq_t = w_q.transpose(0, TWO, 3, 1).reshape(layers, width, dim)
        wo = w_o.reshape(layers, width, dim)
        k_t, v_t = k_cache.transpose(0, 1, 3, TWO), v_cache.transpose(0, 1, 3, TWO)
        padded = pl.cdiv(vocab, 8) * 8
        tail = jnp.pad(embedding[vocab // ROWS * ROWS :], ((0, padded - vocab), (0, 0)))
        scratch = Layers.scratch(dim, hidden, width, seqs, length)
        logits, fresh = pl.pallas_call(
            functools.partial(layers_kernel, layers, tuple(scratch)),
            out_shape=(jax.ShapeDtypeStruct((TWO, padded, batch), F32), jax.ShapeDtypeStruct((layers, TWO, ROWS, HALF), BF16)),
            in_specs=[SMEM] + [VMEM] * 8 + [ANY] * 9,
            out_specs=(ANY, VMEM),
            scratch_shapes=list(scratch.values()),
            compiler_params=params(1, 63),
            name="layers",
        )(own_len, x, h, gains, *turns, tail, wg_t, wu_t, wq_t, wkv_t, w_down, wo, k_t, v_t, embedding)
        logits = pl.pallas_call(
            relayout_kernel,
            grid=(pl.cdiv(vocab, SHEET),),
            out_shape=jax.ShapeDtypeStruct((vocab, TWO, batch), F32),
            in_specs=[pl.BlockSpec((TWO, SHEET, batch), lambda i: (0, i, 0))],
            out_specs=pl.BlockSpec((SHEET, TWO, batch), lambda i: (i, 0, 0)),
            name="relayout",
        )(logits)

        row_ids = lax.broadcasted_iota(jnp.int32, (1, 1, length, 1), TWO)
        new = fresh.reshape(layers, TWO, TWO, LANES, HALF)[:, :, :, :width]

        def written(cache, which):
            for t in range(steps):
                cache = jnp.where(
                    row_ids == own_pos[t][None, :, None, None], new[:, t, which].transpose(0, TWO, 1)[:, :, None, :], cache
                )
            return cache

        return logits.transpose(1, TWO, 0), written(k_cache, 0), written(v_cache, 1)

    cache_spec = P(None, "tp", None, None)
    in_specs = (P(), P(), P("tp", None), P(), P(None, None, "tp", None), P(), P(None, "tp", None, None), P(None, None, "tp"), P(None, None, "tp"), P(None, "tp", None), P(), cache_spec, cache_spec)
    out_specs = (P(None, None, "tp"), cache_spec, cache_spec)
    return jax.shard_map(device_fn, mesh=mesh, in_specs=in_specs, out_specs=out_specs, check_vma=False)
```

```python
import functools

import jax
import jax.numpy as jnp
from jax import lax
from jax.experimental import pallas as pl
from jax.experimental.pallas import tpu as pltpu
from jax.sharding import PartitionSpec as P

LN_EPS = 1e-6
TWO, FOUR = 2, 4
HALF, BLOCK, ROWS, LANES = 32, 64, 256, 128
MESH = pl.DeviceIdType.MESH
BF16, F32 = jnp.bfloat16, jnp.float32
ANY = pl.BlockSpec(memory_space=pl.ANY)
VMEM = pl.BlockSpec(memory_space=pltpu.VMEM)
SMEM = pl.BlockSpec(memory_space=pltpu.SMEM)
DMA = pltpu.SemaphoreType.DMA
FLIPS = [(a, b, e) for a in range(TWO) for b in range(TWO) for e in range(TWO)]
SIDE = 512
ALL = (slice(None),) * 3
CODES = "0123456789abcdefghijklmnopqrstuvwxyz"
STREAMS = "ABCDEFRSTUJKLM"


def numbered(words, slots):
    return tuple(f"{word}{s}" for word in words for s in slots)


TAIL = 40
WIDE = 512
GROUP = 8
SHEET = 264
REDUCE = "37bq2f6paj1e5oi90nhtm4du8lsrcgkv"
ORDER = (
    "A0AqBqB0A4AkA1AlA8A2BlB8B4BkAmA5B1AcArA9A3B2BmA6AaBcBrB3AoAn",
    "B9B5AdBgBoAhAbBaBnAeB6A7ApAiB7BdBpBbAfAgAjBeBhBfBiBjJ0K0R2R1",
    "R6RaS2R3RiReS6SaRpR7RbS3RqS7SiSbR5SpRmRjRfR9R0SqSjSeRoR4S1S5",
    "SfS9RhRsRdSoS0SnRuRnS4R8ShRtSdStRgSuRcS8SmRlSsRrScSgSlSrRkRv",
    "CqC0SkClC2C4CkC1SvDqCaC8C6D0CmDlCcC9C5D2CrD8D4DkD1CgCdC3DcDm",
    "DaDrCeCnD5D9CoD6D3ChC7CbCiDdDgDoDnD7DbCpDeCfDhCjDfDpDiDjL0T2",
    "M0T0T6T3TaT4U2T7TbTpTiTeU3U6UaTqT1TfU7UbUqT5U1ToTmUeUiTjU5T9",
    "UoUfUjU0TsU9ThUpTdU4TuT8UmUnTnTtUhUdUuUtTcTgTlU8UsTrTkUlUrUc",
    "UgTvE0EqUkElE2EkE4E8UvFqF0EcE1EmEaE6ErF4F8FlE3FkEgEoE9E5F1F2",
    "FcEnEeFmFrEbE7F3FgEdEiF5F9F6FaEpEfEhFnFbFoF7FdEjFeFhFpFfFiFj",
)


class Here:
    def __init__(self):
        me = lax.axis_index("tp")
        self.c = lax.rem(me, TWO)
        self.x = lax.rem(lax.div(me, TWO), TWO)
        self.y = lax.rem(lax.div(me, FOUR), TWO)
        z = lax.div(me, 8)
        self.z = z
        self.against = {id(v): 1 - v for v in (self.c, self.x, self.y)}
        inner = lax.rem(lax.div(z + 1, TWO), TWO)
        self.inner = inner == 1
        two, three = lax.rem(z + TWO, FOUR), 3 - z
        self.zs = [z, z + 1 - TWO * lax.rem(z, TWO), inner * three + (1 - inner) * two, inner * two + (1 - inner) * three]
        self.slot = ((z * TWO + self.c) * TWO + self.y) * TWO + self.x
        self.near, self.across = self.dev(self.zs[1]), self.dev(three)
        self.core, self.along_x, self.along_y = self.dev(z, a=1), self.dev(z, e=1), self.dev(z, b=1)

    def flip(self, v, on):
        return self.against[id(v)] if on else v

    def dev(self, z, a=0, b=0, e=0):
        y, x, c = self.flip(self.y, b), self.flip(self.x, e), self.flip(self.c, a)
        return ((z * TWO + y) * TWO + x) * TWO + c

    def apart(self, s):
        inner = lax.rem(lax.div(self.z + 1, TWO), TWO)
        return (0, 1, TWO + inner, 3 - inner)[s]

    def partner(self, s, f):
        a, b, e = lax.div(f, FOUR), lax.rem(lax.div(f, TWO), TWO), lax.rem(f, TWO)
        c, y, x = (on + v - TWO * on * v for on, v in ((a, self.c), (b, self.y), (e, self.x)))
        return self.apart(s) * 8 + f, c, y * TWO + x, ((self.zs[s] * TWO + y) * TWO + x) * TWO + c

    def lines(self):
        return [self.near, self.dev(self.zs[TWO]), self.dev(self.zs[3]), self.core, self.along_x, self.along_y]

    def all(self):
        z = self.z
        zs = [z, self.zs[1], lax.rem(z + TWO, FOUR), 3 - z]
        return [(8 * j + FOUR * a + TWO * b + e, zs[j], (a, b, e)) for j in range(FOUR) for a, b, e in FLIPS if j or a or b or e]


def meet(devices):
    sem = pltpu.get_barrier_semaphore()
    for d in devices:
        pl.semaphore_signal(sem, inc=1, device_id={"tp": d}, device_id_type=MESH)
    pl.semaphore_wait(sem, len(devices))


class Wires:
    def __init__(self, here, send, recv, sizes):
        self.here, self.send, self.recv = here, send, recv
        self.names, self.first, self.started, at = {}, {}, {}, 0
        for kind, count in sizes.items():
            self.first[kind], self.started[kind] = at, []
            at += count

    def go(self, what, src, dst, device, inner=None):
        kind = tuple(src.shape), inner
        k = self.names.setdefault(what, len(self.names))
        copy = pltpu.make_async_remote_copy(
            src_ref=src,
            dst_ref=dst,
            send_sem=self.send.at[self.first[kind] + len(self.started[kind])],
            recv_sem=self.recv.at[k],
            device_id={"tp": device},
            device_id_type=MESH,
        )
        self.started[kind].append(src)
        if inner is None:
            copy.start()
        else:
            pl.when(self.here.inner == inner)(copy.start)

    def got(self, what, like):
        k = self.names.setdefault(what, len(self.names))
        pltpu.make_async_copy(like, like, self.recv.at[k]).wait()

    def step(self, code):
        name = self.STEPS[CODES.index(code)]
        word = name.rstrip(CODES[:FOUR])
        getattr(self, word)(*map(int, name[len(word) :]))

    def run(self, order):
        for code in "".join(order):
            self.step(code)

    def drain(self):
        for (kind, inner), copies in self.started.items():

            def wait(ref=copies[0], first=self.first[kind, inner], count=len(copies)):
                def one(i, carry):
                    pltpu.make_async_copy(ref, ref, self.send.at[first + i]).wait()
                    return carry

                lax.fori_loop(0, count, one, 0)

            if inner is None:
                wait()
            else:
                pl.when(self.here.inner == inner)(wait)


def nt(a, b):
    return lax.dot_general(a, b, (((1,), (1,)), ((), ())), preferred_element_type=F32)


def nn(a, b):
    return lax.dot_general(a, b, (((1,), (0,)), ((), ())), preferred_element_type=F32)


class Gather(Wires):
    COPIES = 48
    STEPS = numbered(("sh", "tx", "ty", "cl", "us"), range(FOUR)) + numbered(("zf", "ff"), range(1, FOUR)) + ("zown", "fown")

    def __init__(self, here, own, plane, send, recv, use):
        rows, dim = own.shape[1:]
        main, four = ((TWO, rows, dim - SIDE)), (TWO, TWO, TWO, rows, SIDE)
        sizes = {(main, None): 19, (main, True): FOUR, ((TWO, rows, dim), None): 6, (four, None): FOUR, (four, True): FOUR}
        super().__init__(here, send, recv, sizes | {(main[1:], None): 6, ((rows, dim), None): TWO})
        self.own, self.plane, self.use = own, plane, use
        self.main, self.side, self.full = pl.ds(0, dim - SIDE), pl.ds(dim - SIDE, SIDE), pl.ds(0, dim)

    def at(self, s, b=0, e=0):
        h = self.here
        return self.plane(h.zs[s], h.c).at[h.flip(h.y, b), h.flip(h.x, e)].at[:, :, self.main if s else self.full]

    def fours(self, s):
        return self.plane(self.here.zs[s], self.here.c).at[:, :, :, :, self.side]

    def pass_on(self, what, s, ref):
        h = self.here
        self.go((what, 3 if s == 1 else s), ref, ref, h.across if s == 1 else h.near, True)

    def zown(self):
        h = self.here
        src, dst = self.own.at[:, :, self.main], self.at(0).at[:, :, self.main]
        self.go(("z", 1), src, dst, h.near)
        self.go(("z", TWO), src, dst, h.across, True)

    def zf(self, s):
        self.got(("z", s), self.at(s))
        self.pass_on("z", s, self.at(s))

    def fown(self):
        h, ref = self.here, self.fours(0)
        self.go(("f", 1), ref, ref, h.near)
        self.go(("f", TWO), ref, ref, h.across, True)

    def ff(self, s):
        ref = self.fours(s)
        self.got(("f", s), ref)
        self.pass_on("f", s, ref)
        self.go(("cf", s), ref, ref, self.here.core)

    def sh(self, s):
        h, dst = self.here, self.at(s)
        src = dst if s else self.own
        self.go(("x", s), src, dst, h.along_x)
        self.go(("y", s), src, dst, h.along_y)
        self.go(("c", s), src, dst, h.core)

    def tx(self, s):
        ref = self.at(s, e=1)
        self.got(("x", s), ref)
        self.go(("xy", s), ref.at[0], ref.at[0], self.here.along_y)
        self.go(("cx", s), ref, ref, self.here.core)

    def ty(self, s):
        ref = self.at(s, b=1)
        self.got(("y", s), ref)
        self.go(("yx", s), ref.at[1], ref.at[1], self.here.along_x)
        self.go(("cy", s), ref, ref, self.here.core)

    def cl(self, s):
        ref = self.at(s, 1, 1)
        self.got(("xy", s), ref.at[0])
        self.got(("yx", s), ref.at[1])
        self.go(("cd", s), ref, ref, self.here.core)

    def us(self, s):
        for what in ("c", "cx", "cy", "cd"):
            self.got((what, s), self.at(s))
        if s:
            self.got(("cf", s), self.fours(s))
        self.use(s)


class Loans:
    def __init__(self, here, send, free):
        self.here, self.send, self.free = here, send, free
        self.lent, self.out = [], set()

    def take(self, s):
        if s in self.out:
            pl.semaphore_wait(self.free.at[s], 1)
        self.out.add(s)

    def give(self, s):
        pl.semaphore_signal(self.free.at[s], inc=1, device_id={"tp": self.here.core}, device_id_type=MESH)

    def settle(self):
        for copy in self.lent[-TWO:]:
            copy.wait_send()
        for s in self.out:
            pl.semaphore_wait(self.free.at[s], 1)


class Reduce(Wires):
    COPIES = 48
    STEPS = numbered(("fo", "ca", *"dpqu"), range(FOUR)) + numbered(("fz", "gz"), range(1, FOUR)) + ("fin", "end")

    @staticmethod
    def scratch(rows, dim, dtype):
        return [
            pltpu.VMEM((FOUR, FOUR, TWO, rows, dim), dtype),
            pltpu.VMEM((TWO, FOUR, TWO, rows, dim), dtype),
            pltpu.VMEM((FOUR, FOUR, TWO, rows, dim), dtype),
            pltpu.VMEM((FOUR, TWO, rows, dim), dtype),
            pltpu.VMEM((FOUR, TWO, rows, dim), dtype),
            pltpu.VMEM((FOUR, TWO, rows, dim), dtype),
            pltpu.VMEM((5, TWO, rows, dim - SIDE), dtype),
            pltpu.VMEM((5, FOUR, TWO, rows, SIDE), dtype),
            DMA((Reduce.COPIES,)),
            DMA((Reduce.COPIES,)),
            DMA((TWO,)),
            pltpu.SemaphoreType.REGULAR((FOUR,)),
        ]

    def __init__(self, here, fill, finish, loans, part, sib, core_in, diag_in, x_in, y_in, z_in, side_in, send, recv):
        rows, dim = part.shape[3:]
        main, four = (TWO, rows, dim - SIDE), (FOUR, TWO, rows, SIDE)
        sizes = {(main[1:], None): 18, ((rows, dim), None): 6, (four, True): 3, (four, False): 3, (main, True): 3, (main, False): 3}
        super().__init__(here, send, recv, sizes)
        self.fill, self.finish, self.loans = fill, finish, loans
        self.part, self.sib, self.core_in, self.diag_in = part, sib, core_in, diag_in
        self.x_in, self.y_in, self.z_in, self.side_in = x_in, y_in, z_in, side_in
        dim = part.shape[-1]
        self.main, self.side, self.full = pl.ds(0, dim - SIDE), pl.ds(dim - SIDE, SIDE), pl.ds(0, dim)

    def quad(self, b, e):
        h = self.here
        return h.flip(h.y, b) * TWO + h.flip(h.x, e)

    def piece(self, buf, s, *where):
        return buf, (s, *where, slice(None), self.main if s else self.full)

    def add(self, ref, *more):
        buf, index = ref
        total = buf[index]
        for other, where in more:
            total = total + other[where]
        buf[index] = total

    def fo(self, s):
        loans, n = self.loans, len(self.loans.lent)
        if n > 1:
            loans.lent[n - TWO].wait_send()
        k = self.names.setdefault(("c", s), len(self.names))
        copy = pltpu.make_async_remote_copy(
            src_ref=self.sib.at[n % TWO],
            dst_ref=self.core_in.at[s],
            send_sem=loans.send.at[n % TWO],
            recv_sem=self.recv.at[k],
            device_id={"tp": self.here.core},
            device_id_type=MESH,
        )

        def send():
            loans.take(s)
            copy.start()
            loans.lent.append(copy)

        self.fill(s, self.sib.at[n % TWO], self.part.at[s], send)

    def ca(self, s):
        self.got(("c", s), self.core_in.at[s])
        for t in range(TWO):

            def add(i, carry):
                self.add((self.part, (s, i, t)), (self.core_in, (s, i, t)))
                return carry

            lax.fori_loop(0, FOUR, add, 0)
        self.loans.give(s)

    def along_z(self, what, s, ref, landing):
        h = self.here
        k = 5 if s == 1 else s
        to = 1 if s == 1 else s + TWO

        @pl.when(h.inner)
        def _():
            self.got((what, k), landing.at[k - 1])
            self.add(ref, (landing, k - 1))

        self.go((what, to), ref[0].at[ref[1]], landing.at[to - 1], h.near if s == 1 else h.across, True)
        self.go((what, s), ref[0].at[ref[1]], landing.at[s - 1], h.near, False)

    def last_z(self, what, ref, landing):
        self.got((what, 1), landing.at[0])
        self.add(ref, (landing, 0))

        @pl.when(self.here.inner)
        def _():
            self.got((what, FOUR), landing.at[3])
            self.add(ref, (landing, 3))

    def fz(self, s):
        self.along_z("f", s, (self.part, (s, *ALL, self.side)), self.side_in)

    def fin(self):
        self.last_z("f", (self.part, (0, *ALL, self.side)), self.side_in)

    def d(self, s):
        h, part = self.here, self.part
        far = self.quad(1, 1)
        self.pass_on("dy", s, self.piece(part, s, far, 0), self.piece(self.diag_in, s, 0), h.along_y)
        self.pass_on("dx", s, self.piece(part, s, far, 1), self.piece(self.diag_in, s, 1), h.along_x)
        self.pass_on("x1", s, self.piece(part, s, self.quad(0, 1), 1), self.piece(self.x_in, s, 1), h.along_x)
        self.pass_on("y0", s, self.piece(part, s, self.quad(1, 0), 0), self.piece(self.y_in, s, 0), h.along_y)

    def pass_on(self, what, s, src, dst, device):
        self.go((what, s), src[0].at[src[1]], dst[0].at[dst[1]], device)

    def came(self, what, s, ref):
        self.got((what, s), ref[0].at[ref[1]])

    def p(self, s):
        ref = self.piece(self.part, s, self.quad(0, 1), 0)
        self.came("dy", s, ref)
        self.add(ref, self.piece(self.diag_in, s, 0))
        self.pass_on("x0", s, ref, self.piece(self.x_in, s, 0), self.here.along_x)

    def q(self, s):
        ref = self.piece(self.part, s, self.quad(1, 0), 1)
        self.came("dx", s, ref)
        self.add(ref, self.piece(self.diag_in, s, 1))
        self.pass_on("y1", s, ref, self.piece(self.y_in, s, 1), self.here.along_y)

    def u(self, s):
        for t in range(TWO):
            ref = self.piece(self.part, s, self.quad(0, 0), t)
            self.came(f"x{t}", s, ref)
            self.came(f"y{t}", s, ref)
            self.add(ref, self.piece(self.x_in, s, t), self.piece(self.y_in, s, t))

    def gz(self, s):
        self.along_z("g", s, (self.part, (s, self.quad(0, 0), *ALL[:TWO], self.main)), self.z_in)

    def end(self):
        mine = self.quad(0, 0)
        self.last_z("g", (self.part, (0, mine, *ALL[:TWO], self.main)), self.z_in)
        for t in range(TWO):
            for lo in range(0, self.part.shape[3], 16):
                self.finish(t, lo, self.part[0, mine, t, lo : lo + 16])


def normed(x, gain):
    rows = x.astype(F32)
    centred = rows - jnp.mean(rows, axis=-1, keepdims=True)
    var = jnp.mean(centred * centred, axis=-1, keepdims=True)
    return (centred * lax.rsqrt(var + LN_EPS) * gain).astype(BF16)


def load(pairs, sems):
    copies = [pltpu.make_async_copy(src, dst, sems.at[i]) for i, (src, dst) in enumerate(pairs)]
    for copy in copies:
        copy.start()
    return copies


def embed_kernel(tok_ref, emb_hbm, gain_ref, x_ref, h_ref, emb, tail, sem, *scratch):
    here = Here()
    vocab, dim = emb_hbm.shape
    whole = vocab // ROWS * ROWS
    rest = vocab - whole
    (fetch,) = load([(emb_hbm, emb)], sem)
    meet(here.lines())
    fetch.wait()
    tail[...] = jnp.zeros_like(tail)
    tail[0:rest] = emb[whole:vocab]
    base = lax.axis_index("tp") * vocab

    def fill(s, other, own, send):
        for core, ref, then in ((here.flip(here.c, 1), other, send), (here.c, own, None)):
            tok = tok_ref[here.zs[s] * TWO + core] - base
            hot = (tok == lax.broadcasted_iota(jnp.int32, (ROWS, whole), 1)).astype(F32).astype(BF16)
            hot_tail = (tok == lax.broadcasted_iota(jnp.int32, (ROWS, LANES), 1) + whole).astype(F32).astype(BF16)

            def columns(n, carry):
                cols = pl.ds(pl.multiple_of(n * ROWS, ROWS), ROWS)
                rows = nn(hot, emb[0:whole, cols]) + nn(hot_tail, tail[:, cols])
                ref[:, :, :, cols] = rows.astype(BF16).reshape(FOUR, TWO, HALF, ROWS)
                return carry

            lax.fori_loop(0, dim // ROWS, columns, 0)
            if then:
                then()

    def finish(t, lo, rows):
        x_ref[t, lo : lo + 16] = rows
        h_ref[t, lo : lo + 16] = normed(rows, gain_ref[...])

    *rs, lent, free = scratch
    loans = Loans(here, lent, free)
    red = Reduce(here, fill, finish, loans, *rs)
    red.run(REDUCE)
    red.drain()
    loans.settle()


def attention(t, lengths, q_rows, fresh, keys, values, o_rows):
    seqs, width, length = keys.shape
    col = lax.broadcasted_iota(jnp.int32, (HALF, length), 1)
    blank = jnp.zeros((LANES - width, length), BF16)

    def several(i, carry):
        some = [i * GROUP + u for u in range(GROUP)]
        pos = [lengths[s] for s in some]
        q = [q_rows[pl.ds(s, HALF, stride=HALF), :] for s in some]
        new = [[fresh[step, pl.ds(s, 1), :] for step in range(t + 1)] for s in some]
        score = [nn(a.astype(BF16), jnp.concatenate([keys[s], blank], 0)) for a, s in zip(q, some)]
        own = [[jnp.sum(a * row[:, 0:LANES], axis=-1, keepdims=True) for row in rows] for a, rows in zip(q, new)]
        for u in range(GROUP):
            for step in range(t + 1):
                score[u] = jnp.where(col == pos[u] + step, own[u][step], score[u])
            score[u] = jnp.where(col <= pos[u] + t, score[u] * width**-0.5, -jnp.inf)
        top = [jnp.max(a, axis=-1, keepdims=True) for a in score]
        weight = [jnp.exp(a - b) for a, b in zip(score, top)]
        total = [jnp.sum(a, axis=-1, keepdims=True) for a in weight]
        weight = [(a / b).astype(BF16).astype(F32) for a, b in zip(weight, total)]
        at = [[col == p + step for step in range(t + 1)] for p in pos]
        mine = [[jnp.sum(jnp.where(hit, a, 0.0), axis=-1, keepdims=True) for hit in hits] for a, hits in zip(weight, at)]
        for u in range(GROUP):
            for hit in at[u]:
                weight[u] = jnp.where(hit, 0.0, weight[u])
        out = [nt(a.astype(BF16), jnp.concatenate([values[s], blank], 0)) for a, s in zip(weight, some)]
        for u in range(GROUP):
            for step in range(t + 1):
                out[u] = out[u] + mine[u][step] * new[u][step][:, LANES:ROWS]
            o_rows[pl.ds(some[u], HALF, stride=HALF), :] = out[u]
        return carry

    lax.fori_loop(0, seqs // GROUP, several, 0)


class Layers:
    @staticmethod
    def scratch(dim, hidden, width, seqs, length):
        up_at = pl.cdiv(hidden, LANES) * LANES
        return dict(
            x=pltpu.VMEM((TWO, TWO, 16, dim), BF16),
            h=pltpu.VMEM((TWO, TWO, 16, dim), BF16),
            every=pltpu.VMEM((TWO, FOUR, TWO, TWO, TWO, TWO, 16, dim), BF16),
            wide=pltpu.VMEM((TWO * up_at, dim), BF16),
            wq=pltpu.VMEM((LANES, dim), BF16),
            wkv=pltpu.VMEM((TWO * width, dim), BF16),
            wd=pltpu.VMEM((hidden, dim), BF16),
            wo=pltpu.VMEM((LANES, dim), BF16),
            ready=pltpu.VMEM((ROWS, TWO * up_at), F32),
            m=pltpu.VMEM((TWO, FOUR, ROWS, hidden), BF16),
            q_out=pltpu.VMEM((TWO, FOUR, TWO, FOUR, HALF, LANES), BF16),
            q_in=pltpu.VMEM((TWO, 8, FOUR, HALF, LANES), BF16),
            o_out=pltpu.VMEM((TWO, 8, FOUR, HALF, LANES), BF16),
            o_in=pltpu.VMEM((TWO, 8, FOUR, HALF, LANES), BF16),
            q_rows=pltpu.VMEM((1024, LANES), F32),
            o_rows=pltpu.VMEM((1024, LANES), F32),
            fresh=pltpu.VMEM((TWO, LANES, ROWS), F32),
            keys=pltpu.VMEM((seqs, width, length), BF16),
            values=pltpu.VMEM((seqs, width, length), BF16),
            tiles=pltpu.VMEM((3, ROWS, dim), BF16),
            logits=pltpu.VMEM((TWO, ROWS, ROWS), F32),
            last=pltpu.VMEM((TAIL, ROWS), F32),
            w_sem=DMA((8,)),
            tile_sem=DMA((3,)),
            logit_sem=DMA((3,)),
            q_send=DMA((TWO, HALF)),
            q_recv=DMA((TWO, HALF)),
            o_send=DMA((TWO, HALF)),
            o_recv=DMA((TWO, HALF)),
            g_send=DMA((TWO, Gather.COPIES)),
            g_recv=DMA((TWO, Gather.COPIES)),
            part=pltpu.VMEM((TWO, FOUR, FOUR, TWO, 16, dim), F32),
            sib=pltpu.VMEM((TWO, FOUR, TWO, 16, dim), F32),
            core_in=pltpu.VMEM((FOUR, FOUR, TWO, 16, dim), F32),
            diag_in=pltpu.VMEM((TWO, FOUR, TWO, 16, dim), F32),
            x_in=pltpu.VMEM((TWO, FOUR, TWO, 16, dim), F32),
            y_in=pltpu.VMEM((TWO, FOUR, TWO, 16, dim), F32),
            z_in=pltpu.VMEM((TWO, 5, TWO, 16, dim - SIDE), F32),
            side_in=pltpu.VMEM((TWO, 5, FOUR, TWO, 16, SIDE), F32),
            r_send=DMA((TWO, Reduce.COPIES)),
            r_recv=DMA((TWO, Reduce.COPIES)),
            lent=DMA((TWO,)),
            free=pltpu.SemaphoreType.REGULAR((FOUR,)),
        )

    def __init__(self, layers, **refs):
        self.__dict__.update(refs)
        here = self.here = Here()
        self.count = layers
        self.dim, self.hidden, self.width = self.h.shape[-1], self.m.shape[-1], self.keys.shape[1]
        self.up_at = self.wide.shape[0] // TWO
        self.whole = self.emb_hbm.shape[0] // ROWS * ROWS
        self.loads, self.answered, self.heads, self.fills = {}, set(), 0, 0
        self.stream = {}
        self.loans = Loans(here, self.lent, self.free)
        letters = iter(STREAMS)
        for l in range(layers + 1):
            for t in range(TWO):
                use = functools.partial(self.project if l < layers else self.head, l, t)
                if l < layers:
                    plane = functools.partial(lambda t, z, c: self.every.at[t, z, c], t)
                else:
                    plane = functools.partial(lambda t, z, c: self.every.at[t, z, :, :, c], t)
                self.stream[next(letters)] = Gather(here, self.h.at[t], plane, self.g_send.at[t], self.g_recv.at[t], use)
        for l in range(layers):
            for t in range(TWO):
                fill, finish = functools.partial(self.fill, l, t), functools.partial(self.finish, l, t)
                mine = [ref.at[t] for ref in (self.diag_in, self.x_in, self.y_in, self.z_in, self.side_in, self.r_send, self.r_recv)]
                reduce = Reduce(here, fill, finish, self.loans, self.part.at[t], self.sib, self.core_in, *mine)
                self.stream[next(letters)] = reduce
        for l in range(layers):
            for t in range(TWO):
                self.stream[next(letters)] = (l, t)

    def load(self, name, l):
        groups = {
            "in": [(self.wg_hbm, self.wide.at[0 : self.hidden]), (self.wu_hbm, self.wide.at[self.up_at : self.up_at + self.hidden]),
                   (self.wq_hbm, self.wq.at[0 : self.width])],
            "out": [(self.wd_hbm, self.wd), (self.wo_hbm, self.wo.at[0 : self.width])],
            "kv": [(self.wkv_hbm, self.wkv), (self.k_hbm, self.keys), (self.v_hbm, self.values)],
        }
        first = {"in": 0, "out": 3, "kv": 5}[name]
        copies = [pltpu.make_async_copy(src.at[l], dst, self.w_sem.at[first + i]) for i, (src, dst) in enumerate(groups[name])]
        for copy in copies:
            copy.start()
        self.loads[name] = copies

    def ready_for(self, name):
        for copy in self.loads.pop(name, ()):
            copy.wait()

    def turned(self, rows, cos, sin):
        half = self.width // TWO
        lo, hi = rows[0:half], rows[half : self.width]
        return lo * cos - hi * sin, lo * sin + hi * cos

    def each(self, s, body, own=None):
        if s == 0 and own:
            own(self.here.c, self.here.y * TWO + self.here.x)

        def one(f, carry):
            body(*self.here.partner(s, f))
            return carry

        lax.fori_loop(0 if s else 1, 8, one, 0)

    def trip(self, kind, t, r, src, dst, device):
        sends, recvs = (self.q_send, self.q_recv) if kind == "q" else (self.o_send, self.o_recv)
        return pltpu.make_async_remote_copy(
            src_ref=src, dst_ref=dst, send_sem=sends.at[t, r], recv_sem=recvs.at[t, r], device_id={"tp": device}, device_id_type=MESH
        )

    def arrived(self, sems, t, r):
        ref = self.q_in.at[t, 0, 0]
        pltpu.make_async_copy(ref, ref, sems.at[t, r]).wait()

    def all_arrived(self, t, *sems):
        def one(r, carry):
            for sem in sems:
                self.arrived(sem, t, r)
            return carry

        lax.fori_loop(1, HALF, one, 0)

    def mine(self):
        h = self.here
        return h.z * TWO + h.c, h.y * TWO + h.x

    def project(self, l, t, s):
        self.ready_for("in")
        z, dim = self.here.zs[s], self.dim

        def rows():
            return self.every[t, z].reshape(ROWS, dim)

        q = nt(self.wq[...], rows())
        lo, hi = self.turned(q, self.cos[t, z], self.sin[t, z])
        q = jnp.concatenate([lo, hi, jnp.zeros((LANES - self.width, ROWS), F32)], 0)
        self.q_out[t, z] = q.T.astype(BF16).reshape(TWO, FOUR, HALF, LANES)
        zc, quad = self.mine()

        def ask(r, core, four, device):
            self.trip("q", t, r, self.q_out.at[t, z, core, four], self.q_in.at[t, zc, quad], device).start()

        def keep(core, four):
            self.q_in[t, zc, quad] = self.q_out[t, z, core, four]

        self.each(s, ask, keep)

        def tile(n, carry):
            cols = pl.ds(pl.multiple_of(n * ROWS, ROWS), ROWS)
            self.ready[:, cols] = nt(rows(), self.wide[cols])
            return carry

        lax.fori_loop(0, self.wide.shape[0] // ROWS, tile, 0)

        def gated(n, carry):
            some = pl.ds(pl.multiple_of(n * HALF, HALF), HALF)
            gate, up = self.ready[some, 0 : self.hidden], self.ready[some, self.up_at : self.up_at + self.hidden]
            self.m[t, z, some] = (gate * jax.nn.sigmoid(gate) * up).astype(BF16)
            return carry

        lax.fori_loop(0, 8, gated, 0)

    def attend(self, l, t):
        width = self.width
        self.ready_for("kv")
        self.stream[STREAMS[TWO * l + t]].drain()
        self.all_arrived(t, self.q_recv, self.q_send)
        mine = jnp.concatenate([self.h[t].reshape(HALF, self.dim), jnp.zeros((LANES - HALF, self.dim), BF16)], 0)
        rows = nt(self.wkv[...], mine)
        lo, hi = self.turned(rows, self.cos_own[t], self.sin_own[t])
        blank = jnp.zeros((LANES - width, LANES), BF16)
        new = jnp.concatenate([jnp.concatenate([lo, hi], 0).astype(BF16), blank, rows[width:].astype(BF16), blank], 0)
        self.kv_out[l, t] = new[:, 0:HALF]
        self.fresh[t] = new.astype(F32).T
        self.q_rows[...] = self.q_in[t].reshape(1024, LANES).astype(F32)
        attention(t, self.lengths, self.q_rows, self.fresh, self.keys, self.values, self.o_rows)
        self.o_out[t] = self.o_rows[...].astype(BF16).reshape(8, FOUR, HALF, LANES)
        zc, quad = self.mine()
        for s in range(FOUR):
            z = self.here.zs[s]

            def answer(r, core, four, device, z=z):
                self.trip("o", t, r, self.o_out.at[t, z * TWO + core, four], self.o_in.at[t, zc, quad], device).start()

            def keep(core, four, z=z):
                self.o_in[t, zc, quad] = self.o_out[t, z * TWO + core, four]

            self.each(s, answer, keep)
        if t and l + 1 < self.count:
            self.load("in", l + 1)
            self.load("kv", l + 1)

    def fill(self, l, t, s, other, own, send):
        self.ready_for("out")
        if (l, t, s) not in self.answered:
            self.answered.add((l, t, s))
            self.each(s, lambda r, core, four, device: self.arrived(self.o_recv, t, r))
        z, c = self.here.zs[s], self.here.c
        cores = self.here.flip(c, 1), c
        heads = jnp.concatenate([self.o_in[t, z * TWO + core].reshape(LANES, LANES) for core in cores], 0)
        hidden = jnp.concatenate([self.m[t, z, pl.ds(pl.multiple_of(core * LANES, LANES), LANES)] for core in cores], 0)

        def columns(n, carry):
            cols = pl.ds(pl.multiple_of(n * WIDE, WIDE), WIDE)
            rows = nn(heads, self.wo[:, cols]) + nn(hidden, self.wd[:, cols])
            other[:, :, :, cols] = rows[0:LANES].reshape(FOUR, TWO, 16, WIDE)
            own[:, :, :, cols] = rows[LANES:].reshape(FOUR, TWO, 16, WIDE)
            return carry

        lax.fori_loop(0, self.dim // WIDE, columns, 0)
        send()
        self.fills += 1
        if self.fills == 8 * (l + 1) and l + 1 < self.count:
            self.load("out", l + 1)

    def finish(self, l, t, half, lo, rows):
        x = (self.x[t, half].astype(F32) + rows).astype(BF16)
        self.x[t, half] = x
        self.h[t, half] = normed(x, self.gains[pl.ds(l, 1)])

    def tile(self, i):
        at = lax.rem(i, 3)
        return pltpu.make_async_copy(self.emb_hbm.at[pl.ds(pl.multiple_of(i * ROWS, ROWS), ROWS)], self.tiles.at[at], self.tile_sem.at[at])

    def store(self, t, z, i):
        at = lax.rem(i, TWO)
        rows, cols = pl.ds(pl.multiple_of(i * ROWS, ROWS), ROWS), pl.ds(pl.multiple_of(z * ROWS, ROWS), ROWS)
        return pltpu.make_async_copy(self.logits.at[at], self.out_hbm.at[t, rows, cols], self.logit_sem.at[at])

    def store_last(self, t, z):
        rows, cols = pl.ds(self.whole, TAIL), pl.ds(pl.multiple_of(z * ROWS, ROWS), ROWS)
        return pltpu.make_async_copy(self.last, self.out_hbm.at[t, rows, cols], self.logit_sem.at[TWO])

    def head(self, l, t, s):
        z, dim, count = self.here.zs[s], self.dim, self.whole // ROWS
        first, final = self.heads == 0, self.heads == 7
        self.heads += 1

        def rows():
            return self.every[t, z].reshape(ROWS, dim)

        if not first:
            self.store_last(t, z).wait()
        self.last[...] = nt(self.emb_tail[...], rows()) * dim**-0.5
        self.store_last(t, z).start()

        def one(i, carry):
            @pl.when((i + TWO < count) if final else (i >= 0))
            def _():
                self.tile(lax.rem(i + TWO, count)).start()

            self.tile(i).wait()

            @pl.when((i >= TWO) if first else (i >= 0))
            def _():
                self.store(t, z, i).wait()

            self.logits[lax.rem(i, TWO)] = nt(self.tiles[lax.rem(i, 3)], rows()) * dim**-0.5
            self.store(t, z, i).start()
            return carry

        lax.fori_loop(0, count, one, 0)
        if final:
            self.store(t, z, 0).wait()
            self.store(t, z, 1).wait()
            self.store_last(t, z).wait()

    def run(self, order):
        h = self.here
        for name in ("in", "kv", "out"):
            self.load(name, 0)
        self.tile(0).start()
        self.tile(1).start()
        self.h[...] = self.h_ref[...].reshape(self.h.shape)
        self.x[...] = self.x_ref[...].reshape(self.x.shape)
        self.wq[self.width : LANES] = jnp.zeros((LANES - self.width, self.dim), BF16)
        self.wo[self.width : LANES] = jnp.zeros((LANES - self.width, self.dim), BF16)
        for at in (0, self.up_at):
            self.wide[at + self.hidden : at + self.up_at] = jnp.zeros((self.up_at - self.hidden, self.dim), BF16)
        meet([h.dev(z, *f) for _, z, f in h.all()])
        placed = set()
        order = "".join(order)
        for letter, code in zip(order[::TWO], order[1::TWO], strict=True):
            who, at = self.stream[letter], STREAMS.index(letter)
            if isinstance(who, tuple):
                self.attend(*who)
                continue
            if letter not in placed and isinstance(who, Gather):
                placed.add(letter)
                core_inner = (h.y, h.x, h.c) if letter in "EF" else (h.c, h.y, h.x)
                self.every[(at % TWO, h.z, *core_inner)] = self.h[at % TWO]
            who.step(code)
            if who.STEPS[CODES.index(code)] == "end":
                who.drain()
                self.all_arrived(at % TWO, self.o_send)
        for letter in "EF":
            self.stream[letter].drain()
        self.loans.settle()


def layers_kernel(layers, names, lengths, x_ref, h_ref, gains, cos, sin, cos_own, sin_own, emb_tail, wg_hbm, wu_hbm, wq_hbm, wkv_hbm,
                  wd_hbm, wo_hbm, k_hbm, v_hbm, emb_hbm, out_hbm, kv_out, *scratch):
    refs = dict(locals(), **dict(zip(names, scratch, strict=True)))
    del refs["names"], refs["scratch"]
    Layers(**refs).run(ORDER)


def relayout_kernel(in_ref, out_ref):
    for t in range(TWO):
        out_ref[:, t, :] = in_ref[t]


def params(index, mib):
    return pltpu.CompilerParams(collective_id=index, has_side_effects=True, vmem_limit_bytes=mib << 20)


def solution(mesh):
    def device_fn(tokens, lengths, embedding, ln_scale, w_q, w_kv, w_o, w_gate, w_up, w_down, final_scale, k_cache, v_cache):
        me = lax.axis_index("tp")
        steps, batch = tokens.shape
        vocab, dim = embedding.shape
        layers, seqs, length, width = k_cache.shape
        hidden = w_gate.shape[-1]
        half = width // TWO
        block = jax.ShapeDtypeStruct((TWO, HALF, dim), BF16)

        def ordered(rows):
            return rows.reshape(TWO, FOUR, TWO, TWO, TWO, HALF).transpose(0, 1, FOUR, TWO, 3, 5).reshape(TWO, FOUR, TWO, LANES)

        positions = lengths[None, :] + jnp.arange(steps, dtype=jnp.int32)[:, None]
        own_len = lax.dynamic_slice_in_dim(lengths, me * seqs, seqs)
        own_pos = own_len[None, :] + jnp.arange(steps, dtype=jnp.int32)[:, None]
        inv_freq = 10000.0 ** (-jnp.arange(half, dtype=F32) / half)
        angles = ordered(positions).reshape(TWO, FOUR, 1, ROWS).astype(F32) * inv_freq[None, None, :, None]
        own_angles = jnp.pad(own_pos, ((0, 0), (0, LANES - HALF)))[:, None, :].astype(F32) * inv_freq[None, :, None]
        tok = ordered(tokens).reshape(TWO, FOUR, TWO, FOUR, HALF).transpose(1, TWO, 3, 0, FOUR).reshape(8, ROWS, 1)
        turns = jnp.cos(angles), jnp.sin(angles), jnp.cos(own_angles), jnp.sin(own_angles)
        gains = jnp.concatenate([ln_scale[1:], final_scale[None]], 0)

        x, h = pl.pallas_call(
            embed_kernel,
            out_shape=(block, block),
            in_specs=[VMEM, ANY, VMEM],
            out_specs=(VMEM, VMEM),
            scratch_shapes=[pltpu.VMEM((vocab, dim), BF16), pltpu.VMEM((LANES, dim), BF16), DMA((1,)), *Reduce.scratch(HALF, dim, BF16)],
            compiler_params=params(0, 60),
            name="embed",
        )(tok, embedding, ln_scale[:1])

        wg_t, wu_t, wkv_t = (w.transpose(0, TWO, 1) for w in (w_gate, w_up, w_kv))
        wq_t = w_q.transpose(0, TWO, 3, 1).reshape(layers, width, dim)
        wo = w_o.reshape(layers, width, dim)
        k_t, v_t = k_cache.transpose(0, 1, 3, TWO), v_cache.transpose(0, 1, 3, TWO)
        padded = pl.cdiv(vocab, 8) * 8
        tail = jnp.pad(embedding[vocab // ROWS * ROWS :], ((0, padded - vocab), (0, 0)))
        scratch = Layers.scratch(dim, hidden, width, seqs, length)
        logits, fresh = pl.pallas_call(
            functools.partial(layers_kernel, layers, tuple(scratch)),
            out_shape=(jax.ShapeDtypeStruct((TWO, padded, batch), F32), jax.ShapeDtypeStruct((layers, TWO, ROWS, HALF), BF16)),
            in_specs=[SMEM] + [VMEM] * 8 + [ANY] * 9,
            out_specs=(ANY, VMEM),
            scratch_shapes=list(scratch.values()),
            compiler_params=params(1, 63),
            name="layers",
        )(own_len, x, h, gains, *turns, tail, wg_t, wu_t, wq_t, wkv_t, w_down, wo, k_t, v_t, embedding)
        logits = pl.pallas_call(
            relayout_kernel,
            grid=(pl.cdiv(vocab, SHEET),),
            out_shape=jax.ShapeDtypeStruct((vocab, TWO, batch), F32),
            in_specs=[pl.BlockSpec((TWO, SHEET, batch), lambda i: (0, i, 0))],
            out_specs=pl.BlockSpec((SHEET, TWO, batch), lambda i: (i, 0, 0)),
            name="relayout",
        )(logits)

        row_ids = lax.broadcasted_iota(jnp.int32, (1, 1, length, 1), TWO)
        new = fresh.reshape(layers, TWO, TWO, LANES, HALF)[:, :, :, :width]

        def written(cache, which):
            for t in range(steps):
                cache = jnp.where(
                    row_ids == own_pos[t][None, :, None, None], new[:, t, which].transpose(0, TWO, 1)[:, :, None, :], cache
                )
            return cache

        return logits.transpose(1, TWO, 0), written(k_cache, 0), written(v_cache, 1)

    cache_spec = P(None, "tp", None, None)
    in_specs = (P(), P(), P("tp", None), P(), P(None, None, "tp", None), P(), P(None, "tp", None, None), P(None, None, "tp"), P(None, None, "tp"), P(None, "tp", None), P(), cache_spec, cache_spec)
    out_specs = (P(None, None, "tp"), cache_spec, cache_spec)
    return jax.shard_map(device_fn, mesh=mesh, in_specs=in_specs, out_specs=out_specs, check_vma=False)
```

```python
import functools

import jax
import jax.numpy as jnp
from jax import lax
from jax.experimental import pallas as pl
from jax.experimental.pallas import tpu as pltpu
from jax.sharding import PartitionSpec as P

LN_EPS = 1e-6
TWO, FOUR = 2, 4
HALF, BLOCK, ROWS, LANES = 32, 64, 256, 128
MESH = pl.DeviceIdType.MESH
BF16, F32 = jnp.bfloat16, jnp.float32
ANY = pl.BlockSpec(memory_space=pl.ANY)
VMEM = pl.BlockSpec(memory_space=pltpu.VMEM)
SMEM = pl.BlockSpec(memory_space=pltpu.SMEM)
DMA = pltpu.SemaphoreType.DMA
FLIPS = [(a, b, e) for a in range(TWO) for b in range(TWO) for e in range(TWO)]
SIDE = 512
ALL = (slice(None),) * 3
CODES = "0123456789abcdefghijklmnopqrstuvwxyz"
STREAMS = "ABCDEFRSTUJKLM"


def numbered(words, slots):
    return tuple(f"{word}{s}" for word in words for s in slots)


TAIL = 40
WIDE = 512
GROUP = 8
REDUCE = "37bq2f6paj1e5oi90nhtm4du8lsrcgkv"
ORDER = (
    "A0AqBqB0A4AkA1AlA8A2BlB8B4BkAmA5B1AcArA9A3B2BmA6AaBcBrB3AoAn",
    "B9B5AdBgBoAhAbBaBnAeB6A7ApAiB7BdBpBbAfAgAjBeBhBfBiBjJ0K0R2R1",
    "R6RaS2R3RiReS6SaRpR7RbS3RqS7SiSbR5SpRmRjRfR9R0SqSjSeRoR4S1S5",
    "SfS9RhRsRdSoS0SnRuRnS4R8ShRtSdStRgSuRcS8SmRlSsRrScSgSlSrRkRv",
    "CqC0SkClC2C4CkC1SvDqCaC8C6D0CmDlCcC9C5D2CrD8D4DkD1CgCdC3DcDm",
    "DaDrCeCnD5D9CoD6D3ChC7CbCiDdDgDoDnD7DbCpDeCfDhCjDfDpDiDjL0T2",
    "M0T0T6T3TaT4U2T7TbTpTiTeU3U6UaTqT1TfU7UbUqT5U1ToTmUeUiTjU5T9",
    "UoUfUjU0TsU9ThUpTdU4TuT8UmUnTnTtUhUdUuUtTcTgTlU8UsTrTkUlUrUc",
    "UgTvE0EqUkElE2EkE4E8UvFqF0EcE1EmEaE6ErF4F8FlE3FkEgEoE9E5F1F2",
    "FcEnEeFmFrEbE7F3FgEdEiF5F9F6FaEpEfEhFnFbFoF7FdEjFeFhFpFfFiFj",
)


class Here:
    def __init__(self):
        me = lax.axis_index("tp")
        self.c = lax.rem(me, TWO)
        self.x = lax.rem(lax.div(me, TWO), TWO)
        self.y = lax.rem(lax.div(me, FOUR), TWO)
        z = lax.div(me, 8)
        self.z = z
        self.against = {id(v): 1 - v for v in (self.c, self.x, self.y)}
        inner = lax.rem(lax.div(z + 1, TWO), TWO)
        self.inner = inner == 1
        two, three = lax.rem(z + TWO, FOUR), 3 - z
        self.zs = [z, z + 1 - TWO * lax.rem(z, TWO), inner * three + (1 - inner) * two, inner * two + (1 - inner) * three]
        self.slot = ((z * TWO + self.c) * TWO + self.y) * TWO + self.x
        self.near, self.across = self.dev(self.zs[1]), self.dev(three)
        self.core, self.along_x, self.along_y = self.dev(z, a=1), self.dev(z, e=1), self.dev(z, b=1)

    def flip(self, v, on):
        return self.against[id(v)] if on else v

    def dev(self, z, a=0, b=0, e=0):
        y, x, c = self.flip(self.y, b), self.flip(self.x, e), self.flip(self.c, a)
        return ((z * TWO + y) * TWO + x) * TWO + c

    def apart(self, s):
        inner = lax.rem(lax.div(self.z + 1, TWO), TWO)
        return (0, 1, TWO + inner, 3 - inner)[s]

    def partner(self, s, f):
        a, b, e = lax.div(f, FOUR), lax.rem(lax.div(f, TWO), TWO), lax.rem(f, TWO)
        c, y, x = (on + v - TWO * on * v for on, v in ((a, self.c), (b, self.y), (e, self.x)))
        return self.apart(s) * 8 + f, c, y * TWO + x, ((self.zs[s] * TWO + y) * TWO + x) * TWO + c

    def lines(self):
        return [self.near, self.dev(self.zs[TWO]), self.dev(self.zs[3]), self.core, self.along_x, self.along_y]

    def all(self):
        z = self.z
        zs = [z, self.zs[1], lax.rem(z + TWO, FOUR), 3 - z]
        return [(8 * j + FOUR * a + TWO * b + e, zs[j], (a, b, e)) for j in range(FOUR) for a, b, e in FLIPS if j or a or b or e]


def meet(devices):
    sem = pltpu.get_barrier_semaphore()
    for d in devices:
        pl.semaphore_signal(sem, inc=1, device_id={"tp": d}, device_id_type=MESH)
    pl.semaphore_wait(sem, len(devices))


class Wires:
    def __init__(self, here, send, recv, sizes):
        self.here, self.send, self.recv = here, send, recv
        self.names, self.first, self.started, at = {}, {}, {}, 0
        for kind, count in sizes.items():
            self.first[kind], self.started[kind] = at, []
            at += count

    def go(self, what, src, dst, device, inner=None):
        kind = tuple(src.shape), inner
        k = self.names.setdefault(what, len(self.names))
        copy = pltpu.make_async_remote_copy(
            src_ref=src,
            dst_ref=dst,
            send_sem=self.send.at[self.first[kind] + len(self.started[kind])],
            recv_sem=self.recv.at[k],
            device_id={"tp": device},
            device_id_type=MESH,
        )
        self.started[kind].append(src)
        if inner is None:
            copy.start()
        else:
            pl.when(self.here.inner == inner)(copy.start)

    def got(self, what, like):
        k = self.names.setdefault(what, len(self.names))
        pltpu.make_async_copy(like, like, self.recv.at[k]).wait()

    def step(self, code):
        name = self.STEPS[CODES.index(code)]
        word = name.rstrip(CODES[:FOUR])
        getattr(self, word)(*map(int, name[len(word) :]))

    def run(self, order):
        for code in "".join(order):
            self.step(code)

    def drain(self):
        for (kind, inner), copies in self.started.items():

            def wait(ref=copies[0], first=self.first[kind, inner], count=len(copies)):
                def one(i, carry):
                    pltpu.make_async_copy(ref, ref, self.send.at[first + i]).wait()
                    return carry

                lax.fori_loop(0, count, one, 0)

            if inner is None:
                wait()
            else:
                pl.when(self.here.inner == inner)(wait)


def nt(a, b):
    return lax.dot_general(a, b, (((1,), (1,)), ((), ())), preferred_element_type=F32)


def nn(a, b):
    return lax.dot_general(a, b, (((1,), (0,)), ((), ())), preferred_element_type=F32)


class Gather(Wires):
    COPIES = 48
    STEPS = numbered(("sh", "tx", "ty", "cl", "us"), range(FOUR)) + numbered(("zf", "ff"), range(1, FOUR)) + ("zown", "fown")

    def __init__(self, here, own, plane, send, recv, use):
        rows, dim = own.shape[1:]
        main, four = ((TWO, rows, dim - SIDE)), (TWO, TWO, TWO, rows, SIDE)
        sizes = {(main, None): 19, (main, True): FOUR, ((TWO, rows, dim), None): 6, (four, None): FOUR, (four, True): FOUR}
        super().__init__(here, send, recv, sizes | {(main[1:], None): 6, ((rows, dim), None): TWO})
        self.own, self.plane, self.use = own, plane, use
        self.main, self.side, self.full = pl.ds(0, dim - SIDE), pl.ds(dim - SIDE, SIDE), pl.ds(0, dim)

    def at(self, s, b=0, e=0):
        h = self.here
        return self.plane(h.zs[s], h.c).at[h.flip(h.y, b), h.flip(h.x, e)].at[:, :, self.main if s else self.full]

    def fours(self, s):
        return self.plane(self.here.zs[s], self.here.c).at[:, :, :, :, self.side]

    def pass_on(self, what, s, ref):
        h = self.here
        self.go((what, 3 if s == 1 else s), ref, ref, h.across if s == 1 else h.near, True)

    def zown(self):
        h = self.here
        src, dst = self.own.at[:, :, self.main], self.at(0).at[:, :, self.main]
        self.go(("z", 1), src, dst, h.near)
        self.go(("z", TWO), src, dst, h.across, True)

    def zf(self, s):
        self.got(("z", s), self.at(s))
        self.pass_on("z", s, self.at(s))

    def fown(self):
        h, ref = self.here, self.fours(0)
        self.go(("f", 1), ref, ref, h.near)
        self.go(("f", TWO), ref, ref, h.across, True)

    def ff(self, s):
        ref = self.fours(s)
        self.got(("f", s), ref)
        self.pass_on("f", s, ref)
        self.go(("cf", s), ref, ref, self.here.core)

    def sh(self, s):
        h, dst = self.here, self.at(s)
        src = dst if s else self.own
        self.go(("x", s), src, dst, h.along_x)
        self.go(("y", s), src, dst, h.along_y)
        self.go(("c", s), src, dst, h.core)

    def tx(self, s):
        ref = self.at(s, e=1)
        self.got(("x", s), ref)
        self.go(("xy", s), ref.at[0], ref.at[0], self.here.along_y)
        self.go(("cx", s), ref, ref, self.here.core)

    def ty(self, s):
        ref = self.at(s, b=1)
        self.got(("y", s), ref)
        self.go(("yx", s), ref.at[1], ref.at[1], self.here.along_x)
        self.go(("cy", s), ref, ref, self.here.core)

    def cl(self, s):
        ref = self.at(s, 1, 1)
        self.got(("xy", s), ref.at[0])
        self.got(("yx", s), ref.at[1])
        self.go(("cd", s), ref, ref, self.here.core)

    def us(self, s):
        for what in ("c", "cx", "cy", "cd"):
            self.got((what, s), self.at(s))
        if s:
            self.got(("cf", s), self.fours(s))
        self.use(s)


class Loans:
    def __init__(self, here, send, free):
        self.here, self.send, self.free = here, send, free
        self.lent, self.out = [], set()

    def take(self, s):
        if s in self.out:
            pl.semaphore_wait(self.free.at[s], 1)
        self.out.add(s)

    def give(self, s):
        pl.semaphore_signal(self.free.at[s], inc=1, device_id={"tp": self.here.core}, device_id_type=MESH)

    def settle(self):
        for copy in self.lent[-TWO:]:
            copy.wait_send()
        for s in self.out:
            pl.semaphore_wait(self.free.at[s], 1)


class Reduce(Wires):
    COPIES = 48
    STEPS = numbered(("fo", "ca", *"dpqu"), range(FOUR)) + numbered(("fz", "gz"), range(1, FOUR)) + ("fin", "end")

    @staticmethod
    def scratch(rows, dim, dtype):
        return [
            pltpu.VMEM((FOUR, FOUR, TWO, rows, dim), dtype),
            pltpu.VMEM((TWO, FOUR, TWO, rows, dim), dtype),
            pltpu.VMEM((FOUR, FOUR, TWO, rows, dim), dtype),
            pltpu.VMEM((FOUR, TWO, rows, dim), dtype),
            pltpu.VMEM((FOUR, TWO, rows, dim), dtype),
            pltpu.VMEM((FOUR, TWO, rows, dim), dtype),
            pltpu.VMEM((5, TWO, rows, dim - SIDE), dtype),
            pltpu.VMEM((5, FOUR, TWO, rows, SIDE), dtype),
            DMA((Reduce.COPIES,)),
            DMA((Reduce.COPIES,)),
            DMA((TWO,)),
            pltpu.SemaphoreType.REGULAR((FOUR,)),
        ]

    def __init__(self, here, fill, finish, loans, part, sib, core_in, diag_in, x_in, y_in, z_in, side_in, send, recv):
        rows, dim = part.shape[3:]
        main, four = (TWO, rows, dim - SIDE), (FOUR, TWO, rows, SIDE)
        sizes = {(main[1:], None): 18, ((rows, dim), None): 6, (four, True): 3, (four, False): 3, (main, True): 3, (main, False): 3}
        super().__init__(here, send, recv, sizes)
        self.fill, self.finish, self.loans = fill, finish, loans
        self.part, self.sib, self.core_in, self.diag_in = part, sib, core_in, diag_in
        self.x_in, self.y_in, self.z_in, self.side_in = x_in, y_in, z_in, side_in
        dim = part.shape[-1]
        self.main, self.side, self.full = pl.ds(0, dim - SIDE), pl.ds(dim - SIDE, SIDE), pl.ds(0, dim)

    def quad(self, b, e):
        h = self.here
        return h.flip(h.y, b) * TWO + h.flip(h.x, e)

    def piece(self, buf, s, *where):
        return buf, (s, *where, slice(None), self.main if s else self.full)

    def add(self, ref, *more):
        buf, index = ref
        total = buf[index]
        for other, where in more:
            total = total + other[where]
        buf[index] = total

    def fo(self, s):
        loans, n = self.loans, len(self.loans.lent)
        if n > 1:
            loans.lent[n - TWO].wait_send()
        k = self.names.setdefault(("c", s), len(self.names))
        copy = pltpu.make_async_remote_copy(
            src_ref=self.sib.at[n % TWO],
            dst_ref=self.core_in.at[s],
            send_sem=loans.send.at[n % TWO],
            recv_sem=self.recv.at[k],
            device_id={"tp": self.here.core},
            device_id_type=MESH,
        )

        def send():
            loans.take(s)
            copy.start()
            loans.lent.append(copy)

        self.fill(s, self.sib.at[n % TWO], self.part.at[s], send)

    def ca(self, s):
        self.got(("c", s), self.core_in.at[s])
        for t in range(TWO):

            def add(i, carry):
                self.add((self.part, (s, i, t)), (self.core_in, (s, i, t)))
                return carry

            lax.fori_loop(0, FOUR, add, 0)
        self.loans.give(s)

    def along_z(self, what, s, ref, landing):
        h = self.here
        k = 5 if s == 1 else s
        to = 1 if s == 1 else s + TWO

        @pl.when(h.inner)
        def _():
            self.got((what, k), landing.at[k - 1])
            self.add(ref, (landing, k - 1))

        self.go((what, to), ref[0].at[ref[1]], landing.at[to - 1], h.near if s == 1 else h.across, True)
        self.go((what, s), ref[0].at[ref[1]], landing.at[s - 1], h.near, False)

    def last_z(self, what, ref, landing):
        self.got((what, 1), landing.at[0])
        self.add(ref, (landing, 0))

        @pl.when(self.here.inner)
        def _():
            self.got((what, FOUR), landing.at[3])
            self.add(ref, (landing, 3))

    def fz(self, s):
        self.along_z("f", s, (self.part, (s, *ALL, self.side)), self.side_in)

    def fin(self):
        self.last_z("f", (self.part, (0, *ALL, self.side)), self.side_in)

    def d(self, s):
        h, part = self.here, self.part
        far = self.quad(1, 1)
        self.pass_on("dy", s, self.piece(part, s, far, 0), self.piece(self.diag_in, s, 0), h.along_y)
        self.pass_on("dx", s, self.piece(part, s, far, 1), self.piece(self.diag_in, s, 1), h.along_x)
        self.pass_on("x1", s, self.piece(part, s, self.quad(0, 1), 1), self.piece(self.x_in, s, 1), h.along_x)
        self.pass_on("y0", s, self.piece(part, s, self.quad(1, 0), 0), self.piece(self.y_in, s, 0), h.along_y)

    def pass_on(self, what, s, src, dst, device):
        self.go((what, s), src[0].at[src[1]], dst[0].at[dst[1]], device)

    def came(self, what, s, ref):
        self.got((what, s), ref[0].at[ref[1]])

    def p(self, s):
        ref = self.piece(self.part, s, self.quad(0, 1), 0)
        self.came("dy", s, ref)
        self.add(ref, self.piece(self.diag_in, s, 0))
        self.pass_on("x0", s, ref, self.piece(self.x_in, s, 0), self.here.along_x)

    def q(self, s):
        ref = self.piece(self.part, s, self.quad(1, 0), 1)
        self.came("dx", s, ref)
        self.add(ref, self.piece(self.diag_in, s, 1))
        self.pass_on("y1", s, ref, self.piece(self.y_in, s, 1), self.here.along_y)

    def u(self, s):
        for t in range(TWO):
            ref = self.piece(self.part, s, self.quad(0, 0), t)
            self.came(f"x{t}", s, ref)
            self.came(f"y{t}", s, ref)
            self.add(ref, self.piece(self.x_in, s, t), self.piece(self.y_in, s, t))

    def gz(self, s):
        self.along_z("g", s, (self.part, (s, self.quad(0, 0), *ALL[:TWO], self.main)), self.z_in)

    def end(self):
        mine = self.quad(0, 0)
        self.last_z("g", (self.part, (0, mine, *ALL[:TWO], self.main)), self.z_in)
        for t in range(TWO):
            for lo in range(0, self.part.shape[3], 16):
                self.finish(t, lo, self.part[0, mine, t, lo : lo + 16])


def normed(x, gain):
    rows = x.astype(F32)
    centred = rows - jnp.mean(rows, axis=-1, keepdims=True)
    var = jnp.mean(centred * centred, axis=-1, keepdims=True)
    return (centred * lax.rsqrt(var + LN_EPS) * gain).astype(BF16)


def load(pairs, sems):
    copies = [pltpu.make_async_copy(src, dst, sems.at[i]) for i, (src, dst) in enumerate(pairs)]
    for copy in copies:
        copy.start()
    return copies


def embed_kernel(tok_ref, emb_hbm, gain_ref, x_ref, h_ref, emb, tail, sem, *scratch):
    here = Here()
    vocab, dim = emb_hbm.shape
    whole = vocab // ROWS * ROWS
    rest = vocab - whole
    (fetch,) = load([(emb_hbm, emb)], sem)
    meet(here.lines())
    fetch.wait()
    tail[...] = jnp.zeros_like(tail)
    tail[0:rest] = emb[whole:vocab]
    toks = tok_ref[...].astype(F32).T.astype(jnp.int32) - lax.axis_index("tp") * vocab

    def fill(s, other, own, send):
        for core, ref, then in ((here.flip(here.c, 1), other, send), (here.c, own, None)):
            row = here.zs[s] * TWO + core
            tok = jnp.sum(jnp.where(lax.broadcasted_iota(jnp.int32, (ROWS, 8), 1) == row, toks, 0), axis=1, keepdims=True)
            hot = (tok == lax.broadcasted_iota(jnp.int32, (ROWS, whole), 1)).astype(F32).astype(BF16)
            hot_tail = (tok == lax.broadcasted_iota(jnp.int32, (ROWS, LANES), 1) + whole).astype(F32).astype(BF16)

            def columns(n, carry):
                cols = pl.ds(pl.multiple_of(n * WIDE, WIDE), WIDE)
                rows = nn(hot, emb[0:whole, cols]) + nn(hot_tail, tail[:, cols])
                ref[:, :, :, cols] = rows.astype(BF16).reshape(FOUR, TWO, HALF, WIDE)
                return carry

            lax.fori_loop(0, dim // WIDE, columns, 0)
            if then:
                then()

    def finish(t, lo, rows):
        x_ref[t, lo : lo + 16] = rows
        h_ref[t, lo : lo + 16] = normed(rows, gain_ref[0:1])

    *rs, lent, free = scratch
    loans = Loans(here, lent, free)
    red = Reduce(here, fill, finish, loans, *rs)
    red.run(REDUCE)
    red.drain()
    loans.settle()


def attention(t, lengths, q_rows, fresh, keys, values, o_rows):
    seqs, width, length = keys.shape
    col = lax.broadcasted_iota(jnp.int32, (HALF, length), 1)
    blank = jnp.zeros((LANES - width, length), BF16)

    def several(i, carry):
        some = [i * GROUP + u for u in range(GROUP)]
        pos = [lengths[s] for s in some]
        q = [q_rows[pl.ds(s, HALF, stride=HALF), :] for s in some]
        new = [[fresh[step, pl.ds(s, 1), :] for step in range(t + 1)] for s in some]
        score = [nn(a.astype(BF16), jnp.concatenate([keys[s], blank], 0)) for a, s in zip(q, some)]
        own = [[jnp.sum(a * row[:, 0:LANES], axis=-1, keepdims=True) for row in rows] for a, rows in zip(q, new)]
        for u in range(GROUP):
            for step in range(t + 1):
                score[u] = jnp.where(col == pos[u] + step, own[u][step], score[u])
            score[u] = jnp.where(col <= pos[u] + t, score[u] * width**-0.5, -jnp.inf)
        top = [jnp.max(a, axis=-1, keepdims=True) for a in score]
        weight = [jnp.exp(a - b) for a, b in zip(score, top)]
        total = [jnp.sum(a, axis=-1, keepdims=True) for a in weight]
        weight = [(a / b).astype(BF16).astype(F32) for a, b in zip(weight, total)]
        at = [[col == p + step for step in range(t + 1)] for p in pos]
        mine = [[jnp.sum(jnp.where(hit, a, 0.0), axis=-1, keepdims=True) for hit in hits] for a, hits in zip(weight, at)]
        for u in range(GROUP):
            for hit in at[u]:
                weight[u] = jnp.where(hit, 0.0, weight[u])
        out = [nt(a.astype(BF16), jnp.concatenate([values[s], blank], 0)) for a, s in zip(weight, some)]
        for u in range(GROUP):
            for step in range(t + 1):
                out[u] = out[u] + mine[u][step] * new[u][step][:, LANES:ROWS]
            o_rows[pl.ds(some[u], HALF, stride=HALF), :] = out[u]
        return carry

    lax.fori_loop(0, seqs // GROUP, several, 0)


class Layers:
    @staticmethod
    def scratch(dim, hidden, width, seqs, length):
        up_at = pl.cdiv(hidden, LANES) * LANES
        return dict(
            x=pltpu.VMEM((TWO, TWO, 16, dim), BF16),
            h=pltpu.VMEM((TWO, TWO, 16, dim), BF16),
            every=pltpu.VMEM((TWO, FOUR, TWO, TWO, TWO, TWO, 16, dim), BF16),
            wide=pltpu.VMEM((TWO * up_at, dim), BF16),
            wq=pltpu.VMEM((LANES, dim), BF16),
            wkv=pltpu.VMEM((TWO * width, dim), BF16),
            wd=pltpu.VMEM((hidden, dim), BF16),
            wo=pltpu.VMEM((LANES, dim), BF16),
            ready=pltpu.VMEM((ROWS, TWO * up_at), F32),
            m=pltpu.VMEM((TWO, FOUR, ROWS, hidden), BF16),
            q_out=pltpu.VMEM((TWO, FOUR, TWO, FOUR, HALF, LANES), BF16),
            q_in=pltpu.VMEM((TWO, 8, FOUR, HALF, LANES), BF16),
            o_out=pltpu.VMEM((TWO, 8, FOUR, HALF, LANES), BF16),
            o_in=pltpu.VMEM((TWO, 8, FOUR, HALF, LANES), BF16),
            q_rows=pltpu.VMEM((1024, LANES), F32),
            o_rows=pltpu.VMEM((1024, LANES), F32),
            fresh=pltpu.VMEM((TWO, LANES, ROWS), F32),
            keys=pltpu.VMEM((seqs, width, length), BF16),
            values=pltpu.VMEM((seqs, width, length), BF16),
            tiles=pltpu.VMEM((3, ROWS, dim), BF16),
            logits=pltpu.VMEM((TWO, ROWS, ROWS), F32),
            last=pltpu.VMEM((TAIL, ROWS), F32),
            w_sem=DMA((8,)),
            tile_sem=DMA((3,)),
            logit_sem=DMA((3,)),
            q_send=DMA((TWO, HALF)),
            q_recv=DMA((TWO, HALF)),
            o_send=DMA((TWO, HALF)),
            o_recv=DMA((TWO, HALF)),
            g_send=DMA((TWO, Gather.COPIES)),
            g_recv=DMA((TWO, Gather.COPIES)),
            part=pltpu.VMEM((TWO, FOUR, FOUR, TWO, 16, dim), F32),
            sib=pltpu.VMEM((TWO, FOUR, TWO, 16, dim), F32),
            core_in=pltpu.VMEM((FOUR, FOUR, TWO, 16, dim), F32),
            diag_in=pltpu.VMEM((TWO, FOUR, TWO, 16, dim), F32),
            x_in=pltpu.VMEM((TWO, FOUR, TWO, 16, dim), F32),
            y_in=pltpu.VMEM((TWO, FOUR, TWO, 16, dim), F32),
            z_in=pltpu.VMEM((TWO, 5, TWO, 16, dim - SIDE), F32),
            side_in=pltpu.VMEM((TWO, 5, FOUR, TWO, 16, SIDE), F32),
            r_send=DMA((TWO, Reduce.COPIES)),
            r_recv=DMA((TWO, Reduce.COPIES)),
            lent=DMA((TWO,)),
            free=pltpu.SemaphoreType.REGULAR((FOUR,)),
        )

    def __init__(self, layers, **refs):
        self.__dict__.update(refs)
        here = self.here = Here()
        self.count = layers
        self.dim, self.hidden, self.width = self.h.shape[-1], self.m.shape[-1], self.keys.shape[1]
        self.up_at = self.wide.shape[0] // TWO
        self.whole = self.emb_hbm.shape[0] // ROWS * ROWS
        self.loads, self.answered, self.heads, self.fills = {}, set(), 0, 0
        self.stream = {}
        self.loans = Loans(here, self.lent, self.free)
        letters = iter(STREAMS)
        for l in range(layers + 1):
            for t in range(TWO):
                use = functools.partial(self.project if l < layers else self.head, l, t)
                if l < layers:
                    plane = functools.partial(lambda t, z, c: self.every.at[t, z, c], t)
                else:
                    plane = functools.partial(lambda t, z, c: self.every.at[t, z, :, :, c], t)
                self.stream[next(letters)] = Gather(here, self.h.at[t], plane, self.g_send.at[t], self.g_recv.at[t], use)
        for l in range(layers):
            for t in range(TWO):
                fill, finish = functools.partial(self.fill, l, t), functools.partial(self.finish, l, t)
                mine = [ref.at[t] for ref in (self.diag_in, self.x_in, self.y_in, self.z_in, self.side_in, self.r_send, self.r_recv)]
                reduce = Reduce(here, fill, finish, self.loans, self.part.at[t], self.sib, self.core_in, *mine)
                self.stream[next(letters)] = reduce
        for l in range(layers):
            for t in range(TWO):
                self.stream[next(letters)] = (l, t)

    def load(self, name, l):
        groups = {
            "in": [(self.wg_hbm, self.wide.at[0 : self.hidden]), (self.wu_hbm, self.wide.at[self.up_at : self.up_at + self.hidden]),
                   (self.wq_hbm, self.wq.at[0 : self.width])],
            "out": [(self.wd_hbm, self.wd), (self.wo_hbm, self.wo.at[0 : self.width])],
            "kv": [(self.wkv_hbm, self.wkv), (self.k_hbm, self.keys), (self.v_hbm, self.values)],
        }
        first = {"in": 0, "out": 3, "kv": 5}[name]
        copies = [pltpu.make_async_copy(src.at[l], dst, self.w_sem.at[first + i]) for i, (src, dst) in enumerate(groups[name])]
        for copy in copies:
            copy.start()
        self.loads[name] = copies

    def ready_for(self, name):
        for copy in self.loads.pop(name, ()):
            copy.wait()

    def turned(self, rows, cos, sin):
        half = self.width // TWO
        lo, hi = rows[0:half], rows[half : self.width]
        return lo * cos - hi * sin, lo * sin + hi * cos

    def each(self, s, body, own=None):
        if s == 0 and own:
            own(self.here.c, self.here.y * TWO + self.here.x)

        def one(f, carry):
            body(*self.here.partner(s, f))
            return carry

        lax.fori_loop(0 if s else 1, 8, one, 0)

    def trip(self, kind, t, r, src, dst, device):
        sends, recvs = (self.q_send, self.q_recv) if kind == "q" else (self.o_send, self.o_recv)
        return pltpu.make_async_remote_copy(
            src_ref=src, dst_ref=dst, send_sem=sends.at[t, r], recv_sem=recvs.at[t, r], device_id={"tp": device}, device_id_type=MESH
        )

    def arrived(self, sems, t, r):
        ref = self.q_in.at[t, 0, 0]
        pltpu.make_async_copy(ref, ref, sems.at[t, r]).wait()

    def all_arrived(self, t, *sems):
        def one(r, carry):
            for sem in sems:
                self.arrived(sem, t, r)
            return carry

        lax.fori_loop(1, HALF, one, 0)

    def mine(self):
        h = self.here
        return h.z * TWO + h.c, h.y * TWO + h.x

    def project(self, l, t, s):
        self.ready_for("in")
        z, dim = self.here.zs[s], self.dim

        def rows():
            return self.every[t, z].reshape(ROWS, dim)

        q = nt(self.wq[...], rows())
        lo, hi = self.turned(q, self.cos[t, z], self.sin[t, z])
        q = jnp.concatenate([lo, hi, jnp.zeros((LANES - self.width, ROWS), F32)], 0)
        self.q_out[t, z] = q.T.astype(BF16).reshape(TWO, FOUR, HALF, LANES)
        zc, quad = self.mine()

        def ask(r, core, four, device):
            self.trip("q", t, r, self.q_out.at[t, z, core, four], self.q_in.at[t, zc, quad], device).start()

        def keep(core, four):
            self.q_in[t, zc, quad] = self.q_out[t, z, core, four]

        self.each(s, ask, keep)

        def tile(n, carry):
            cols = pl.ds(pl.multiple_of(n * ROWS, ROWS), ROWS)
            self.ready[:, cols] = nt(rows(), self.wide[cols])
            return carry

        lax.fori_loop(0, self.wide.shape[0] // ROWS, tile, 0)

        def gated(n, carry):
            some = pl.ds(pl.multiple_of(n * HALF, HALF), HALF)
            gate, up = self.ready[some, 0 : self.hidden], self.ready[some, self.up_at : self.up_at + self.hidden]
            self.m[t, z, some] = (gate * jax.nn.sigmoid(gate) * up).astype(BF16)
            return carry

        lax.fori_loop(0, 8, gated, 0)

    def attend(self, l, t):
        width = self.width
        self.ready_for("kv")
        self.stream[STREAMS[TWO * l + t]].drain()
        self.all_arrived(t, self.q_recv, self.q_send)
        mine = jnp.concatenate([self.h[t].reshape(HALF, self.dim), jnp.zeros((LANES - HALF, self.dim), BF16)], 0)
        rows = nt(self.wkv[...], mine)
        lo, hi = self.turned(rows, self.cos_own[t], self.sin_own[t])
        blank = jnp.zeros((LANES - width, LANES), BF16)
        new = jnp.concatenate([jnp.concatenate([lo, hi], 0).astype(BF16), blank, rows[width:].astype(BF16), blank], 0)
        self.kv_out[l, :, HALF * t : HALF * t + HALF] = new[:, 0:HALF]
        self.fresh[t] = new.astype(F32).T
        self.q_rows[...] = self.q_in[t].reshape(1024, LANES).astype(F32)
        attention(t, self.lengths, self.q_rows, self.fresh, self.keys, self.values, self.o_rows)
        self.o_out[t] = self.o_rows[...].astype(BF16).reshape(8, FOUR, HALF, LANES)
        zc, quad = self.mine()
        for s in range(FOUR):
            z = self.here.zs[s]

            def answer(r, core, four, device, z=z):
                self.trip("o", t, r, self.o_out.at[t, z * TWO + core, four], self.o_in.at[t, zc, quad], device).start()

            def keep(core, four, z=z):
                self.o_in[t, zc, quad] = self.o_out[t, z * TWO + core, four]

            self.each(s, answer, keep)
        if t and l + 1 < self.count:
            self.load("in", l + 1)
            self.load("kv", l + 1)

    def fill(self, l, t, s, other, own, send):
        self.ready_for("out")
        if (l, t, s) not in self.answered:
            self.answered.add((l, t, s))
            self.each(s, lambda r, core, four, device: self.arrived(self.o_recv, t, r))
        z, c = self.here.zs[s], self.here.c
        cores = self.here.flip(c, 1), c
        heads = jnp.concatenate([self.o_in[t, z * TWO + core].reshape(LANES, LANES) for core in cores], 0)
        hidden = jnp.concatenate([self.m[t, z, pl.ds(pl.multiple_of(core * LANES, LANES), LANES)] for core in cores], 0)

        def columns(n, carry):
            cols = pl.ds(pl.multiple_of(n * WIDE, WIDE), WIDE)
            rows = nn(heads, self.wo[:, cols]) + nn(hidden, self.wd[:, cols])
            other[:, :, :, cols] = rows[0:LANES].reshape(FOUR, TWO, 16, WIDE)
            own[:, :, :, cols] = rows[LANES:].reshape(FOUR, TWO, 16, WIDE)
            return carry

        lax.fori_loop(0, self.dim // WIDE, columns, 0)
        send()
        self.fills += 1
        if self.fills == 8 * (l + 1) and l + 1 < self.count:
            self.load("out", l + 1)

    def finish(self, l, t, half, lo, rows):
        x = (self.x[t, half].astype(F32) + rows).astype(BF16)
        self.x[t, half] = x
        self.h[t, half] = normed(x, self.gains[l + 1 : l + TWO] if l + 1 < self.count else self.last_gain[...])

    def tile(self, i):
        at = lax.rem(i, 3)
        return pltpu.make_async_copy(self.emb_hbm.at[pl.ds(pl.multiple_of(i * ROWS, ROWS), ROWS)], self.tiles.at[at], self.tile_sem.at[at])

    def store(self, t, z, i):
        at = lax.rem(i, TWO)
        rows, cols = pl.ds(pl.multiple_of(i * ROWS, ROWS), ROWS), pl.ds(pl.multiple_of(z * ROWS, ROWS), ROWS)
        return pltpu.make_async_copy(self.logits.at[at], self.out_hbm.at[t, rows, cols], self.logit_sem.at[at])

    def store_last(self, t, z):
        rows, cols = pl.ds(self.whole, TAIL), pl.ds(pl.multiple_of(z * ROWS, ROWS), ROWS)
        return pltpu.make_async_copy(self.last, self.out_hbm.at[t, rows, cols], self.logit_sem.at[TWO])

    def head(self, l, t, s):
        z, dim, count = self.here.zs[s], self.dim, self.whole // ROWS
        first, final = self.heads == 0, self.heads == 7
        self.heads += 1

        def rows():
            return self.every[t, z].reshape(ROWS, dim)

        if not first:
            self.store_last(t, z).wait()
        self.last[...] = nt(self.emb_tail[...], rows()) * dim**-0.5
        self.store_last(t, z).start()

        def one(i, carry):
            @pl.when((i + TWO < count) if final else (i >= 0))
            def _():
                self.tile(lax.rem(i + TWO, count)).start()

            self.tile(i).wait()

            @pl.when((i >= TWO) if first else (i >= 0))
            def _():
                self.store(t, z, i).wait()

            self.logits[lax.rem(i, TWO)] = nt(self.tiles[lax.rem(i, 3)], rows()) * dim**-0.5
            self.store(t, z, i).start()
            return carry

        lax.fori_loop(0, count, one, 0)
        if final:
            self.store(t, z, 0).wait()
            self.store(t, z, 1).wait()
            self.store_last(t, z).wait()

    def run(self, order):
        h = self.here
        for name in ("in", "kv", "out"):
            self.load(name, 0)
        self.tile(0).start()
        self.tile(1).start()
        self.h[...] = self.h_ref[...].reshape(self.h.shape)
        self.x[...] = self.x_ref[...].reshape(self.x.shape)
        self.wq[self.width : LANES] = jnp.zeros((LANES - self.width, self.dim), BF16)
        self.wo[self.width : LANES] = jnp.zeros((LANES - self.width, self.dim), BF16)
        for at in (0, self.up_at):
            self.wide[at + self.hidden : at + self.up_at] = jnp.zeros((self.up_at - self.hidden, self.dim), BF16)
        meet([h.dev(z, *f) for _, z, f in h.all()])
        placed = set()
        order = "".join(order)
        for letter, code in zip(order[::TWO], order[1::TWO], strict=True):
            who, at = self.stream[letter], STREAMS.index(letter)
            if isinstance(who, tuple):
                self.attend(*who)
                continue
            if letter not in placed and isinstance(who, Gather):
                placed.add(letter)
                core_inner = (h.y, h.x, h.c) if letter in "EF" else (h.c, h.y, h.x)
                self.every[(at % TWO, h.z, *core_inner)] = self.h[at % TWO]
            who.step(code)
            if who.STEPS[CODES.index(code)] == "end":
                who.drain()
                self.all_arrived(at % TWO, self.o_send)
        for letter in "EF":
            self.stream[letter].drain()
        self.loans.settle()


def layers_kernel(layers, names, lengths, x_ref, h_ref, gains, last_gain, cos, sin, cos_own, sin_own, emb_tail, wg_hbm, wu_hbm, wq_hbm, wkv_hbm,
                  wd_hbm, wo_hbm, k_hbm, v_hbm, emb_hbm, out_hbm, kv_out, *scratch):
    refs = dict(locals(), **dict(zip(names, scratch, strict=True)))
    del refs["names"], refs["scratch"]
    Layers(**refs).run(ORDER)


def last_kernel(lengths, in_ref, k_ref, v_ref, new_ref, out_ref, k_out, v_out):
    for t in range(TWO):
        out_ref[:, t, :] = in_ref[t]
    some, width, length = k_ref.shape
    seqs = lengths.shape[0]
    row = lax.broadcasted_iota(jnp.int32, (TWO * seqs, length), 0)
    col = lax.broadcasted_iota(jnp.int32, (TWO * seqs, length), 1)
    cols = lax.broadcasted_iota(jnp.int32, (width, length), 1)
    first = lax.rem(pl.program_id(0) * some, seqs)
    pos = [lengths[first + u] for u in range(some)]
    place = [((row == first + u) & (col == p)) | ((row == first + u + seqs) & (col == p + 1)) for u, p in enumerate(pos)]
    new = [nn(new_ref[0], a.astype(F32).astype(BF16)).astype(BF16) for a in place]
    for u, p in enumerate(pos):
        fresh = (cols == p) | (cols == p + 1)
        k_out[u] = jnp.where(fresh, new[u][0:width], k_ref[u])
        v_out[u] = jnp.where(fresh, new[u][LANES : LANES + width], v_ref[u])


def params(index, mib):
    return pltpu.CompilerParams(collective_id=index, has_side_effects=True, vmem_limit_bytes=mib << 20)


def solution(mesh):
    def device_fn(tokens, lengths, embedding, ln_scale, w_q, w_kv, w_o, w_gate, w_up, w_down, final_scale, k_cache, v_cache):
        me = lax.axis_index("tp")
        batch = tokens.shape[1]
        vocab, dim = embedding.shape
        layers, seqs, length, width = k_cache.shape
        hidden = w_gate.shape[-1]
        half = width // TWO
        block = jax.ShapeDtypeStruct((TWO, HALF, dim), BF16)

        def ordered(rows):
            return rows.reshape(TWO, FOUR, TWO, TWO, TWO, HALF).transpose(0, 1, FOUR, TWO, 3, 5).reshape(TWO, FOUR, TWO, LANES)

        positions = lengths[None, :] + jnp.arange(TWO, dtype=jnp.int32)[:, None]
        own_len = lax.dynamic_slice_in_dim(lengths, me * seqs, seqs)
        own_pos = own_len[None, :] + jnp.arange(TWO, dtype=jnp.int32)[:, None]
        inv_freq = 10000.0 ** (-jnp.arange(half, dtype=F32) / half)
        angles = ordered(positions).reshape(TWO, FOUR, 1, ROWS).astype(F32) * inv_freq[None, None, :, None]
        own_angles = jnp.pad(own_pos, ((0, 0), (0, LANES - HALF)))[:, None, :].astype(F32) * inv_freq[None, :, None]
        tok = ordered(tokens).reshape(TWO, FOUR, TWO, FOUR, HALF).transpose(1, TWO, 3, 0, FOUR).reshape(8, ROWS)
        turns = jnp.cos(angles), jnp.sin(angles), jnp.cos(own_angles), jnp.sin(own_angles)

        x, h = pl.pallas_call(
            embed_kernel,
            out_shape=(block, block),
            in_specs=[VMEM, ANY, VMEM],
            out_specs=(VMEM, VMEM),
            scratch_shapes=[pltpu.VMEM((vocab, dim), BF16), pltpu.VMEM((LANES, dim), BF16), DMA((1,)), *Reduce.scratch(HALF, dim, BF16)],
            compiler_params=params(0, 60),
            name="embed",
        )(tok, embedding, ln_scale)

        wg_t, wu_t, wkv_t = (w.transpose(0, TWO, 1) for w in (w_gate, w_up, w_kv))
        wq_t = w_q.transpose(0, TWO, 3, 1).reshape(layers, width, dim)
        wo = w_o.reshape(layers, width, dim)
        k_t, v_t = k_cache.transpose(0, 1, 3, TWO), v_cache.transpose(0, 1, 3, TWO)
        padded = pl.cdiv(vocab, 8) * 8
        tail = jnp.pad(embedding[vocab // ROWS * ROWS :], ((0, padded - vocab), (0, 0)))
        scratch = Layers.scratch(dim, hidden, width, seqs, length)
        logits, fresh = pl.pallas_call(
            functools.partial(layers_kernel, layers, tuple(scratch)),
            out_shape=(jax.ShapeDtypeStruct((TWO, padded, batch), F32), jax.ShapeDtypeStruct((layers, ROWS, BLOCK), BF16)),
            in_specs=[SMEM] + [VMEM] * 9 + [ANY] * 9,
            out_specs=(ANY, VMEM),
            scratch_shapes=list(scratch.values()),
            compiler_params=params(1, 63),
            name="layers",
        )(own_len, x, h, ln_scale, final_scale[None], *turns, tail, wg_t, wu_t, wq_t, wkv_t, w_down, wo, k_t, v_t, embedding)
        steps = 8
        some = layers * seqs // steps
        flat = (layers * seqs, width, length)
        sheet = pl.cdiv(pl.cdiv(vocab, steps), 8) * 8
        cache = pl.BlockSpec((some, width, length), lambda i: (i, 0, 0))
        logits, k_out, v_out = pl.pallas_call(
            last_kernel,
            grid=(steps,),
            out_shape=(jax.ShapeDtypeStruct((vocab, TWO, batch), F32), jax.ShapeDtypeStruct(flat, BF16), jax.ShapeDtypeStruct(flat, BF16)),
            in_specs=[
                SMEM,
                pl.BlockSpec((TWO, sheet, batch), lambda i: (0, i, 0)),
                cache,
                cache,
                pl.BlockSpec((1, ROWS, BLOCK), lambda i: (i * some // seqs, 0, 0)),
            ],
            out_specs=(pl.BlockSpec((sheet, TWO, batch), lambda i: (i, 0, 0)), cache, cache),
            name="last",
        )(own_len, logits, k_t.reshape(flat), v_t.reshape(flat), fresh)
        k_out, v_out = (a.reshape(layers, seqs, width, length).transpose(0, 1, 3, TWO) for a in (k_out, v_out))
        return logits.transpose(1, TWO, 0), k_out, v_out

    cache_spec = P(None, "tp", None, None)
    in_specs = (P(), P(), P("tp", None), P(), P(None, None, "tp", None), P(), P(None, "tp", None, None), P(None, None, "tp"), P(None, None, "tp"), P(None, "tp", None), P(), cache_spec, cache_spec)
    out_specs = (P(None, None, "tp"), cache_spec, cache_spec)
    return jax.shard_map(device_fn, mesh=mesh, in_specs=in_specs, out_specs=out_specs, check_vma=False)
```

```python
import functools

import jax
import jax.numpy as jnp
from jax import lax
from jax.experimental import pallas as pl
from jax.experimental.pallas import tpu as pltpu
from jax.sharding import PartitionSpec as P

LN_EPS = 1e-6
TWO, FOUR = 2, 4
HALF, BLOCK, ROWS, LANES = 32, 64, 256, 128
MESH = pl.DeviceIdType.MESH
BF16, F32 = jnp.bfloat16, jnp.float32
ANY = pl.BlockSpec(memory_space=pl.ANY)
VMEM = pl.BlockSpec(memory_space=pltpu.VMEM)
SMEM = pl.BlockSpec(memory_space=pltpu.SMEM)
DMA = pltpu.SemaphoreType.DMA
FLIPS = [(a, b, e) for a in range(TWO) for b in range(TWO) for e in range(TWO)]
SIDE = 512
ALL = (slice(None),) * 3
CODES = "0123456789abcdefghijklmnopqrstuvwxyz"
STREAMS = "ABCDEFRSTUJKLM"


def numbered(words, slots):
    return tuple(f"{word}{s}" for word in words for s in slots)


TAIL = 40
WIDE = 512
GROUP = 8
REDUCE = "37bq2f6paj1e5oi90nhtm4du8lsrcgkv"
ORDER = (
    "A0AqBqB0A4AkA1AlA8A2BlB8B4BkAmA5B1AcArA9A3B2BmA6AaBcBrB3AoAn",
    "B9B5AdBgBoAhAbBaBnAeB6A7ApAiB7BdBpBbAfAgAjBeBhBfBiBjJ0K0R2R1",
    "R6RaS2R3RiReS6SaRpR7RbS3RqS7SiSbR5SpRmRjRfR9R0SqSjSeRoR4S1S5",
    "SfS9RhRsRdSoS0SnRuRnS4R8ShRtSdStRgSuRcS8SmRlSsRrScSgSlSrRkRv",
    "CqC0SkClC2C4CkC1SvDqCaC8C6D0CmDlCcC9C5D2CrD8D4DkD1CgCdC3DcDm",
    "DaDrCeCnD5D9CoD6D3ChC7CbCiDdDgDoDnD7DbCpDeCfDhCjDfDpDiDjL0T2",
    "M0T0T6T3TaT4U2T7TbTpTiTeU3U6UaTqT1TfU7UbUqT5U1ToTmUeUiTjU5T9",
    "UoUfUjU0TsU9ThUpTdU4TuT8UmUnTnTtUhUdUuUtTcTgTlU8UsTrTkUlUrUc",
    "UgTvE0EqUkElE2EkE4E8UvFqF0EcE1EmEaE6ErF4F8FlE3FkEgEoE9E5F1F2",
    "FcEnEeFmFrEbE7F3FgEdEiF5F9F6FaEpEfEhFnFbFoF7FdEjFeFhFpFfFiFj",
)


class Here:
    def __init__(self):
        me = lax.axis_index("tp")
        self.c = lax.rem(me, TWO)
        self.x = lax.rem(lax.div(me, TWO), TWO)
        self.y = lax.rem(lax.div(me, FOUR), TWO)
        z = lax.div(me, 8)
        self.z = z
        self.against = {id(v): 1 - v for v in (self.c, self.x, self.y)}
        inner = lax.rem(lax.div(z + 1, TWO), TWO)
        self.inner = inner == 1
        two, three = lax.rem(z + TWO, FOUR), 3 - z
        self.zs = [z, z + 1 - TWO * lax.rem(z, TWO), inner * three + (1 - inner) * two, inner * two + (1 - inner) * three]
        self.slot = ((z * TWO + self.c) * TWO + self.y) * TWO + self.x
        self.near, self.across = self.dev(self.zs[1]), self.dev(three)
        self.core, self.along_x, self.along_y = self.dev(z, a=1), self.dev(z, e=1), self.dev(z, b=1)

    def flip(self, v, on):
        return self.against[id(v)] if on else v

    def dev(self, z, a=0, b=0, e=0):
        y, x, c = self.flip(self.y, b), self.flip(self.x, e), self.flip(self.c, a)
        return ((z * TWO + y) * TWO + x) * TWO + c

    def apart(self, s):
        inner = lax.rem(lax.div(self.z + 1, TWO), TWO)
        return (0, 1, TWO + inner, 3 - inner)[s]

    def partner(self, s, f):
        a, b, e = lax.div(f, FOUR), lax.rem(lax.div(f, TWO), TWO), lax.rem(f, TWO)
        c, y, x = (on + v - TWO * on * v for on, v in ((a, self.c), (b, self.y), (e, self.x)))
        return self.apart(s) * 8 + f, c, y * TWO + x, ((self.zs[s] * TWO + y) * TWO + x) * TWO + c

    def lines(self):
        return [self.near, self.dev(self.zs[TWO]), self.dev(self.zs[3]), self.core, self.along_x, self.along_y]

    def all(self):
        z = self.z
        zs = [z, self.zs[1], lax.rem(z + TWO, FOUR), 3 - z]
        return [(8 * j + FOUR * a + TWO * b + e, zs[j], (a, b, e)) for j in range(FOUR) for a, b, e in FLIPS if j or a or b or e]


def meet(devices):
    sem = pltpu.get_barrier_semaphore()
    for d in devices:
        pl.semaphore_signal(sem, inc=1, device_id={"tp": d}, device_id_type=MESH)
    pl.semaphore_wait(sem, len(devices))


class Wires:
    def __init__(self, here, send, recv, sizes):
        self.here, self.send, self.recv = here, send, recv
        self.names, self.first, self.started, at = {}, {}, {}, 0
        for kind, count in sizes.items():
            self.first[kind], self.started[kind] = at, []
            at += count

    def go(self, what, src, dst, device, inner=None):
        kind = tuple(src.shape), inner
        k = self.names.setdefault(what, len(self.names))
        copy = pltpu.make_async_remote_copy(
            src_ref=src,
            dst_ref=dst,
            send_sem=self.send.at[self.first[kind] + len(self.started[kind])],
            recv_sem=self.recv.at[k],
            device_id={"tp": device},
            device_id_type=MESH,
        )
        self.started[kind].append(src)
        if inner is None:
            copy.start()
        else:
            pl.when(self.here.inner == inner)(copy.start)

    def got(self, what, like):
        k = self.names.setdefault(what, len(self.names))
        pltpu.make_async_copy(like, like, self.recv.at[k]).wait()

    def step(self, code):
        name = self.STEPS[CODES.index(code)]
        word = name.rstrip(CODES[:FOUR])
        getattr(self, word)(*map(int, name[len(word) :]))

    def run(self, order):
        for code in "".join(order):
            self.step(code)

    def drain(self):
        for (kind, inner), copies in self.started.items():

            def wait(ref=copies[0], first=self.first[kind, inner], count=len(copies)):
                def one(i, carry):
                    pltpu.make_async_copy(ref, ref, self.send.at[first + i]).wait()
                    return carry

                lax.fori_loop(0, count, one, 0)

            if inner is None:
                wait()
            else:
                pl.when(self.here.inner == inner)(wait)


def nt(a, b):
    return lax.dot_general(a, b, (((1,), (1,)), ((), ())), preferred_element_type=F32)


def nn(a, b):
    return lax.dot_general(a, b, (((1,), (0,)), ((), ())), preferred_element_type=F32)


class Gather(Wires):
    COPIES = 48
    STEPS = numbered(("sh", "tx", "ty", "cl", "us"), range(FOUR)) + numbered(("zf", "ff"), range(1, FOUR)) + ("zown", "fown")

    def __init__(self, here, own, plane, send, recv, use):
        rows, dim = own.shape[1:]
        main, four = ((TWO, rows, dim - SIDE)), (TWO, TWO, TWO, rows, SIDE)
        sizes = {(main, None): 19, (main, True): FOUR, ((TWO, rows, dim), None): 6, (four, None): FOUR, (four, True): FOUR}
        super().__init__(here, send, recv, sizes | {(main[1:], None): 6, ((rows, dim), None): TWO})
        self.own, self.plane, self.use = own, plane, use
        self.main, self.side, self.full = pl.ds(0, dim - SIDE), pl.ds(dim - SIDE, SIDE), pl.ds(0, dim)

    def at(self, s, b=0, e=0):
        h = self.here
        return self.plane(h.zs[s], h.c).at[h.flip(h.y, b), h.flip(h.x, e)].at[:, :, self.main if s else self.full]

    def fours(self, s):
        return self.plane(self.here.zs[s], self.here.c).at[:, :, :, :, self.side]

    def pass_on(self, what, s, ref):
        h = self.here
        self.go((what, 3 if s == 1 else s), ref, ref, h.across if s == 1 else h.near, True)

    def zown(self):
        h = self.here
        src, dst = self.own.at[:, :, self.main], self.at(0).at[:, :, self.main]
        self.go(("z", 1), src, dst, h.near)
        self.go(("z", TWO), src, dst, h.across, True)

    def zf(self, s):
        self.got(("z", s), self.at(s))
        self.pass_on("z", s, self.at(s))

    def fown(self):
        h, ref = self.here, self.fours(0)
        self.go(("f", 1), ref, ref, h.near)
        self.go(("f", TWO), ref, ref, h.across, True)

    def ff(self, s):
        ref = self.fours(s)
        self.got(("f", s), ref)
        self.pass_on("f", s, ref)
        self.go(("cf", s), ref, ref, self.here.core)

    def sh(self, s):
        h, dst = self.here, self.at(s)
        src = dst if s else self.own
        self.go(("x", s), src, dst, h.along_x)
        self.go(("y", s), src, dst, h.along_y)
        self.go(("c", s), src, dst, h.core)

    def tx(self, s):
        ref = self.at(s, e=1)
        self.got(("x", s), ref)
        self.go(("xy", s), ref.at[0], ref.at[0], self.here.along_y)
        self.go(("cx", s), ref, ref, self.here.core)

    def ty(self, s):
        ref = self.at(s, b=1)
        self.got(("y", s), ref)
        self.go(("yx", s), ref.at[1], ref.at[1], self.here.along_x)
        self.go(("cy", s), ref, ref, self.here.core)

    def cl(self, s):
        ref = self.at(s, 1, 1)
        self.got(("xy", s), ref.at[0])
        self.got(("yx", s), ref.at[1])
        self.go(("cd", s), ref, ref, self.here.core)

    def us(self, s):
        for what in ("c", "cx", "cy", "cd"):
            self.got((what, s), self.at(s))
        if s:
            self.got(("cf", s), self.fours(s))
        self.use(s)


class Loans:
    def __init__(self, here, send, free):
        self.here, self.send, self.free = here, send, free
        self.lent, self.out = [], set()

    def take(self, s):
        if s in self.out:
            pl.semaphore_wait(self.free.at[s], 1)
        self.out.add(s)

    def give(self, s):
        pl.semaphore_signal(self.free.at[s], inc=1, device_id={"tp": self.here.core}, device_id_type=MESH)

    def settle(self):
        for copy in self.lent[-TWO:]:
            copy.wait_send()
        for s in self.out:
            pl.semaphore_wait(self.free.at[s], 1)


class Reduce(Wires):
    COPIES = 48
    STEPS = numbered(("fo", "ca", *"dpqu"), range(FOUR)) + numbered(("fz", "gz"), range(1, FOUR)) + ("fin", "end")

    @staticmethod
    def scratch(rows, dim, dtype):
        return [
            pltpu.VMEM((FOUR, FOUR, TWO, rows, dim), dtype),
            pltpu.VMEM((TWO, FOUR, TWO, rows, dim), dtype),
            pltpu.VMEM((FOUR, FOUR, TWO, rows, dim), dtype),
            pltpu.VMEM((FOUR, TWO, rows, dim), dtype),
            pltpu.VMEM((FOUR, TWO, rows, dim), dtype),
            pltpu.VMEM((FOUR, TWO, rows, dim), dtype),
            pltpu.VMEM((5, TWO, rows, dim - SIDE), dtype),
            pltpu.VMEM((5, FOUR, TWO, rows, SIDE), dtype),
            DMA((Reduce.COPIES,)),
            DMA((Reduce.COPIES,)),
            DMA((TWO,)),
            pltpu.SemaphoreType.REGULAR((FOUR,)),
        ]

    def __init__(self, here, fill, finish, loans, part, sib, core_in, diag_in, x_in, y_in, z_in, side_in, send, recv):
        rows, dim = part.shape[3:]
        main, four = (TWO, rows, dim - SIDE), (FOUR, TWO, rows, SIDE)
        sizes = {(main[1:], None): 18, ((rows, dim), None): 6, (four, True): 3, (four, False): 3, (main, True): 3, (main, False): 3}
        super().__init__(here, send, recv, sizes)
        self.fill, self.finish, self.loans = fill, finish, loans
        self.part, self.sib, self.core_in, self.diag_in = part, sib, core_in, diag_in
        self.x_in, self.y_in, self.z_in, self.side_in = x_in, y_in, z_in, side_in
        dim = part.shape[-1]
        self.main, self.side, self.full = pl.ds(0, dim - SIDE), pl.ds(dim - SIDE, SIDE), pl.ds(0, dim)

    def quad(self, b, e):
        h = self.here
        return h.flip(h.y, b) * TWO + h.flip(h.x, e)

    def piece(self, buf, s, *where):
        return buf, (s, *where, slice(None), self.main if s else self.full)

    def add(self, ref, *more):
        buf, index = ref
        total = buf[index]
        for other, where in more:
            total = total + other[where]
        buf[index] = total

    def fo(self, s):
        loans, n = self.loans, len(self.loans.lent)
        if n > 1:
            loans.lent[n - TWO].wait_send()
        k = self.names.setdefault(("c", s), len(self.names))
        copy = pltpu.make_async_remote_copy(
            src_ref=self.sib.at[n % TWO],
            dst_ref=self.core_in.at[s],
            send_sem=loans.send.at[n % TWO],
            recv_sem=self.recv.at[k],
            device_id={"tp": self.here.core},
            device_id_type=MESH,
        )

        def send():
            loans.take(s)
            copy.start()
            loans.lent.append(copy)

        self.fill(s, self.sib.at[n % TWO], self.part.at[s], send)

    def ca(self, s):
        self.got(("c", s), self.core_in.at[s])
        for t in range(TWO):

            def add(i, carry):
                self.add((self.part, (s, i, t)), (self.core_in, (s, i, t)))
                return carry

            lax.fori_loop(0, FOUR, add, 0)
        self.loans.give(s)

    def along_z(self, what, s, ref, landing):
        h = self.here
        k = 5 if s == 1 else s
        to = 1 if s == 1 else s + TWO

        @pl.when(h.inner)
        def _():
            self.got((what, k), landing.at[k - 1])
            self.add(ref, (landing, k - 1))

        self.go((what, to), ref[0].at[ref[1]], landing.at[to - 1], h.near if s == 1 else h.across, True)
        self.go((what, s), ref[0].at[ref[1]], landing.at[s - 1], h.near, False)

    def last_z(self, what, ref, landing):
        self.got((what, 1), landing.at[0])
        self.add(ref, (landing, 0))

        @pl.when(self.here.inner)
        def _():
            self.got((what, FOUR), landing.at[3])
            self.add(ref, (landing, 3))

    def fz(self, s):
        self.along_z("f", s, (self.part, (s, *ALL, self.side)), self.side_in)

    def fin(self):
        self.last_z("f", (self.part, (0, *ALL, self.side)), self.side_in)

    def d(self, s):
        h, part = self.here, self.part
        far = self.quad(1, 1)
        self.pass_on("dy", s, self.piece(part, s, far, 0), self.piece(self.diag_in, s, 0), h.along_y)
        self.pass_on("dx", s, self.piece(part, s, far, 1), self.piece(self.diag_in, s, 1), h.along_x)
        self.pass_on("x1", s, self.piece(part, s, self.quad(0, 1), 1), self.piece(self.x_in, s, 1), h.along_x)
        self.pass_on("y0", s, self.piece(part, s, self.quad(1, 0), 0), self.piece(self.y_in, s, 0), h.along_y)

    def pass_on(self, what, s, src, dst, device):
        self.go((what, s), src[0].at[src[1]], dst[0].at[dst[1]], device)

    def came(self, what, s, ref):
        self.got((what, s), ref[0].at[ref[1]])

    def p(self, s):
        ref = self.piece(self.part, s, self.quad(0, 1), 0)
        self.came("dy", s, ref)
        self.add(ref, self.piece(self.diag_in, s, 0))
        self.pass_on("x0", s, ref, self.piece(self.x_in, s, 0), self.here.along_x)

    def q(self, s):
        ref = self.piece(self.part, s, self.quad(1, 0), 1)
        self.came("dx", s, ref)
        self.add(ref, self.piece(self.diag_in, s, 1))
        self.pass_on("y1", s, ref, self.piece(self.y_in, s, 1), self.here.along_y)

    def u(self, s):
        for t in range(TWO):
            ref = self.piece(self.part, s, self.quad(0, 0), t)
            self.came(f"x{t}", s, ref)
            self.came(f"y{t}", s, ref)
            self.add(ref, self.piece(self.x_in, s, t), self.piece(self.y_in, s, t))

    def gz(self, s):
        self.along_z("g", s, (self.part, (s, self.quad(0, 0), *ALL[:TWO], self.main)), self.z_in)

    def end(self):
        mine = self.quad(0, 0)
        self.last_z("g", (self.part, (0, mine, *ALL[:TWO], self.main)), self.z_in)
        for t in range(TWO):
            for lo in range(0, self.part.shape[3], 16):
                self.finish(t, lo, self.part[0, mine, t, lo : lo + 16])


def normed(x, gain):
    rows = x.astype(F32)
    centred = rows - jnp.mean(rows, axis=-1, keepdims=True)
    var = jnp.mean(centred * centred, axis=-1, keepdims=True)
    return (centred * lax.rsqrt(var + LN_EPS) * gain).astype(BF16)


def load(pairs, sems):
    copies = [pltpu.make_async_copy(src, dst, sems.at[i]) for i, (src, dst) in enumerate(pairs)]
    for copy in copies:
        copy.start()
    return copies


def embed_kernel(tok_ref, emb_hbm, gain_ref, x_ref, h_ref, tail_ref, emb, tail, toks, sem, *scratch):
    here = Here()
    vocab, dim = emb_hbm.shape
    whole = vocab // ROWS * ROWS
    rest = vocab - whole
    (fetch,) = load([(emb_hbm, emb)], sem)
    meet(here.lines())
    fetch.wait()
    tail[...] = jnp.zeros_like(tail)
    tail[0:rest] = emb[whole:vocab]
    tail_ref[...] = tail[0:TAIL]
    toks[...] = jnp.concatenate([tok_ref[...].astype(F32), jnp.zeros((6, tok_ref.shape[1]), F32)], 0).T
    base = lax.axis_index("tp") * vocab

    def fill(s, other, own, send):
        for core, ref, then in ((here.flip(here.c, 1), other, send), (here.c, own, None)):
            tok = []
            for quad in range(FOUR):
                rows = toks[pl.ds(pl.multiple_of(here.zs[s] * ROWS + quad * BLOCK + core * HALF, HALF), HALF), :]
                for t in range(TWO):
                    step = lax.broadcasted_iota(jnp.int32, rows.shape, 1) == t
                    tok.append(jnp.sum(jnp.where(step, rows, 0.0), axis=1, keepdims=True))
            tok = jnp.concatenate(tok, 0).astype(jnp.int32) - base
            hot = (tok == lax.broadcasted_iota(jnp.int32, (ROWS, whole), 1)).astype(F32).astype(BF16)
            hot_tail = (tok == lax.broadcasted_iota(jnp.int32, (ROWS, LANES), 1) + whole).astype(F32).astype(BF16)

            def columns(n, carry):
                cols = pl.ds(pl.multiple_of(n * WIDE, WIDE), WIDE)
                rows = nn(hot, emb[0:whole, cols]) + nn(hot_tail, tail[:, cols])
                ref[:, :, :, cols] = rows.astype(BF16).reshape(FOUR, TWO, HALF, WIDE)
                return carry

            lax.fori_loop(0, dim // WIDE, columns, 0)
            if then:
                then()

    def finish(t, lo, rows):
        x_ref[t, lo : lo + 16] = rows
        h_ref[t, lo : lo + 16] = normed(rows, gain_ref[0:1])

    *rs, lent, free = scratch
    loans = Loans(here, lent, free)
    red = Reduce(here, fill, finish, loans, *rs)
    red.run(REDUCE)
    red.drain()
    loans.settle()


def attention(t, lengths, q_rows, fresh, keys, values, o_rows):
    seqs, width, length = keys.shape
    col = lax.broadcasted_iota(jnp.int32, (HALF, length), 1)
    blank = jnp.zeros((LANES - width, length), BF16)

    def several(i, carry):
        some = [i * GROUP + u for u in range(GROUP)]
        pos = [lengths[s] for s in some]
        q = [q_rows[pl.ds(s, HALF, stride=HALF), :] for s in some]
        new = [[fresh[step, pl.ds(s, 1), :] for step in range(t + 1)] for s in some]
        score = [nn(a.astype(BF16), jnp.concatenate([keys[s], blank], 0)) for a, s in zip(q, some)]
        own = [[jnp.sum(a * row[:, 0:LANES], axis=-1, keepdims=True) for row in rows] for a, rows in zip(q, new)]
        for u in range(GROUP):
            for step in range(t + 1):
                score[u] = jnp.where(col == pos[u] + step, own[u][step], score[u])
            score[u] = jnp.where(col <= pos[u] + t, score[u] * width**-0.5, -jnp.inf)
        top = [jnp.max(a, axis=-1, keepdims=True) for a in score]
        weight = [jnp.exp(a - b) for a, b in zip(score, top)]
        total = [jnp.sum(a, axis=-1, keepdims=True) for a in weight]
        weight = [(a / b).astype(BF16).astype(F32) for a, b in zip(weight, total)]
        at = [[col == p + step for step in range(t + 1)] for p in pos]
        mine = [[jnp.sum(jnp.where(hit, a, 0.0), axis=-1, keepdims=True) for hit in hits] for a, hits in zip(weight, at)]
        for u in range(GROUP):
            for hit in at[u]:
                weight[u] = jnp.where(hit, 0.0, weight[u])
        out = [nt(a.astype(BF16), jnp.concatenate([values[s], blank], 0)) for a, s in zip(weight, some)]
        for u in range(GROUP):
            for step in range(t + 1):
                out[u] = out[u] + mine[u][step] * new[u][step][:, LANES:ROWS]
            o_rows[pl.ds(some[u], HALF, stride=HALF), :] = out[u]
        return carry

    lax.fori_loop(0, seqs // GROUP, several, 0)


class Layers:
    @staticmethod
    def scratch(dim, hidden, width, seqs, length):
        up_at = pl.cdiv(hidden, LANES) * LANES
        return dict(
            x=pltpu.VMEM((TWO, TWO, 16, dim), BF16),
            h=pltpu.VMEM((TWO, TWO, 16, dim), BF16),
            every=pltpu.VMEM((TWO, FOUR, TWO, TWO, TWO, TWO, 16, dim), BF16),
            wide=pltpu.VMEM((TWO * up_at, dim), BF16),
            wq=pltpu.VMEM((LANES, dim), BF16),
            wkv=pltpu.VMEM((TWO * width, dim), BF16),
            wd=pltpu.VMEM((hidden, dim), BF16),
            wo=pltpu.VMEM((LANES, dim), BF16),
            ready=pltpu.VMEM((ROWS, TWO * up_at), F32),
            m=pltpu.VMEM((TWO, FOUR, ROWS, hidden), BF16),
            q_out=pltpu.VMEM((TWO, FOUR, TWO, FOUR, HALF, LANES), BF16),
            q_in=pltpu.VMEM((TWO, 8, FOUR, HALF, LANES), BF16),
            o_out=pltpu.VMEM((TWO, 8, FOUR, HALF, LANES), BF16),
            o_in=pltpu.VMEM((TWO, 8, FOUR, HALF, LANES), BF16),
            q_rows=pltpu.VMEM((1024, LANES), F32),
            o_rows=pltpu.VMEM((1024, LANES), F32),
            fresh=pltpu.VMEM((TWO, LANES, ROWS), F32),
            keys=pltpu.VMEM((seqs, width, length), BF16),
            values=pltpu.VMEM((seqs, width, length), BF16),
            tiles=pltpu.VMEM((3, ROWS, dim), BF16),
            logits=pltpu.VMEM((TWO, ROWS, ROWS), F32),
            last=pltpu.VMEM((TAIL, ROWS), F32),
            w_sem=DMA((8,)),
            tile_sem=DMA((3,)),
            logit_sem=DMA((3,)),
            q_send=DMA((TWO, HALF)),
            q_recv=DMA((TWO, HALF)),
            o_send=DMA((TWO, HALF)),
            o_recv=DMA((TWO, HALF)),
            g_send=DMA((TWO, Gather.COPIES)),
            g_recv=DMA((TWO, Gather.COPIES)),
            part=pltpu.VMEM((TWO, FOUR, FOUR, TWO, 16, dim), F32),
            sib=pltpu.VMEM((TWO, FOUR, TWO, 16, dim), F32),
            core_in=pltpu.VMEM((FOUR, FOUR, TWO, 16, dim), F32),
            diag_in=pltpu.VMEM((TWO, FOUR, TWO, 16, dim), F32),
            x_in=pltpu.VMEM((TWO, FOUR, TWO, 16, dim), F32),
            y_in=pltpu.VMEM((TWO, FOUR, TWO, 16, dim), F32),
            z_in=pltpu.VMEM((TWO, 5, TWO, 16, dim - SIDE), F32),
            side_in=pltpu.VMEM((TWO, 5, FOUR, TWO, 16, SIDE), F32),
            r_send=DMA((TWO, Reduce.COPIES)),
            r_recv=DMA((TWO, Reduce.COPIES)),
            lent=DMA((TWO,)),
            free=pltpu.SemaphoreType.REGULAR((FOUR,)),
        )

    def __init__(self, layers, **refs):
        self.__dict__.update(refs)
        here = self.here = Here()
        self.count = layers
        self.dim, self.hidden, self.width = self.h.shape[-1], self.m.shape[-1], self.keys.shape[1]
        self.up_at = self.wide.shape[0] // TWO
        self.whole = self.emb_hbm.shape[0] // ROWS * ROWS
        self.loads, self.answered, self.heads, self.fills = {}, set(), 0, 0
        self.stream = {}
        self.loans = Loans(here, self.lent, self.free)
        letters = iter(STREAMS)
        for l in range(layers + 1):
            for t in range(TWO):
                use = functools.partial(self.project if l < layers else self.head, l, t)
                if l < layers:
                    plane = functools.partial(lambda t, z, c: self.every.at[t, z, c], t)
                else:
                    plane = functools.partial(lambda t, z, c: self.every.at[t, z, :, :, c], t)
                self.stream[next(letters)] = Gather(here, self.h.at[t], plane, self.g_send.at[t], self.g_recv.at[t], use)
        for l in range(layers):
            for t in range(TWO):
                fill, finish = functools.partial(self.fill, l, t), functools.partial(self.finish, l, t)
                mine = [ref.at[t] for ref in (self.diag_in, self.x_in, self.y_in, self.z_in, self.side_in, self.r_send, self.r_recv)]
                reduce = Reduce(here, fill, finish, self.loans, self.part.at[t], self.sib, self.core_in, *mine)
                self.stream[next(letters)] = reduce
        for l in range(layers):
            for t in range(TWO):
                self.stream[next(letters)] = (l, t)

    def load(self, name, l):
        groups = {
            "in": [(self.wg_hbm, self.wide.at[0 : self.hidden]), (self.wu_hbm, self.wide.at[self.up_at : self.up_at + self.hidden]),
                   (self.wq_hbm, self.wq.at[0 : self.width])],
            "out": [(self.wd_hbm, self.wd), (self.wo_hbm, self.wo.at[0 : self.width])],
            "kv": [(self.wkv_hbm, self.wkv), (self.k_hbm, self.keys), (self.v_hbm, self.values)],
        }
        first = {"in": 0, "out": 3, "kv": 5}[name]
        copies = [pltpu.make_async_copy(src.at[l], dst, self.w_sem.at[first + i]) for i, (src, dst) in enumerate(groups[name])]
        for copy in copies:
            copy.start()
        self.loads[name] = copies

    def ready_for(self, name):
        for copy in self.loads.pop(name, ()):
            copy.wait()

    def turned(self, rows, cos, sin):
        half = self.width // TWO
        lo, hi = rows[0:half], rows[half : self.width]
        return lo * cos - hi * sin, lo * sin + hi * cos

    def each(self, s, body, own=None):
        if s == 0 and own:
            own(self.here.c, self.here.y * TWO + self.here.x)

        def one(f, carry):
            body(*self.here.partner(s, f))
            return carry

        lax.fori_loop(0 if s else 1, 8, one, 0)

    def trip(self, kind, t, r, src, dst, device):
        sends, recvs = (self.q_send, self.q_recv) if kind == "q" else (self.o_send, self.o_recv)
        return pltpu.make_async_remote_copy(
            src_ref=src, dst_ref=dst, send_sem=sends.at[t, r], recv_sem=recvs.at[t, r], device_id={"tp": device}, device_id_type=MESH
        )

    def arrived(self, sems, t, r):
        ref = self.q_in.at[t, 0, 0]
        pltpu.make_async_copy(ref, ref, sems.at[t, r]).wait()

    def all_arrived(self, t, *sems):
        def one(r, carry):
            for sem in sems:
                self.arrived(sem, t, r)
            return carry

        lax.fori_loop(1, HALF, one, 0)

    def mine(self):
        h = self.here
        return h.z * TWO + h.c, h.y * TWO + h.x

    def project(self, l, t, s):
        self.ready_for("in")
        z, dim = self.here.zs[s], self.dim

        def rows():
            return self.every[t, z].reshape(ROWS, dim)

        q = nt(self.wq[...], rows())
        lo, hi = self.turned(q, self.cos[t, z], self.sin[t, z])
        q = jnp.concatenate([lo, hi, jnp.zeros((LANES - self.width, ROWS), F32)], 0)
        self.q_out[t, z] = q.T.astype(BF16).reshape(TWO, FOUR, HALF, LANES)
        zc, quad = self.mine()

        def ask(r, core, four, device):
            self.trip("q", t, r, self.q_out.at[t, z, core, four], self.q_in.at[t, zc, quad], device).start()

        def keep(core, four):
            self.q_in[t, zc, quad] = self.q_out[t, z, core, four]

        self.each(s, ask, keep)

        def tile(n, carry):
            cols = pl.ds(pl.multiple_of(n * ROWS, ROWS), ROWS)
            self.ready[:, cols] = nt(rows(), self.wide[cols])
            return carry

        lax.fori_loop(0, self.wide.shape[0] // ROWS, tile, 0)

        def gated(n, carry):
            some = pl.ds(pl.multiple_of(n * HALF, HALF), HALF)
            gate, up = self.ready[some, 0 : self.hidden], self.ready[some, self.up_at : self.up_at + self.hidden]
            self.m[t, z, some] = (gate * jax.nn.sigmoid(gate) * up).astype(BF16)
            return carry

        lax.fori_loop(0, 8, gated, 0)

    def attend(self, l, t):
        width = self.width
        self.ready_for("kv")
        self.stream[STREAMS[TWO * l + t]].drain()
        self.all_arrived(t, self.q_recv, self.q_send)
        mine = jnp.concatenate([self.h[t].reshape(HALF, self.dim), jnp.zeros((LANES - HALF, self.dim), BF16)], 0)
        rows = nt(self.wkv[...], mine)
        lo, hi = self.turned(rows, self.cos_own[t], self.sin_own[t])
        blank = jnp.zeros((LANES - width, LANES), BF16)
        new = jnp.concatenate([jnp.concatenate([lo, hi], 0).astype(BF16), blank, rows[width:].astype(BF16), blank], 0)
        self.kv_out[l, :, HALF * t : HALF * t + HALF] = new[:, 0:HALF]
        self.fresh[t] = new.astype(F32).T
        self.q_rows[...] = self.q_in[t].reshape(1024, LANES).astype(F32)
        attention(t, self.lengths, self.q_rows, self.fresh, self.keys, self.values, self.o_rows)
        self.o_out[t] = self.o_rows[...].astype(BF16).reshape(8, FOUR, HALF, LANES)
        zc, quad = self.mine()
        for s in range(FOUR):
            z = self.here.zs[s]

            def answer(r, core, four, device, z=z):
                self.trip("o", t, r, self.o_out.at[t, z * TWO + core, four], self.o_in.at[t, zc, quad], device).start()

            def keep(core, four, z=z):
                self.o_in[t, zc, quad] = self.o_out[t, z * TWO + core, four]

            self.each(s, answer, keep)
        if t and l + 1 < self.count:
            self.load("in", l + 1)
            self.load("kv", l + 1)

    def fill(self, l, t, s, other, own, send):
        self.ready_for("out")
        if (l, t, s) not in self.answered:
            self.answered.add((l, t, s))
            self.each(s, lambda r, core, four, device: self.arrived(self.o_recv, t, r))
        z, c = self.here.zs[s], self.here.c
        cores = self.here.flip(c, 1), c
        heads = jnp.concatenate([self.o_in[t, z * TWO + core].reshape(LANES, LANES) for core in cores], 0)
        hidden = jnp.concatenate([self.m[t, z, pl.ds(pl.multiple_of(core * LANES, LANES), LANES)] for core in cores], 0)

        def columns(n, carry):
            cols = pl.ds(pl.multiple_of(n * WIDE, WIDE), WIDE)
            rows = nn(heads, self.wo[:, cols]) + nn(hidden, self.wd[:, cols])
            other[:, :, :, cols] = rows[0:LANES].reshape(FOUR, TWO, 16, WIDE)
            own[:, :, :, cols] = rows[LANES:].reshape(FOUR, TWO, 16, WIDE)
            return carry

        lax.fori_loop(0, self.dim // WIDE, columns, 0)
        send()
        self.fills += 1
        if self.fills == 8 * (l + 1) and l + 1 < self.count:
            self.load("out", l + 1)

    def finish(self, l, t, half, lo, rows):
        x = (self.x[t, half].astype(F32) + rows).astype(BF16)
        self.x[t, half] = x
        self.h[t, half] = normed(x, self.gains[l + 1 : l + TWO])

    def tile(self, i):
        at = lax.rem(i, 3)
        return pltpu.make_async_copy(self.emb_hbm.at[pl.ds(pl.multiple_of(i * ROWS, ROWS), ROWS)], self.tiles.at[at], self.tile_sem.at[at])

    def store(self, t, z, i):
        at = lax.rem(i, TWO)
        rows, cols = pl.ds(pl.multiple_of(i * ROWS, ROWS), ROWS), pl.ds(pl.multiple_of(z * ROWS, ROWS), ROWS)
        return pltpu.make_async_copy(self.logits.at[at], self.out_hbm.at[t, rows, cols], self.logit_sem.at[at])

    def store_last(self, t, z):
        rows, cols = pl.ds(self.whole, TAIL), pl.ds(pl.multiple_of(z * ROWS, ROWS), ROWS)
        return pltpu.make_async_copy(self.last, self.out_hbm.at[t, rows, cols], self.logit_sem.at[TWO])

    def head(self, l, t, s):
        z, dim, count = self.here.zs[s], self.dim, self.whole // ROWS
        first, final = self.heads == 0, self.heads == 7
        self.heads += 1

        def rows():
            return self.every[t, z].reshape(ROWS, dim)

        if not first:
            self.store_last(t, z).wait()
        self.last[...] = nt(self.emb_tail[0:TAIL], rows()) * dim**-0.5
        self.store_last(t, z).start()

        def one(i, carry):
            @pl.when((i + TWO < count) if final else (i >= 0))
            def _():
                self.tile(lax.rem(i + TWO, count)).start()

            self.tile(i).wait()

            @pl.when((i >= TWO) if first else (i >= 0))
            def _():
                self.store(t, z, i).wait()

            self.logits[lax.rem(i, TWO)] = nt(self.tiles[lax.rem(i, 3)], rows()) * dim**-0.5
            self.store(t, z, i).start()
            return carry

        lax.fori_loop(0, count, one, 0)
        if final:
            self.store(t, z, 0).wait()
            self.store(t, z, 1).wait()
            self.store_last(t, z).wait()

    def run(self, order):
        h = self.here
        for name in ("in", "kv", "out"):
            self.load(name, 0)
        self.tile(0).start()
        self.tile(1).start()
        self.h[...] = self.h_ref[...].reshape(self.h.shape)
        self.x[...] = self.x_ref[...].reshape(self.x.shape)
        self.wq[self.width : LANES] = jnp.zeros((LANES - self.width, self.dim), BF16)
        self.wo[self.width : LANES] = jnp.zeros((LANES - self.width, self.dim), BF16)
        for at in (0, self.up_at):
            self.wide[at + self.hidden : at + self.up_at] = jnp.zeros((self.up_at - self.hidden, self.dim), BF16)
        meet([h.dev(z, *f) for _, z, f in h.all()])
        placed = set()
        order = "".join(order)
        for letter, code in zip(order[::TWO], order[1::TWO], strict=True):
            who, at = self.stream[letter], STREAMS.index(letter)
            if isinstance(who, tuple):
                self.attend(*who)
                continue
            if letter not in placed and isinstance(who, Gather):
                placed.add(letter)
                core_inner = (h.y, h.x, h.c) if letter in "EF" else (h.c, h.y, h.x)
                self.every[(at % TWO, h.z, *core_inner)] = self.h[at % TWO]
            who.step(code)
            if who.STEPS[CODES.index(code)] == "end":
                who.drain()
                self.all_arrived(at % TWO, self.o_send)
        for letter in "EF":
            self.stream[letter].drain()
        self.loans.settle()


def layers_kernel(layers, names, lengths, x_ref, h_ref, gains, cos, sin, cos_own, sin_own, emb_tail, wg_hbm, wu_hbm, wq_hbm, wkv_hbm,
                  wd_hbm, wo_hbm, k_hbm, v_hbm, emb_hbm, out_hbm, kv_out, *scratch):
    refs = dict(locals(), **dict(zip(names, scratch, strict=True)))
    del refs["names"], refs["scratch"]
    Layers(**refs).run(ORDER)


def last_kernel(lengths, in_ref, k_ref, v_ref, new_ref, out_ref, k_out, v_out):
    for t in range(TWO):
        out_ref[:, t, :] = in_ref[t]
    some, width, length = k_ref.shape
    seqs = lengths.shape[0]
    row = lax.broadcasted_iota(jnp.int32, (TWO * seqs, length), 0)
    col = lax.broadcasted_iota(jnp.int32, (TWO * seqs, length), 1)
    cols = lax.broadcasted_iota(jnp.int32, (width, length), 1)
    first = lax.rem(pl.program_id(0) * some, seqs)
    pos = [lengths[first + u] for u in range(some)]
    place = [((row == first + u) & (col == p)) | ((row == first + u + seqs) & (col == p + 1)) for u, p in enumerate(pos)]
    new = [nn(new_ref[0], a.astype(F32).astype(BF16)).astype(BF16) for a in place]
    for u, p in enumerate(pos):
        fresh = (cols == p) | (cols == p + 1)
        k_out[u] = jnp.where(fresh, new[u][0:width], k_ref[u])
        v_out[u] = jnp.where(fresh, new[u][LANES : LANES + width], v_ref[u])


def params(index, mib):
    return pltpu.CompilerParams(collective_id=index, has_side_effects=True, vmem_limit_bytes=mib << 20)


def solution(mesh):
    def device_fn(tokens, lengths, embedding, ln_scale, w_q, w_kv, w_o, w_gate, w_up, w_down, final_scale, k_cache, v_cache):
        me = lax.axis_index("tp")
        batch = tokens.shape[1]
        vocab, dim = embedding.shape
        layers, seqs, length, width = k_cache.shape
        hidden = w_gate.shape[-1]
        half = width // TWO
        block = jax.ShapeDtypeStruct((TWO, HALF, dim), BF16)

        def ordered(rows):
            return rows.reshape(TWO, FOUR, TWO, TWO, TWO, HALF).transpose(0, 1, FOUR, TWO, 3, 5).reshape(TWO, FOUR, TWO, LANES)

        positions = lengths[None, :] + jnp.arange(TWO, dtype=jnp.int32)[:, None]
        own_len = lax.dynamic_slice_in_dim(lengths, me * seqs, seqs)
        own_pos = own_len[None, :] + jnp.arange(TWO, dtype=jnp.int32)[:, None]
        inv_freq = 10000.0 ** (-jnp.arange(half, dtype=F32) / half)
        angles = ordered(positions).reshape(TWO, FOUR, 1, ROWS).astype(F32) * inv_freq[None, None, :, None]
        own_angles = jnp.pad(own_pos, ((0, 0), (0, LANES - HALF)))[:, None, :].astype(F32) * inv_freq[None, :, None]
        turns = jnp.cos(angles), jnp.sin(angles), jnp.cos(own_angles), jnp.sin(own_angles)

        gains = jnp.concatenate([ln_scale, final_scale[None]], 0)
        padded = pl.cdiv(vocab, 8) * 8
        x, h, tail = pl.pallas_call(
            embed_kernel,
            out_shape=(block, block, jax.ShapeDtypeStruct((TAIL, dim), BF16)),
            in_specs=[VMEM, ANY, VMEM],
            out_specs=(VMEM, VMEM, VMEM),
            scratch_shapes=[pltpu.VMEM((vocab, dim), BF16), pltpu.VMEM((LANES, dim), BF16), pltpu.VMEM((batch, 8), F32), DMA((1,)), *Reduce.scratch(HALF, dim, BF16)],
            compiler_params=params(0, 60),
            name="embed",
        )(tokens, embedding, gains)

        wg_t, wu_t, wkv_t = (w.transpose(0, TWO, 1) for w in (w_gate, w_up, w_kv))
        wq_t = w_q.transpose(0, TWO, 3, 1).reshape(layers, width, dim)
        wo = w_o.reshape(layers, width, dim)
        k_t, v_t = k_cache.transpose(0, 1, 3, TWO), v_cache.transpose(0, 1, 3, TWO)
        scratch = Layers.scratch(dim, hidden, width, seqs, length)
        logits, fresh = pl.pallas_call(
            functools.partial(layers_kernel, layers, tuple(scratch)),
            out_shape=(jax.ShapeDtypeStruct((TWO, padded, batch), F32), jax.ShapeDtypeStruct((layers, ROWS, BLOCK), BF16)),
            in_specs=[SMEM] + [VMEM] * 8 + [ANY] * 9,
            out_specs=(ANY, VMEM),
            scratch_shapes=list(scratch.values()),
            compiler_params=params(1, 63),
            name="layers",
        )(own_len, x, h, gains, *turns, tail, wg_t, wu_t, wq_t, wkv_t, w_down, wo, k_t, v_t, embedding)
        steps = 16
        some = layers * seqs // steps
        flat = (layers * seqs, width, length)
        sheet = pl.cdiv(pl.cdiv(vocab, steps), 8) * 8
        cache = pl.BlockSpec((some, width, length), lambda i: (i, 0, 0))
        logits, k_out, v_out = pl.pallas_call(
            last_kernel,
            grid=(steps,),
            out_shape=(jax.ShapeDtypeStruct((vocab, TWO, batch), F32), jax.ShapeDtypeStruct(flat, BF16), jax.ShapeDtypeStruct(flat, BF16)),
            in_specs=[
                SMEM,
                pl.BlockSpec((TWO, sheet, batch), lambda i: (0, i, 0)),
                cache,
                cache,
                pl.BlockSpec((1, ROWS, BLOCK), lambda i: (i * some // seqs, 0, 0)),
            ],
            out_specs=(pl.BlockSpec((sheet, TWO, batch), lambda i: (i, 0, 0)), cache, cache),
            name="last",
        )(own_len, logits, k_t.reshape(flat), v_t.reshape(flat), fresh)
        k_out, v_out = (a.reshape(layers, seqs, width, length).transpose(0, 1, 3, TWO) for a in (k_out, v_out))
        return logits.transpose(1, TWO, 0), k_out, v_out

    cache_spec = P(None, "tp", None, None)
    in_specs = (P(), P(), P("tp", None), P(), P(None, None, "tp", None), P(), P(None, "tp", None, None), P(None, None, "tp"), P(None, None, "tp"), P(None, "tp", None), P(), cache_spec, cache_spec)
    out_specs = (P(None, None, "tp"), cache_spec, cache_spec)
    return jax.shard_map(device_fn, mesh=mesh, in_specs=in_specs, out_specs=out_specs, check_vma=False)
```
